256 devices in a mesh: seq: 32 (over z, x), tp: 8 (over y, core).
Axes of the slice: x: 4, y: 4, z: 8, core: 2. Of those that a mesh axis runs over, the one named last changes fastest.
Arguments:
- packed_input: int32 [2048, 5120], P('seq', 'tp'), may hold values from -2147483648 to 2147483646
- block_exponent: int32 [40, 16384], P('tp', 'seq'), may hold values from -5 to -1
- gate_input: bfloat16 [16384, 5120], P('seq', 'tp'), may hold values from -80 to 80
- state_write: bfloat16 [16384, 128], P('seq'), may hold values from -6 to 6
- state_read: bfloat16 [16384, 128], P('seq'), may hold values from -6 to 6
- log_decay: float32 [80, 16384], P('tp', 'seq'), may hold values from -1.6 to 0
- skip_weight: float32 [80], P('tp'), may hold values from 0.3 to 3
- norm_gain: float32 [5120], P('tp'), may hold values from 0.5 to 1.5
- out_weight: bfloat16 [5120, 2560], P('tp'), may hold values from -0.078125 to 0.078125
- out_cotangent: bfloat16 [16384, 2560], P('seq', 'tp'), may hold values from -6 to 6
Outputs:
- grad_input: bfloat16 [16384, 5120], P('seq', 'tp')
- grad_gate: bfloat16 [16384, 5120], P('seq', 'tp')
- grad_write: float32 [16384, 128], P('seq')
- grad_read: float32 [16384, 128], P('seq')
- grad_decay: float32 [80, 16384], P('tp', 'seq')
- grad_skip: float32 [80], P('tp')
- grad_gain: float32 [5120], P('tp')
- grad_out_weight: float32 [5120, 2560], P('tp', 'seq')
The draws below stay inside these ranges and needn't reach their ends.
All inputs are finite; a program needn't handle non-finite values.
Results may differ from the reference program's by a relative error of at most 0.0049.
Values may be sent and summed in bfloat16 or wider, within the bound.
A program may use at most 128 MiB of HBM per device.

```python
import math
import jax
import jax.numpy as jnp
from jax import lax

D = 2560
HEAD_NUMBER = 80
N = 128
QBLOCK = 128
TOK_DEV = 512
TOKEN_NUMBER = 16384
HP = 5120


def draw_gate_input(key, part):
    first_key, second_key = jax.random.split(jax.random.fold_in(key, 11))
    column_pos = jnp.arange(HP, dtype=jnp.float32) / (HP - 1)
    base = jax.random.truncated_normal(first_key, -4.0, 4.0, (TOKEN_NUMBER, HP), jnp.float32)
    column_scale = 3.0 ** column_pos
    row_scale = jnp.exp(jax.random.uniform(second_key, (TOKEN_NUMBER, 1), jnp.float32, math.log(0.3), math.log(3.0)))
    return (base * column_scale[None, :] * row_scale).astype(jnp.bfloat16)


def draw_log_decay(key, part):
    random_keys = jax.random.split(jax.random.fold_in(key, 23), 7)
    slow_share = 0.5
    is_slow = jax.random.uniform(random_keys[0], (HEAD_NUMBER, 1), jnp.float32) < slow_share
    slow_rate = jax.random.uniform(random_keys[1], (HEAD_NUMBER, 1), jnp.float32, 0.15, 0.6) / TOKEN_NUMBER
    fast_rate = jnp.exp(jax.random.uniform(random_keys[2], (HEAD_NUMBER, 1), jnp.float32, math.log(1.0 / 50.0), math.log(1.0 / 30.0)))
    baseline_rate = jnp.where(is_slow, slow_rate, fast_rate)
    coarse_values = jnp.exp(jax.random.uniform(random_keys[3], (HEAD_NUMBER, TOKEN_NUMBER), jnp.float32, math.log(0.5), math.log(2.0)))
    block_multiplier = jnp.exp(jax.random.uniform(random_keys[4], (HEAD_NUMBER, TOKEN_NUMBER // TOK_DEV), jnp.float32, math.log(0.5), math.log(2.0)))
    block_multiplier = jnp.repeat(block_multiplier, TOK_DEV, axis=1)
    spike_position = jax.random.randint(random_keys[5], (HEAD_NUMBER, 2), 0, TOKEN_NUMBER)
    spike_magnitude = jax.random.uniform(random_keys[6], (HEAD_NUMBER, 2), jnp.float32, 0.22, 0.69)
    token_places = jnp.arange(TOKEN_NUMBER)[None, :]
    spike_list = jnp.where(token_places == spike_position[:, 0:1], spike_magnitude[:, 0:1], 0.0) + jnp.where(token_places == spike_position[:, 1:2], spike_magnitude[:, 1:2], 0.0)
    return -(baseline_rate * coarse_values * block_multiplier + spike_list)


def set_ends(entries, rng, least, high):
    longest = entries.shape.index(max(entries.shape))
    spots = []
    for shift in (0, 1):
        where = [jax.random.randint(jax.random.fold_in(rng, axis), (), 0, length) for axis, length in enumerate(entries.shape)]
        where[longest] = (where[longest] + shift) % entries.shape[longest]
        spots.append(tuple(where))
    return entries.at[spots[0]].set(least).at[spots[1]].set(high)


def levels(rng, shape, cuts, low, high):
    gain = 1.0
    for axis_at, parts in cuts:
        steps = jax.random.uniform(jax.random.fold_in(jax.random.fold_in(rng, 6), axis_at), (parts,), jnp.float32, low / len(cuts), high / len(cuts))
        gain = gain * jnp.repeat(jnp.exp(steps), shape[axis_at] // parts).reshape((-1,) + (1,) * (len(shape) - 1 - axis_at))
    return gain


def bell_draw(stream_key, extent, scale, limit, pieces=(), kind=jnp.bfloat16):
    drawn = jax.random.normal(stream_key, extent, jnp.float32) * scale
    if len(pieces) > 0:
        drawn = levels(stream_key, extent, pieces, -0.22, 0.18) * drawn
    return jnp.clip(drawn, min=-limit, max=limit).astype(kind)


def setup_inputs(seed: int = 0) -> dict:
    splits = jax.random.split(jax.random.key(seed), 11)
    return {
        "packed_input": set_ends(jax.random.randint(splits[0], (TOKEN_NUMBER // 8, HP), -2147483648, 2147483647), jax.random.fold_in(splits[0], 1), -2147483648, 2147483646).astype(jnp.int32),
        "block_exponent": set_ends(jax.random.randint(splits[1], (HP // QBLOCK, TOKEN_NUMBER), -5, 0), jax.random.fold_in(splits[1], 1), -5, -1).astype(jnp.int32),
        "gate_input": draw_gate_input(jax.random.fold_in(splits[10], 71), 0),
        "state_write": bell_draw(splits[3], (TOKEN_NUMBER, N), 1.0, 6.0, ((0, 32),)),
        "state_read": bell_draw(splits[4], (TOKEN_NUMBER, N), 1.0, 6.0, ((0, 32),)),
        "log_decay": draw_log_decay(jax.random.fold_in(splits[10], 71), 0),
        "skip_weight": jnp.clip(jnp.exp(math.log(3.0) - 2.3025851 * jax.random.uniform(splits[6], (HEAD_NUMBER,), jnp.float32) ** levels(splits[6], (HEAD_NUMBER,), ((0, 8),), -0.2, 0.2)), 0.3, 3.0),
        "norm_gain": jnp.clip(1.0 + 0.1 * jax.random.normal(splits[7], (HP,), jnp.float32), 0.5, 1.5),
        "out_weight": bell_draw(splits[8], (HP, D), HP ** -0.5, 0.078125, ((0, 8),)),
        "out_cotangent": bell_draw(splits[9], (TOKEN_NUMBER, D), 1.0, 6.0, ((0, 32), (1, 8))),
    }


PRECISE = lax.Precision.HIGHEST

def dequantize(packed_words, exponents):
    shifts = 4 * jnp.arange(8, dtype=jnp.int32)
    fields = jnp.bitwise_and(jnp.right_shift(packed_words[:, None, :], shifts[None, :, None]), 15) - 8
    fields = fields.reshape(packed_words.shape[0] * 8, packed_words.shape[1])
    factors = jnp.exp2(exponents.astype(jnp.float32))
    group_width = fields.shape[1] // exponents.shape[0]
    factors = jnp.repeat(factors.T, group_width, axis=1)
    return (fields.astype(jnp.float32) * factors).astype(jnp.bfloat16)

def lower_decays(seg_sum):
    length = seg_sum.shape[1]
    is_lower = (jnp.arange(length)[:, None] >= jnp.arange(length)[None, :])[None]
    spread = seg_sum[:, :, None] - seg_sum[:, None, :]
    return jnp.where(is_lower, jnp.exp(jnp.where(is_lower, spread, 0.0)), 0.0)

def block_step(state_now, inputs):
    x_part, decay_part, write_part, read_part = inputs
    seg_sum = jnp.cumsum(decay_part, axis=1)
    mixing = lower_decays(seg_sum) * jnp.dot(read_part, write_part.T, precision=PRECISE)[None]
    carried_in = jnp.einsum('in,hpn->ihp', read_part, state_now, precision=PRECISE)
    result = jnp.einsum('hij,jhp->ihp', mixing, x_part, precision=PRECISE) + jnp.exp(seg_sum).T[:, :, None] * carried_in
    end_weight = jnp.exp(seg_sum[:, -1:] - seg_sum)
    state_next = jnp.exp(seg_sum[:, -1])[:, None, None] * state_now + jnp.einsum('jhp,jn->hpn', x_part * end_weight.T[:, :, None], write_part, precision=PRECISE)
    return (state_next, result)

def scan_states(x_heads, log_decay, write_rows, read_rows):
    total, head_count, head_width = x_heads.shape
    block_len = min(256, TOK_DEV)
    blocks = total // block_len
    x_blocks = x_heads.reshape(blocks, block_len, head_count, head_width)
    decay_blocks = log_decay.reshape(head_count, blocks, block_len).transpose(1, 0, 2)
    write_blocks = write_rows.reshape(blocks, block_len, -1)
    read_blocks = read_rows.reshape(blocks, block_len, -1)
    initial = jnp.zeros((head_count, head_width, write_rows.shape[1]), jnp.float32)
    _, outputs = lax.scan(jax.checkpoint(block_step), initial, (x_blocks, decay_blocks, write_blocks, read_blocks))
    return outputs.reshape(total, head_count, head_width)

def add_block(running, pair):
    part_sum = jnp.dot(pair[0].T, pair[1], preferred_element_type=jnp.float32)
    rounded = lax.optimization_barrier(part_sum.astype(jnp.bfloat16))
    return (running + rounded.astype(jnp.float32), None)

def reference(packed_input, block_exponent, gate_input, state_write, state_read, log_decay, skip_weight, norm_gain, out_weight, out_cotangent):
    x_values = dequantize(packed_input, block_exponent)
    total, width = x_values.shape
    head_count = log_decay.shape[0]
    x_heads = x_values.astype(jnp.float32).reshape(total, head_count, width // head_count)
    write_rows = state_write.astype(jnp.float32)
    read_rows = state_read.astype(jnp.float32)
    core, pullback = jax.vjp(scan_states, x_heads, log_decay, write_rows, read_rows)
    y_full = (core + skip_weight[None, :, None] * x_heads).reshape(total, width)
    gate = gate_input.astype(jnp.float32)
    sigma = jax.nn.sigmoid(gate)
    active = gate * sigma
    mixed = y_full * active
    scale_row = lax.rsqrt(lax.optimization_barrier(jnp.mean(mixed * mixed, axis=1, keepdims=True)) + 1e-05)
    normed = (mixed * scale_row * norm_gain).astype(jnp.bfloat16)
    grad_v = jnp.dot(out_cotangent, out_weight.T, preferred_element_type=jnp.float32)
    model_width = out_weight.shape[1]
    normed_blocks = normed.reshape(-1, TOK_DEV, width)
    cot_blocks = out_cotangent.reshape(-1, TOK_DEV, model_width)
    grad_out_weight, _ = lax.scan(add_block, jnp.zeros((width, model_width), jnp.float32), (normed_blocks, cot_blocks))
    scaled = grad_v * norm_gain
    grad_gain = lax.optimization_barrier(jnp.sum(grad_v * mixed * scale_row, axis=0))
    inner = lax.optimization_barrier(jnp.sum(scaled * mixed, axis=1, keepdims=True))
    grad_mixed = scale_row * scaled - mixed * (scale_row * scale_row * scale_row) * inner / width
    grad_gate = (grad_mixed * y_full * sigma * (1.0 + gate * (1.0 - sigma))).astype(jnp.bfloat16)
    grad_y = (grad_mixed * active).reshape(total, head_count, width // head_count)
    grad_skip = lax.optimization_barrier(jnp.sum(grad_y * x_heads, axis=(0, 2)))
    grad_core, grad_decay, grad_write, grad_read = pullback(grad_y)
    grad_input = (grad_core + skip_weight[None, :, None] * grad_y).reshape(total, width).astype(jnp.bfloat16)
    return (grad_input, grad_gate, grad_write, grad_read, grad_decay, grad_skip, grad_gain, grad_out_weight)
```

```python
import functools

import jax
import jax.numpy as jnp
from jax import lax
from jax.experimental import pallas as pl
from jax.experimental.pallas import tpu as pltpu
from jax.sharding import PartitionSpec as P

MESH = pl.DeviceIdType.MESH
F32, BF16 = jnp.float32, jnp.bfloat16
EXACT = lax.Precision.HIGHEST
NX = 4
L = 128
HEAD = 64
SLOT = 16


def dot(a, b, ca=1, cb=0, precision=None):
    return lax.dot_general(
        a, b, (((ca,), (cb,)), ((), ())), preferred_element_type=F32, precision=precision
    )


def iota(shape, dim):
    return lax.broadcasted_iota(jnp.int32, shape, dim)


def rcopy(src, dst, send, recv, dev):
    return pltpu.make_async_remote_copy(
        src_ref=src, dst_ref=dst, send_sem=send, recv_sem=recv, device_id=dev, device_id_type=MESH
    )


def core(nx, nz, ntp, packed, expo, gate_hbm, b_ref, c_ref, ld_ref, skip_ref, gain_ref, w_hbm, cot_hbm,
         gin, ggate, gwrite, gread, gdecay, gskip, ggain, gow, *scratch):
    (gate_v, w_v, cot_all, cot_full, xb, yb, gvb, mixb, dyb, rsb, endb, startb,
     csr, csc, totb, dec, cross, gb, stb, hcb, sumd, segr, segc, dxi,
     sloc, lb, tb, ub, qs, qb, vs, s_in,
     rloc, lb2, tb2, ub2, qs2, qb2, vs2, h_in,
     dxs, dzs, sums, gx, gz, pw, xr, zs, zr, accw, accr, red, redo,
     cp_sem, s_ag, r_ag, s_dx, r_dx, s_dz, r_dz,
     s_p1, r_p1, s_p2, r_p2, s_p3, r_p3, s_p4, r_p4,
     s_h1, r_h1, s_h2, r_h2, s_h3, r_h3, s_h4, r_h4,
     s_tp, r_tp, s_gx, r_gx, s_gz, r_gz, s_rx, r_rx, s_rz, r_rz,
     s_w1, r_w1, s_w2, r_w2, s_c1, r_c1, s_c2, r_c2) = scratch
    tokens, width = xb.shape
    chunks = tokens // L
    pairs = width // 128
    heads = width // HEAD
    total_width = width * ntp
    ny = ntp // 2
    qrows, erows = 128 // nx, 128 // (nx * nz)
    s = lax.axis_index("seq")
    t = lax.axis_index("tp")
    z, x = lax.div(s, nx), lax.rem(s, nx)
    y, half = lax.div(t, 2), lax.rem(t, 2)

    def dev_x(p):
        return {"seq": z * nx + p, "tp": t}

    def dev_z(p):
        return {"seq": p * nx + x, "tp": t}

    def dev_t(p):
        return {"seq": s, "tp": p}

    X, Z, TP = (nx, x, dev_x), (nz, z, dev_z), (ntp, t, dev_t)
    pending = []

    def send(group, src_of, dst, ssem, rsem):
        n, me, dev = group
        for d in range(1, n):
            p = lax.rem(me + d, n)
            copy = rcopy(src_of(p), dst, ssem.at[d], rsem.at[me], dev(p))
            copy.start()
            pending.append(copy)

    def arrive(group, dst_of, ssem, rsem):
        n, me, dev = group
        for d in range(1, n):
            p = lax.rem(me + d, n)
            rcopy(dst_of(p), dst_of(p), ssem.at[d], rsem.at[p], dev(p)).wait_recv()

    load_cot = pltpu.make_async_copy(cot_hbm, cot_all.at[t], cp_sem.at[0])
    load_gate = pltpu.make_async_copy(gate_hbm, gate_v, cp_sem.at[1])
    load_w = pltpu.make_async_copy(w_hbm, w_v, cp_sem.at[2])
    load_cot.start()
    load_gate.start()
    load_w.start()

    barrier = pltpu.get_barrier_semaphore()
    for n, me, dev in (X, Z, TP):
        for d in range(1, n):
            pl.semaphore_signal(
                barrier, inc=1, device_id=dev(lax.rem(me + d, n)), device_id_type=MESH
            )

    spread = (iota((SLOT, width), 1) // HEAD == iota((SLOT, width), 0)).astype(F32)
    gather = (iota((width, SLOT), 0) // HEAD == iota((width, SLOT), 1)).astype(F32)
    upper = (iota((L, L), 0) <= iota((L, L), 1)).astype(F32)
    lower = (iota((L, L), 0) <= iota((L, L), 1)).astype(F32)
    causal = iota((L, L), 0) >= iota((L, L), 1)
    left = iota((L, 128), 1) < HEAD

    csr[...] = jnp.zeros_like(csr)
    segr[...] = jnp.zeros_like(segr)
    log_total = jnp.zeros((1, SLOT), F32)
    for k in range(chunks):
        csr[k, 0:heads, :] = ld_ref[:, k * L : (k + 1) * L]
        rows = dot(csr[k], upper, precision=EXACT)
        csr[k] = rows
        cols = rows.T
        csc[k] = cols
        last = cols[L - 1 : L, :]
        log_total = log_total + last
        totb[k] = dot(jnp.broadcast_to(jnp.exp(last), (8, SLOT)), spread, precision=EXACT)[0:1]
        endb[k * L : (k + 1) * L, :] = dot(jnp.exp(last - cols), spread, precision=EXACT)
        startb[k * L : (k + 1) * L, :] = dot(jnp.exp(cols), spread, precision=EXACT)
    decay_all = dot(jnp.broadcast_to(jnp.exp(log_total), (8, SLOT)), spread, precision=EXACT)[0:1]
    dxs[x] = decay_all

    pl.semaphore_wait(barrier, (nx - 1) + (nz - 1) + (ntp - 1))
    send(X, lambda p: dxs.at[x], dxs.at[x], s_dx, r_dx)

    load_cot.wait()
    sibling = dev_t(2 * y + 1 - half)
    copy = rcopy(cot_all.at[t], cot_all.at[t], s_ag.at[ny], r_ag.at[t], sibling)
    copy.start()
    pending.append(copy)
    for d in range(1, ny):
        p = 2 * lax.rem(y + d, ny) + half
        copy = rcopy(cot_all.at[t], cot_all.at[t], s_ag.at[d], r_ag.at[t], dev_t(p))
        copy.start()
        pending.append(copy)

    def share_cot(d):
        p = 2 * lax.rem(y + d, ny) + half
        rcopy(cot_all.at[p], cot_all.at[p], s_ag.at[d], r_ag.at[p], dev_t(p)).wait_recv()
        copy = rcopy(cot_all.at[p], cot_all.at[p], s_ag.at[ny + d], r_ag.at[p], sibling)
        copy.start()
        pending.append(copy)

    def sibling_cot():
        for d in range(ny):
            p = 2 * lax.rem(y + d, ny) + 1 - half
            rcopy(cot_all.at[p], cot_all.at[p], s_ag.at[d], r_ag.at[p], sibling).wait_recv()

    powers = lax.shift_left(jnp.ones_like(expo[...]), expo[...] + 5).astype(F32) * (1.0 / 32.0)
    nibble = 4 * iota((8, width), 0)
    for k in range(chunks):
        factor_rows = jnp.concatenate(
            [powers[:, k * L : (k + 1) * L], jnp.zeros((8 - pairs, L), F32)], axis=0
        )
        factor = factor_rows.T
        wide = jnp.concatenate(
            [jnp.broadcast_to(factor[:, p : p + 1], (L, 128)) for p in range(pairs)], axis=1
        )
        words = packed[k * (L // 8) : (k + 1) * (L // 8), :]
        fields = jnp.concatenate(
            [
                lax.bitwise_and(
                    lax.shift_right_arithmetic(
                        jnp.broadcast_to(words[r : r + 1, :], (8, width)), nibble
                    ),
                    15,
                )
                - 8
                for r in range(L // 8)
            ],
            axis=0,
        )
        xb[k * L : (k + 1) * L, :] = (fields.astype(F32) * wide).astype(BF16)

    run = jnp.zeros((128, width), F32)
    for k in range(chunks):
        rows = slice(k * L, (k + 1) * L)
        weighted = (xb[rows, :].astype(F32) * endb[rows, :]).astype(BF16)
        gb[k] = dot(b_ref[rows, :], weighted, 0, 0)
        run = totb[k] * run + gb[k]
    sloc[...] = run

    def take_rows(ref, at, count):
        return ref[pl.ds(pl.multiple_of(at * count, count), count), :]

    def exchange_1(own, lbuf, ssem, rsem):
        send(
            X,
            lambda p: own.at[pl.ds(pl.multiple_of(p * qrows, qrows), qrows)],
            lbuf.at[x],
            ssem,
            rsem,
        )
        lbuf[x] = take_rows(own, x, qrows)

    def exchange_2(lbuf, tbuf, ubuf, s1, r1, ssem, rsem, backward):
        arrive(X, lambda p: lbuf.at[p], s1, r1)
        order = range(nx - 1, -1, -1) if backward else range(nx)
        row = None
        for k in order:
            row = lbuf[k] if row is None else dxs[k] * row + lbuf[k]
        for k in range(nz):
            tbuf[k] = row[k * erows : (k + 1) * erows, :]
        send(Z, lambda p: tbuf.at[p], ubuf.at[z], ssem, rsem)
        ubuf[z] = tbuf[z]

    def exchange_3(ubuf, qsend, qbuf, s2, r2, ssem, rsem, backward):
        arrive(Z, lambda p: ubuf.at[p], s2, r2)
        order = range(nz - 1, -1, -1) if backward else range(nz)
        row = jnp.zeros((erows, width), F32)
        for k in order:
            qsend[k] = row
            row = dzs[k] * row + ubuf[k]
        send(Z, lambda p: qsend.at[p], qbuf.at[z], ssem, rsem)
        qbuf[z] = qsend[z]

    def exchange_4(qbuf, lbuf, vsend, result, s3, r3, ssem, rsem, backward):
        arrive(Z, lambda p: qbuf.at[p], s3, r3)
        first = nx - 1 if backward else 0
        for k in range(nz):
            vsend[first, k * erows : (k + 1) * erows, :] = qbuf[k]
        order = range(nx - 1, -1, -1) if backward else range(nx)
        row = vsend[first]
        for k in order:
            if k != first:
                vsend[k] = row
            row = dxs[k] * row + lbuf[k]
        mine = result.at[pl.ds(pl.multiple_of(x * qrows, qrows), qrows)]
        send(X, lambda p: vsend.at[p], mine, ssem, rsem)
        result[pl.ds(pl.multiple_of(x * qrows, qrows), qrows), :] = vsend[x]

    def exchange_5(result, s4, r4):
        arrive(X, lambda p: result.at[pl.ds(pl.multiple_of(p * qrows, qrows), qrows)], s4, r4)

    exchange_1(sloc, lb, s_p1, r_p1)

    arrive(X, lambda p: dxs.at[p], s_dx, r_dx)
    row = dxs[0]
    for k in range(1, nx):
        row = row * dxs[k]
    dzs[z] = row
    send(Z, lambda p: dzs.at[z], dzs.at[z], s_dz, r_dz)

    skip_row = dot(
        jnp.concatenate(
            [jnp.broadcast_to(skip_ref[...], (8, heads)), jnp.zeros((8, SLOT - heads), F32)], axis=1
        ),
        spread,
        precision=EXACT,
    )[0:1]

    def at_chunk(k):
        return pl.ds(pl.multiple_of(k * L, L), L)

    def split_pair(v):
        zero = jnp.zeros_like(v)
        return jnp.concatenate([jnp.where(left, v, zero), jnp.where(left, zero, v)], axis=0)

    def inside(k, _):
        rows = at_chunk(k)
        both = dot(c_ref[rows, :], b_ref[rows, :], 1, 1)
        cross[k] = both
        for p in range(pairs):
            mixing = []
            for h in (2 * p, 2 * p + 1):
                spread_log = csc[k][:, h : h + 1] - csr[k][h : h + 1, :]
                decay = jnp.where(causal, jnp.exp(jnp.minimum(spread_log, 0.0)), 0.0)
                dec[k, h] = decay
                mixing.append((decay * both).astype(BF16))
            lanes = slice(128 * p, 128 * (p + 1))
            x_pair = xb[rows, lanes]
            yb[rows, lanes] = (
                dot(jnp.concatenate(mixing, axis=1), split_pair(x_pair))
                + skip_row[:, lanes] * x_pair.astype(F32)
            )
        return 0

    lax.fori_loop(0, chunks // 2, inside, 0)
    exchange_2(lb, tb, ub, s_p1, r_p1, s_p2, r_p2, False)
    lax.fori_loop(chunks // 2, chunks, inside, 0)
    arrive(Z, lambda p: dzs.at[p], s_dz, r_dz)
    exchange_3(ub, qs, qb, s_p2, r_p2, s_p3, r_p3, False)
    exchange_4(qb, lb, vs, s_in, s_p3, r_p3, s_p4, r_p4, False)
    for d in range(1, ny):
        share_cot(d)
    sibling_cot()
    shard = cot_all.shape[2]
    for p in range(ntp):
        cot_full[:, p * shard : (p + 1) * shard] = cot_all[p]
    load_w.wait()

    def project(k, _):
        rows = at_chunk(k)
        gvb[rows, :] = dot(cot_full[rows, :], w_v[...], 1, 1)
        return 0

    lax.fori_loop(0, chunks, project, 0)
    load_gate.wait()
    exchange_5(s_in, s_p4, r_p4)

    gain_row = gain_ref[...]
    stb[0] = s_in[...]
    for k in range(1, chunks):
        stb[k] = totb[k - 1] * stb[k - 1] + gb[k - 1]

    def outputs_of(k, _):
        rows = at_chunk(k)
        start = dot(c_ref[rows, :], stb[k].astype(BF16))
        rsb[rows, :] = start
        y_now = yb[rows, :] + startb[rows, :] * start
        yb[rows, :] = y_now
        gate = gate_v[rows, :].astype(F32)
        mixed = y_now * gate * jax.nn.sigmoid(gate)
        mixb[rows, :] = mixed
        square = jnp.sum(mixed * mixed, axis=1, keepdims=True)
        inner = jnp.sum(gvb[rows, :] * gain_row * mixed, axis=1, keepdims=True)
        lane = iota((L, 128), 1)
        packed_sums = jnp.where(lane == 0, square, jnp.where(lane == 1, inner, 0.0))
        sums[t, k] = packed_sums.T[0:8, :]
        return 0

    lax.fori_loop(0, chunks, outputs_of, 0)
    send(TP, lambda p: sums.at[t], sums.at[t], s_tp, r_tp)
    arrive(TP, lambda p: sums.at[p], s_tp, r_tp)

    def gradients(k, carry):
        gain_sum, skip_sum = carry
        rows = at_chunk(k)
        both = sums[0, k]
        for p in range(1, ntp):
            both = both + sums[p, k]
        both = jnp.concatenate([both, jnp.zeros((120, L), F32)], axis=0).T
        scale = lax.rsqrt(both[:, 0:1] / total_width + 1e-05)
        inner = both[:, 1:2]
        mixed = mixb[rows, :]
        grad_v = gvb[rows, :]
        gate = gate_v[rows, :].astype(F32)
        sigma = jax.nn.sigmoid(gate)
        grad_mixed = scale * (grad_v * gain_row) - mixed * (
            (scale * scale * scale) * inner / total_width
        )
        ggate[rows, :] = (
            grad_mixed * yb[rows, :] * sigma * (1.0 + gate * (1.0 - sigma))
        ).astype(BF16)
        grad_y = grad_mixed * gate * sigma
        dyb[rows, :] = grad_y
        gain_sum = gain_sum + jnp.sum(grad_v * mixed * scale, axis=0, keepdims=True)
        skip_sum = skip_sum + jnp.sum(
            grad_y * xb[rows, :].astype(F32), axis=0, keepdims=True
        )
        hcb[k] = dot(c_ref[rows, :], (grad_y * startb[rows, :]).astype(BF16), 0, 0)
        mixb[rows, :] = mixed * scale * gain_row
        return gain_sum, skip_sum

    zero_row = jnp.zeros((1, width), F32)
    gain_sum, skip_sum = lax.fori_loop(0, chunks, gradients, (zero_row, zero_row))
    run = hcb[chunks - 1]
    for k in range(chunks - 2, -1, -1):
        run = totb[k] * run + hcb[k]
    rloc[...] = run
    exchange_1(rloc, lb2, s_h1, r_h1)
    gx[x, 0:1, :] = gain_sum
    gx[x, 1:2, :] = skip_sum
    send(X, lambda p: gx.at[x], gx.at[x], s_gx, r_gx)

    columns = shard // nx

    def weight_block(k):
        normed = mixb[...].astype(BF16)
        pw[k] = dot(cot_all[k], normed, 0, 0).astype(BF16)
        for d in range(1, nx):
            p = lax.rem(x + d, nx)
            copy = rcopy(
                pw.at[k, pl.ds(pl.multiple_of(p * columns, columns), columns)],
                xr.at[x, k],
                s_rx.at[d, k],
                r_rx.at[x, k],
                dev_x(p),
            )
            copy.start()
            pending.append(copy)

    def weight_rows(k):
        out = pw[k, pl.ds(pl.multiple_of(x * columns, columns), columns), :].astype(F32)
        for d in range(1, nx):
            p = lax.rem(x + d, nx)
            rcopy(xr.at[p, k], xr.at[p, k], s_rx.at[d, k], r_rx.at[p, k], dev_x(p)).wait_recv()
            out = out + xr[p, k].astype(F32)
        zs[k] = out.astype(BF16)

        @pl.when(z != k)
        def _():
            rcopy(zs.at[k], zr.at[z], s_rz.at[k], r_rz.at[z], dev_z(k)).start()

    first_blocks = nz // 2
    for k in range(first_blocks):
        weight_block(k)
    exchange_2(lb2, tb2, ub2, s_h1, r_h1, s_h2, r_h2, True)
    arrive(X, lambda p: gx.at[p], s_gx, r_gx)
    row = gx[0]
    for k in range(1, nx):
        row = row + gx[k]
    gz[z] = row
    send(Z, lambda p: gz.at[z], gz.at[z], s_gz, r_gz)

    def inside_back(k, _):
        rows = at_chunk(k)
        both = cross[k]
        summed = jnp.zeros((L, L), F32)
        lane = iota((L, SLOT), 1)
        row_sums = jnp.zeros((L, SLOT), F32)
        for p in range(pairs):
            lanes = slice(128 * p, 128 * (p + 1))
            x_pair = xb[rows, lanes]
            grads = split_pair(dyb[rows, lanes].astype(BF16))
            dots = dot(grads, x_pair, 1, 1)
            mixing = []
            for i in range(2):
                h = 2 * p + i
                decay = dec[k, h]
                weighted = dots[i * L : (i + 1) * L, :] * decay
                summed = summed + weighted
                terms = weighted * both
                row_sums = row_sums + jnp.where(
                    lane == h, jnp.sum(terms, axis=1, keepdims=True), 0.0
                )
                segr[k, h : h + 1, :] = jnp.sum(terms, axis=0, keepdims=True)
                mixing.append((decay * both).astype(BF16))
            dxi[rows, lanes] = dot(jnp.concatenate(mixing, axis=0), grads, 0, 0)
        sumd[k] = summed
        segc[k] = row_sums - segr[k].T
        scaled = dyb[rows, :] * startb[rows, :]
        accr[rows, :] = dot(summed.astype(BF16), b_ref[rows, :]) + dot(
            scaled.astype(BF16), stb[k].astype(BF16), 1, 1
        )
        return 0

    lax.fori_loop(0, chunks // 2, inside_back, 0)
    exchange_3(ub2, qs2, qb2, s_h2, r_h2, s_h3, r_h3, True)
    lax.fori_loop(chunks // 2, chunks, inside_back, 0)
    exchange_4(qb2, lb2, vs2, h_in, s_h3, r_h3, s_h4, r_h4, True)

    share = tokens // ntp

    def reduce_1(acc, which, ssem, rsem):
        send(
            TP,
            lambda p: acc.at[pl.ds(pl.multiple_of(p * share, share), share)],
            red.at[which, t],
            ssem,
            rsem,
        )
        red[which, t] = take_rows(acc, t, share)

    def reduce_2(which, s1, r1, ssem, rsem):
        arrive(TP, lambda p: red.at[which, p], s1, r1)
        out = red[which, 0]
        for p in range(1, ntp):
            out = out + red[which, p]
        redo[which, t] = out
        send(TP, lambda p: redo.at[which, t], redo.at[which, t], ssem, rsem)

    def reduce_3(out_ref, which, ssem, rsem):
        arrive(TP, lambda p: redo.at[which, p], ssem, rsem)
        for p in range(ntp):
            out_ref[p * share : (p + 1) * share, :] = redo[which, p]

    reduce_1(accr, 0, s_c1, r_c1)
    for k in range(first_blocks, nz):
        weight_block(k)
    for k in range(first_blocks):
        weight_rows(k)
    exchange_5(h_in, s_h4, r_h4)

    def finish(i, run):
        k = chunks - 1 - i
        rows = at_chunk(k)
        h_low = run.astype(BF16)
        end = endb[rows, :]
        grad_y = dyb[rows, :]
        x_now = xb[rows, :].astype(F32)
        write = end * dot(b_ref[rows, :], h_low)
        gin[rows, :] = (skip_row * grad_y + dxi[rows, :] + write).astype(BF16)
        accw[rows, :] = dot(sumd[k].astype(BF16), c_ref[rows, :], 0, 0) + dot(
            (x_now * end).astype(BF16), h_low, 1, 1
        )
        leaving = dot(x_now * write, gather, precision=EXACT)
        arriving = dot(grad_y * startb[rows, :] * rsb[rows, :], gather, precision=EXACT)
        seg = segc[k] + arriving - leaving
        across = totb[k] * jnp.sum(run * stb[k], axis=0, keepdims=True)
        final = jnp.sum(leaving, axis=0, keepdims=True) + dot(
            jnp.broadcast_to(across, (8, width)), gather, precision=EXACT
        )[0:1]
        whole = dot(lower, seg, precision=EXACT) + final
        sumd[k, 0:SLOT, :] = whole.T
        return totb[k] * run + hcb[k]

    lax.fori_loop(0, chunks, finish, h_in[...])
    reduce_1(accw, 1, s_w1, r_w1)
    for k in range(chunks):
        gdecay[:, k * L : (k + 1) * L] = sumd[k, 0:heads, :]
    reduce_2(0, s_c1, r_c1, s_c2, r_c2)
    arrive(Z, lambda p: gz.at[p], s_gz, r_gz)
    row = gz[0]
    for k in range(1, nz):
        row = row + gz[k]
    ggain[...] = row[0:1]
    gskip[...] = dot(row, gather, precision=EXACT)[1:2, 0:heads]
    reduce_2(1, s_w1, r_w1, s_w2, r_w2)
    reduce_3(gread, 0, s_c2, r_c2)
    for k in range(first_blocks, nz):
        weight_rows(k)
    reduce_3(gwrite, 1, s_w2, r_w2)
    zr[z] = zs[z]
    arrive(Z, lambda p: zr.at[p], s_rz, r_rz)
    out = zr[0].astype(F32)
    for k in range(1, nz):
        out = out + zr[k].astype(F32)
    gow[...] = out.T
    for copy in pending:
        copy.wait_send()
    for k in range(nz):

        @pl.when(z != k)
        def _():
            rcopy(zs.at[k], zr.at[z], s_rz.at[k], r_rz.at[z], dev_z(k)).wait_send()


def on_device(nx, nz, ntp, packed, expo, gate, write, read, decay, skip, gain, weight, cot):
    tokens, width = gate.shape
    heads = decay.shape[0]
    model = weight.shape[1]
    shard = cot.shape[1]
    chunks = tokens // L
    n = write.shape[1]
    columns = model // (nx * nz)
    qrows, erows = n // nx, n // (nx * nz)
    ny = ntp // 2
    share = tokens // ntp

    def wide(kind=F32):
        return pltpu.VMEM((tokens, width), kind)

    def exchange():
        return [
            pltpu.VMEM((n, width), F32),
            pltpu.VMEM((nx, qrows, width), F32),
            pltpu.VMEM((nz, erows, width), F32),
            pltpu.VMEM((nz, erows, width), F32),
            pltpu.VMEM((nz, erows, width), F32),
            pltpu.VMEM((nz, erows, width), F32),
            pltpu.VMEM((nx, qrows, width), F32),
            pltpu.VMEM((n, width), F32),
        ]

    def sems(*shape):
        return [pltpu.SemaphoreType.DMA(shape), pltpu.SemaphoreType.DMA(shape)]

    scratch = [
        pltpu.VMEM((tokens, width), BF16),
        pltpu.VMEM((width, model), BF16),
        pltpu.VMEM((ntp, tokens, shard), BF16),
        pltpu.VMEM((tokens, model), BF16),
        wide(BF16),
        *[wide() for _ in range(7)],
        pltpu.VMEM((chunks, SLOT, L), F32),
        pltpu.VMEM((chunks, L, SLOT), F32),
        pltpu.VMEM((chunks, 1, width), F32),
        pltpu.VMEM((chunks, heads, L, L), F32),
        pltpu.VMEM((chunks, L, L), F32),
        pltpu.VMEM((chunks, n, width), F32),
        pltpu.VMEM((chunks, n, width), F32),
        pltpu.VMEM((chunks, n, width), F32),
        pltpu.VMEM((chunks, L, L), F32),
        pltpu.VMEM((chunks, SLOT, L), F32),
        pltpu.VMEM((chunks, L, SLOT), F32),
        wide(),
        *exchange(),
        *exchange(),
        pltpu.VMEM((nx, 1, width), F32),
        pltpu.VMEM((nz, 1, width), F32),
        pltpu.VMEM((ntp, chunks, 8, L), F32),
        pltpu.VMEM((nx, 2, width), F32),
        pltpu.VMEM((nz, 2, width), F32),
        pltpu.VMEM((nz, shard, width), BF16),
        pltpu.VMEM((nx, nz, columns, width), BF16),
        pltpu.VMEM((nz, columns, width), BF16),
        pltpu.VMEM((nz, columns, width), BF16),
        pltpu.VMEM((tokens, n), F32),
        pltpu.VMEM((tokens, n), F32),
        pltpu.VMEM((2, ntp, share, n), F32),
        pltpu.VMEM((2, ntp, share, n), F32),
        pltpu.SemaphoreType.DMA((3,)),
        pltpu.SemaphoreType.DMA((2 * ny,)),
        pltpu.SemaphoreType.DMA((ntp,)),
        *sems(nx),
        *sems(nz),
        *(sems(nx) + sems(nz) + sems(nz) + sems(nx)),
        *(sems(nx) + sems(nz) + sems(nz) + sems(nx)),
        *sems(ntp),
        *sems(nx),
        *sems(nz),
        *sems(nx, nz),
        *sems(nz),
        *(sems(ntp) * 4),
    ]
    vmem = pl.BlockSpec(memory_space=pltpu.VMEM)
    hbm = pl.BlockSpec(memory_space=pl.ANY)
    outs = pl.pallas_call(
        functools.partial(core, nx, nz, ntp),
        out_shape=(
            jax.ShapeDtypeStruct((tokens, width), BF16),
            jax.ShapeDtypeStruct((tokens, width), BF16),
            jax.ShapeDtypeStruct((tokens, n), F32),
            jax.ShapeDtypeStruct((tokens, n), F32),
            jax.ShapeDtypeStruct((heads, tokens), F32),
            jax.ShapeDtypeStruct((1, heads), F32),
            jax.ShapeDtypeStruct((1, width), F32),
            jax.ShapeDtypeStruct((width, columns), F32),
        ),
        in_specs=[vmem, vmem, hbm, vmem, vmem, vmem, vmem, vmem, hbm, hbm],
        out_specs=(vmem,) * 8,
        scratch_shapes=scratch,
        compiler_params=pltpu.CompilerParams(
            collective_id=0, has_side_effects=True, vmem_limit_bytes=60 * 1024 * 1024
        ),
        name="layer_backward",
    )(packed, expo, gate, write, read, decay, skip[None, :], gain[None, :], weight, cot)
    return (*outs[:5], outs[5][0], outs[6][0], outs[7])


def solution(mesh):
    ntp = mesh.shape["tp"]
    nz = mesh.shape["seq"] // NX
    return jax.shard_map(
        functools.partial(on_device, NX, nz, ntp),
        mesh=mesh,
        in_specs=(
            P("seq", "tp"),
            P("tp", "seq"),
            P("seq", "tp"),
            P("seq", None),
            P("seq", None),
            P("tp", "seq"),
            P("tp"),
            P("tp"),
            P("tp", None),
            P("seq", "tp"),
        ),
        out_specs=(
            P("seq", "tp"),
            P("seq", "tp"),
            P("seq", None),
            P("seq", None),
            P("tp", "seq"),
            P("tp"),
            P("tp"),
            P("tp", "seq"),
        ),
        check_vma=False,
    )
```

```python
import functools

import jax
import jax.numpy as jnp
from jax import lax
from jax.experimental import pallas as pl
from jax.experimental.pallas import tpu as pltpu
from jax.sharding import PartitionSpec as P

MESH = pl.DeviceIdType.MESH
F32, BF16 = jnp.float32, jnp.bfloat16
EXACT = lax.Precision.HIGHEST
NX = 4
L = 128
HEAD = 64
SLOT = 16


def dot(a, b, ca=1, cb=0, precision=None):
    return lax.dot_general(
        a, b, (((ca,), (cb,)), ((), ())), preferred_element_type=F32, precision=precision
    )


def pieces(v, count):
    out = []
    for _ in range(count):
        part = v.astype(BF16)
        out.append(part)
        v = v - part.astype(F32)
    return out


def iota(shape, dim):
    return lax.broadcasted_iota(jnp.int32, shape, dim)


def rcopy(src, dst, send, recv, dev):
    return pltpu.make_async_remote_copy(
        src_ref=src, dst_ref=dst, send_sem=send, recv_sem=recv, device_id=dev, device_id_type=MESH
    )


def core(nx, nz, ntp, packed, expo, gate_hbm, b_ref, c_ref, ld_ref, skip_ref, gain_ref, w_hbm, cot_hbm,
         gin, ggate, gwrite, gread, gdecay, gskip, ggain, gow, *scratch):
    (gate_v, w_v, cot, xb, yb, gvb, mixb, dyb, rsb, endb, startb,
     normed, csr, csc, totb, dec, cross, gb, stb, hcb, hst, sumd, segr, segc, dxi,
     sloc, lb, tb, ub, qs, qb, vs, s_in,
     rloc, lb2, tb2, ub2, qs2, qb2, vs2, h_in,
     vtop, dxs, dzs, sums, gx, gz, pw, xa, xd, xm, xc, zs, zr, accw, accr, red, redo,
     cp_sem, s_ag, r_ag, s_dx, r_dx, s_dz, r_dz,
     s_p1, r_p1, s_p2, r_p2, s_p3, r_p3, s_p4, r_p4,
     s_h1, r_h1, s_h2, r_h2, s_h3, r_h3, s_h4, r_h4,
     s_tp, r_tp, s_gx, r_gx, s_gz, r_gz, s_rx, r_rx, s_rz, r_rz,
     s_w1, r_w1, s_w2, r_w2, s_c1, r_c1, s_c2, r_c2) = scratch
    tokens, width = xb.shape
    chunks = tokens // L
    pairs = width // 128
    heads = width // HEAD
    total_width = width * ntp
    ny = ntp // 2
    qrows, erows = 128 // nx, 128 // (nx * nz)
    s = lax.axis_index("seq")
    t = lax.axis_index("tp")
    z, x = lax.div(s, nx), lax.rem(s, nx)
    y, half = lax.div(t, 2), lax.rem(t, 2)
    shard = cot.shape[0] // ntp

    def dev_x(p):
        return {"seq": z * nx + p, "tp": t}

    def dev_z(p):
        return {"seq": p * nx + x, "tp": t}

    def dev_t(p):
        return {"seq": s, "tp": p}

    X, Z, TP = (nx, x, dev_x), (nz, z, dev_z), (ntp, t, dev_t)
    pending = []

    def send(group, src_of, dst, ssem, rsem):
        n, me, dev = group
        for d in range(1, n):
            p = lax.rem(me + d, n)
            copy = rcopy(src_of(p), dst, ssem.at[d], rsem.at[me], dev(p))
            copy.start()
            pending.append(copy)

    def arrive(group, dst_of, ssem, rsem):
        n, me, dev = group
        for d in range(1, n):
            p = lax.rem(me + d, n)
            rcopy(dst_of(p), dst_of(p), ssem.at[d], rsem.at[p], dev(p)).wait_recv()

    def cot_rows(p, first=0, count=shard):
        return cot.at[pl.ds(pl.multiple_of(p * shard + first, 16), count)]

    load_cot = pltpu.make_async_copy(cot_hbm, cot_rows(t), cp_sem.at[0])
    load_gate = pltpu.make_async_copy(gate_hbm, gate_v, cp_sem.at[1])
    load_w = pltpu.make_async_copy(w_hbm, w_v, cp_sem.at[2])
    load_cot.start()
    load_gate.start()
    load_w.start()

    barrier = pltpu.get_barrier_semaphore()
    for n, me, dev in (X, Z, TP):
        for d in range(1, n):
            pl.semaphore_signal(
                barrier, inc=1, device_id=dev(lax.rem(me + d, n)), device_id_type=MESH
            )

    spread = (iota((SLOT, width), 1) // HEAD == iota((SLOT, width), 0)).astype(BF16)
    gather = (iota((width, SLOT), 0) // HEAD == iota((width, SLOT), 1)).astype(BF16)
    upper = (iota((L, L), 0) <= iota((L, L), 1)).astype(BF16)
    causal = iota((L, L), 0) >= iota((L, L), 1)
    left = iota((L, 128), 1) < HEAD

    def spread_heads(v):
        return sum(dot(part, spread) for part in pieces(v, 3))

    def head_sums(v):
        return sum(dot(part, gather) for part in pieces(v, 2))

    csr[...] = jnp.zeros_like(csr)
    segr[...] = jnp.zeros_like(segr)
    for k in range(chunks):
        csr[k, 0:heads, :] = ld_ref[:, k * L : (k + 1) * L]
    rows = csr[...].reshape(chunks * SLOT, L)
    rows = sum(dot(part, upper) for part in pieces(rows, 3))
    log_total = jnp.zeros((1, width), F32)
    for k in range(chunks):
        csr[k] = rows[k * SLOT : (k + 1) * SLOT, :]
        cols = rows[k * SLOT : (k + 1) * SLOT, :].T
        csc[k] = cols
        logs = spread_heads(cols)
        last = logs[L - 1 : L, :]
        log_total = log_total + last
        totb[k] = jnp.exp(last)
        endb[k * L : (k + 1) * L, :] = jnp.exp(last - logs)
        startb[k * L : (k + 1) * L, :] = jnp.exp(logs)
    dxs[x] = jnp.exp(log_total)

    pl.semaphore_wait(barrier, (nx - 1) + (nz - 1) + (ntp - 1))
    send(X, lambda p: dxs.at[x], dxs.at[x], s_dx, r_dx)

    load_cot.wait()
    part = shard // 2
    sibling = 2 * y + 1 - half
    after = 2 * lax.rem(y + 1, ny) + half
    before = 2 * lax.rem(y + ny - 1, ny) + half
    across = 2 * lax.rem(y + 2, ny) + half

    def cot_copy(i, j, p, to, first=0, count=shard):
        return rcopy(cot_rows(p, first, count), cot_rows(p, first, count), s_ag.at[i], r_ag.at[j], dev_t(to))

    def cot_send(i, j, p, to, *rows):
        copy = cot_copy(i, j, p, to, *rows)
        copy.start()
        pending.append(copy)

    def cot_wait(j, p, *rows):
        cot_copy(0, j, p, sibling, *rows).wait_recv()

    cot_send(0, 0, t, sibling)
    if ny == 2:
        cot_send(1, 1, t, after)
    elif ny == 4:
        cot_send(1, 1, t, after, 0, part)
        cot_send(2, 3, t, before, part, part)
        cot_send(3, 2, t, after, part, part)
        cot_send(4, 4, t, before, 0, part)

    def relay_cot():
        if ny == 4:
            cot_wait(1, before, 0, part)
            cot_send(5, 5, before, after, 0, part)
            cot_wait(3, after, part, part)
            cot_send(6, 6, after, before, part, part)

    def near_cot():
        if ny == 2:
            cot_wait(1, after)
            cot_send(2, 7, after, sibling)
        elif ny == 4:
            cot_wait(2, before, part, part)
            cot_send(7, 7, before, sibling)
            cot_wait(4, after, 0, part)
            cot_send(8, 8, after, sibling)

    def far_cot():
        if ny == 4:
            cot_wait(5, across, 0, part)
            cot_wait(6, across, part, part)
            cot_send(9, 9, across, sibling)

    def project(chip, first=False):
        terms = dot(
            cot[pl.ds(pl.multiple_of(chip * 2 * shard, 128), 2 * shard), :],
            w_v[:, pl.ds(pl.multiple_of(chip * 2 * shard, 128), 2 * shard)],
            0,
            1,
        )
        gvb[...] = terms if first else gvb[...] + terms

    def other(p):
        return p + 1 - 2 * half

    powers = lax.shift_left(jnp.ones_like(expo[...]), expo[...] + 5).astype(F32) * (1.0 / 32.0)
    nibble = 4 * iota((8, width), 0)
    for k in range(chunks):
        factor_rows = jnp.concatenate(
            [powers[:, k * L : (k + 1) * L], jnp.zeros((8 - pairs, L), F32)], axis=0
        )
        factor = factor_rows.T
        wide = jnp.concatenate(
            [jnp.broadcast_to(factor[:, p : p + 1], (L, 128)) for p in range(pairs)], axis=1
        )
        words = packed[k * (L // 8) : (k + 1) * (L // 8), :]
        fields = jnp.concatenate(
            [
                lax.bitwise_and(
                    lax.shift_right_arithmetic(
                        jnp.broadcast_to(words[r : r + 1, :], (8, width)), nibble
                    ),
                    15,
                )
                - 8
                for r in range(L // 8)
            ],
            axis=0,
        )
        xb[k * L : (k + 1) * L, :] = (fields.astype(F32) * wide).astype(BF16)

    run = jnp.zeros((128, width), F32)
    for k in range(chunks):
        rows = slice(k * L, (k + 1) * L)
        weighted = xb[rows, :].astype(F32) * endb[rows, :]
        gb[k] = sum(dot(b_ref[rows, :], part, 0, 0) for part in pieces(weighted, 2))
        run = totb[k] * run + gb[k]
    sloc[...] = run

    def take_rows(ref, at, count):
        return ref[pl.ds(pl.multiple_of(at * count, count), count), :]

    def exchange_1(own, lbuf, ssem, rsem):
        send(
            X,
            lambda p: own.at[pl.ds(pl.multiple_of(p * qrows, qrows), qrows)],
            lbuf.at[x],
            ssem,
            rsem,
        )
        lbuf[x] = take_rows(own, x, qrows)

    def exchange_2(lbuf, tbuf, ubuf, s1, r1, ssem, rsem, backward):
        arrive(X, lambda p: lbuf.at[p], s1, r1)
        order = range(nx - 1, -1, -1) if backward else range(nx)
        row = None
        for k in order:
            add = lbuf[k].astype(F32)
            row = add if row is None else dxs[k] * row + add
        for k in range(nz):
            tbuf[k] = row[k * erows : (k + 1) * erows, :]
        send(Z, lambda p: tbuf.at[p], ubuf.at[z], ssem, rsem)
        ubuf[z] = tbuf[z]

    def exchange_3(ubuf, qsend, qbuf, s2, r2, ssem, rsem, backward):
        arrive(Z, lambda p: ubuf.at[p], s2, r2)
        order = range(nz - 1, -1, -1) if backward else range(nz)
        row = jnp.zeros((erows, width), F32)
        for k in order:
            qsend[k] = row
            row = dzs[k] * row + ubuf[k]
        send(Z, lambda p: qsend.at[p], qbuf.at[z], ssem, rsem)
        qbuf[z] = qsend[z]

    def exchange_4(qbuf, lbuf, vsend, result, s3, r3, ssem, rsem, backward):
        arrive(Z, lambda p: qbuf.at[p], s3, r3)
        for k in range(nz):
            vtop[k * erows : (k + 1) * erows, :] = qbuf[k]
        order = range(nx - 1, -1, -1) if backward else range(nx)
        row = vtop[...]
        for k in order:
            vsend[k] = row.astype(vsend.dtype)
            row = dxs[k] * row + lbuf[k].astype(F32)
        mine = result.at[pl.ds(pl.multiple_of(x * qrows, qrows), qrows)]
        send(X, lambda p: vsend.at[p], mine, ssem, rsem)
        result[pl.ds(pl.multiple_of(x * qrows, qrows), qrows), :] = vsend[x]

    def exchange_5(result, s4, r4):
        arrive(X, lambda p: result.at[pl.ds(pl.multiple_of(p * qrows, qrows), qrows)], s4, r4)

    exchange_1(sloc, lb, s_p1, r_p1)

    arrive(X, lambda p: dxs.at[p], s_dx, r_dx)
    row = dxs[0]
    for k in range(1, nx):
        row = row * dxs[k]
    dzs[z] = row
    send(Z, lambda p: dzs.at[z], dzs.at[z], s_dz, r_dz)

    skip_row = jnp.zeros((1, width), F32)
    head_of = iota((1, width), 1) // HEAD
    for h in range(heads):
        skip_row = jnp.where(head_of == h, skip_ref[0, h], skip_row)

    def at_chunk(k):
        return pl.ds(pl.multiple_of(k * L, L), L)

    def split_pair(v):
        zero = jnp.zeros_like(v)
        return jnp.concatenate([jnp.where(left, v, zero), jnp.where(left, zero, v)], axis=0)

    def inside(k, _):
        rows = at_chunk(k)
        both = dot(c_ref[rows, :], b_ref[rows, :], 1, 1)
        cross[k] = both
        for p in range(pairs):
            mixing = []
            for h in (2 * p, 2 * p + 1):
                spread_log = csc[k][:, h : h + 1] - csr[k][h : h + 1, :]
                decay = jnp.where(causal, jnp.exp(jnp.minimum(spread_log, 0.0)), 0.0)
                dec[k, h] = decay
                mixing.append(pieces(decay * both, 2))
            lanes = slice(128 * p, 128 * (p + 1))
            x_pair = xb[rows, lanes]
            x_split = split_pair(x_pair)
            yb[rows, lanes] = (
                dot(jnp.concatenate([m[0] for m in mixing], axis=1), x_split)
                + dot(jnp.concatenate([m[1] for m in mixing], axis=1), x_split)
                + skip_row[:, lanes] * x_pair.astype(F32)
            )
        return 0

    lax.fori_loop(0, chunks // 2, inside, 0)
    load_w.wait()
    cot_wait(0, sibling)
    project(y, True)
    exchange_2(lb, tb, ub, s_p1, r_p1, s_p2, r_p2, False)
    relay_cot()
    lax.fori_loop(chunks // 2, chunks, inside, 0)
    arrive(Z, lambda p: dzs.at[p], s_dz, r_dz)
    exchange_3(ub, qs, qb, s_p2, r_p2, s_p3, r_p3, False)
    near_cot()
    exchange_4(qb, lb, vs, s_in, s_p3, r_p3, s_p4, r_p4, False)
    if ny == 2:
        cot_wait(7, other(after))
        project(lax.rem(y + 1, ny))
    elif ny == 4:
        cot_wait(7, other(before))
        project(lax.rem(y + 3, ny))
        cot_wait(8, other(after))
        project(lax.rem(y + 1, ny))
    far_cot()
    load_gate.wait()
    exchange_5(s_in, s_p4, r_p4)
    gain_row = gain_ref[...].reshape(1, width)
    stb[0] = s_in[...].astype(F32)
    for k in range(1, chunks):
        stb[k] = totb[k - 1] * stb[k - 1] + gb[k - 1]

    def outputs_of(k, _):
        rows = at_chunk(k)
        start = sum(dot(c_ref[rows, :], part) for part in pieces(stb[k], 2))
        rsb[rows, :] = start
        y_now = yb[rows, :] + startb[rows, :] * start
        yb[rows, :] = y_now
        gate = gate_v[rows, :].astype(F32)
        mixed = y_now * gate * jax.nn.sigmoid(gate)
        mixb[rows, :] = mixed
        return 0

    lax.fori_loop(0, chunks, outputs_of, 0)
    if ny == 4:
        cot_wait(9, other(across))
        project(lax.rem(y + 2, ny))

    def sums_of(k, _):
        rows = at_chunk(k)
        mixed = mixb[rows, :]
        square = jnp.sum(mixed * mixed, axis=1, keepdims=True)
        inner = jnp.sum(gvb[rows, :] * gain_row * mixed, axis=1, keepdims=True)
        lane = iota((L, 128), 1)
        packed_sums = jnp.where(lane == 0, square, jnp.where(lane == 1, inner, 0.0))
        sums[t, k] = packed_sums.T[0:8, :]
        return 0

    lax.fori_loop(0, chunks, sums_of, 0)
    send(TP, lambda p: sums.at[t], sums.at[t], s_tp, r_tp)
    arrive(TP, lambda p: sums.at[p], s_tp, r_tp)

    def gradients(k, carry):
        gain_sum, skip_sum = carry
        rows = at_chunk(k)
        both = sums[0, k]
        for p in range(1, ntp):
            both = both + sums[p, k]
        both = jnp.concatenate([both, jnp.zeros((120, L), F32)], axis=0).T
        scale = lax.rsqrt(both[:, 0:1] / total_width + 1e-05)
        inner = both[:, 1:2]
        mixed = mixb[rows, :]
        grad_v = gvb[rows, :]
        gate = gate_v[rows, :].astype(F32)
        sigma = jax.nn.sigmoid(gate)
        grad_mixed = scale * (grad_v * gain_row) - mixed * (
            (scale * scale * scale) * inner / total_width
        )
        ggate[rows, :] = (
            grad_mixed * yb[rows, :] * sigma * (1.0 + gate * (1.0 - sigma))
        ).astype(BF16)
        grad_y = grad_mixed * gate * sigma
        dyb[rows, :] = grad_y
        gain_sum = gain_sum + jnp.sum(grad_v * mixed * scale, axis=0, keepdims=True)
        skip_sum = skip_sum + jnp.sum(
            grad_y * xb[rows, :].astype(F32), axis=0, keepdims=True
        )
        scaled = grad_y * startb[rows, :]
        hcb[k] = sum(dot(c_ref[rows, :], part, 0, 0) for part in pieces(scaled, 2))
        normed[rows, :] = (mixed * scale * gain_row).astype(BF16)
        return gain_sum, skip_sum

    zero_row = jnp.zeros((1, width), F32)
    gain_sum, skip_sum = lax.fori_loop(0, chunks, gradients, (zero_row, zero_row))
    run = hcb[chunks - 1]
    for k in range(chunks - 2, -1, -1):
        run = totb[k] * run + hcb[k]
    rloc[...] = run.astype(BF16)
    exchange_1(rloc, lb2, s_h1, r_h1)
    gx[x, 0:1, :] = gain_sum
    gx[x, 1:2, :] = skip_sum
    send(X, lambda p: gx.at[x], gx.at[x], s_gx, r_gx)

    columns = shard // nx
    steps = sorted(range(1, nz), key=lambda i: -min(i, nz - i)) + [nz]

    def block_of(i):
        return lax.rem(z + i, nz)

    def mine_of(i, p):
        return pw.at[block_of(i), pl.ds(pl.multiple_of(p * columns, columns), columns)]

    def sides(i):
        one, two = lax.rem(x + 1, nx), lax.rem(x + nx - 1, nx)
        return (one, two) if steps.index(i) % 2 == 0 else (two, one)

    def weight_copy(kind, i, to):
        source = (mine_of(i, lax.rem(x + 2, nx)), mine_of(i, to), xm.at[i - 1])[kind]
        target = (xa, xd, xc)[kind].at[i - 1]
        return rcopy(source, target, s_rx.at[kind, i - 1], r_rx.at[kind, i - 1], dev_x(to))

    def weight_send(kind, i, to):
        copy = weight_copy(kind, i, to)
        copy.start()
        pending.append(copy)

    def weight_block(i):
        k = block_of(i)
        pw[k] = dot(cot[pl.ds(pl.multiple_of(k * shard, shard), shard), :], normed[...]).astype(BF16)
        near, far = sides(i)
        if nx == 4:
            weight_send(0, i, near)
        if nx > 1:
            weight_send(1, i, far)

    def weight_relay(i):
        near, _ = sides(i)
        if nx == 4:
            weight_copy(0, i, near).wait_recv()
            xm[i - 1] = (xa[i - 1].astype(F32) + mine_of(i, near)[...].astype(F32)).astype(BF16)
            weight_send(2, i, near)

    def weight_rows(i):
        near, far = sides(i)
        out = mine_of(i, x)[...].astype(F32)
        if nx > 1:
            weight_copy(1, i, far).wait_recv()
            out = out + xd[i - 1].astype(F32)
        if nx == 4:
            weight_copy(2, i, near).wait_recv()
            out = out + xc[i - 1].astype(F32)
        zs[i - 1] = out.astype(BF16)
        if i < nz:
            copy = rcopy(zs.at[i - 1], zr.at[i - 1], s_rz.at[i - 1], r_rz.at[i - 1], dev_z(block_of(i)))
            copy.start()
            pending.append(copy)

    def weight_finish():
        out = zs[nz - 1].astype(F32)
        for i in steps[:-1]:
            rcopy(zs.at[i - 1], zr.at[i - 1], s_rz.at[i - 1], r_rz.at[i - 1], dev_z(block_of(i))).wait_recv()
            out = out + zr[i - 1].astype(F32)
        gow[...] = out

    early = steps[: (3 * nz) // 8]
    later = steps[(3 * nz) // 8 :]
    for i in early:
        weight_block(i)
    exchange_2(lb2, tb2, ub2, s_h1, r_h1, s_h2, r_h2, True)
    arrive(X, lambda p: gx.at[p], s_gx, r_gx)
    row = gx[0]
    for k in range(1, nx):
        row = row + gx[k]
    gz[z] = row
    send(Z, lambda p: gz.at[z], gz.at[z], s_gz, r_gz)

    def inside_back(k, _):
        rows = at_chunk(k)
        both = cross[k]
        summed = jnp.zeros((L, L), F32)
        lane = iota((L, SLOT), 1)
        row_sums = jnp.zeros((L, SLOT), F32)
        for p in range(pairs):
            lanes = slice(128 * p, 128 * (p + 1))
            x_pair = xb[rows, lanes]
            grads = split_pair(dyb[rows, lanes].astype(BF16))
            dots = dot(grads, x_pair, 1, 1)
            mixing = []
            for i in range(2):
                h = 2 * p + i
                decay = dec[k, h]
                weighted = dots[i * L : (i + 1) * L, :] * decay
                summed = summed + weighted
                terms = weighted * both
                row_sums = row_sums + jnp.where(
                    lane == h, jnp.sum(terms, axis=1, keepdims=True), 0.0
                )
                segr[k, h : h + 1, :] = jnp.sum(terms, axis=0, keepdims=True)
                mixing.append((decay * both).astype(BF16))
            dxi[rows, lanes] = dot(jnp.concatenate(mixing, axis=0), grads, 0, 0)
        sumd[k] = summed
        segc[k] = row_sums - segr[k].T
        scaled = dyb[rows, :] * startb[rows, :]
        accr[rows, :] = dot(summed.astype(BF16), b_ref[rows, :]) + dot(
            scaled.astype(BF16), stb[k].astype(BF16), 1, 1
        )
        return 0

    lax.fori_loop(0, chunks // 2, inside_back, 0)
    exchange_3(ub2, qs2, qb2, s_h2, r_h2, s_h3, r_h3, True)
    lax.fori_loop(chunks // 2, chunks, inside_back, 0)
    for i in early[:-1]:
        weight_relay(i)
    exchange_4(qb2, lb2, vs2, h_in, s_h3, r_h3, s_h4, r_h4, True)

    share = tokens // ntp

    def reduce_1(acc, which, ssem, rsem):
        send(
            TP,
            lambda p: acc.at[pl.ds(pl.multiple_of(p * share, share), share)],
            red.at[which, t],
            ssem,
            rsem,
        )
        red[which, t] = take_rows(acc, t, share)

    def reduce_2(which, s1, r1, ssem, rsem):
        arrive(TP, lambda p: red.at[which, p], s1, r1)
        out = red[which, 0]
        for p in range(1, ntp):
            out = out + red[which, p]
        redo[which, t] = out
        send(TP, lambda p: redo.at[which, t], redo.at[which, t], ssem, rsem)

    def reduce_3(out_ref, which, ssem, rsem):
        arrive(TP, lambda p: redo.at[which, p], ssem, rsem)
        for p in range(ntp):
            out_ref[p * share : (p + 1) * share, :] = redo[which, p]

    reduce_1(accr, 0, s_c1, r_c1)
    for i in early[-1:]:
        weight_relay(i)
    for i in later:
        weight_block(i)
    exchange_5(h_in, s_h4, r_h4)

    def states_back(i, run):
        k = chunks - 1 - i
        rows = at_chunk(k)
        hst[k] = run
        accw[rows, :] = dot(sumd[k].astype(BF16), c_ref[rows, :], 0, 0) + dot(
            (xb[rows, :].astype(F32) * endb[rows, :]).astype(BF16), run.astype(BF16), 1, 1
        )
        return totb[k] * run + hcb[k]

    lax.fori_loop(0, chunks, states_back, h_in[...].astype(F32))
    reduce_1(accw, 1, s_w1, r_w1)
    def finish(k, _):
        rows = at_chunk(k)
        grad_y = dyb[rows, :]
        run = hst[k]
        write = endb[rows, :] * sum(dot(b_ref[rows, :], part) for part in pieces(run, 2))
        gin[rows, :] = (skip_row * grad_y + dxi[rows, :] + write).astype(BF16)
        leaving = xb[rows, :].astype(F32) * write
        arriving = grad_y * startb[rows, :] * rsb[rows, :]
        seg = segc[k] + head_sums(arriving - leaving)
        final = jnp.sum(leaving, axis=0, keepdims=True) + totb[k] * jnp.sum(
            run * stb[k], axis=0, keepdims=True
        )
        final = head_sums(jnp.broadcast_to(final, (8, width)))[0:1]
        whole = sum(dot(upper, part) for part in pieces(seg, 2)) + final
        sumd[k, 0:SLOT, :] = whole.T
        return 0

    lax.fori_loop(0, chunks, finish, 0)
    for k in range(chunks):
        gdecay[:, k * L : (k + 1) * L] = sumd[k, 0:heads, :]
    for i in later[:2]:
        weight_relay(i)
    reduce_2(0, s_c1, r_c1, s_c2, r_c2)
    reduce_2(1, s_w1, r_w1, s_w2, r_w2)
    for i in early:
        weight_rows(i)
    for i in later[2:3]:
        weight_relay(i)
    arrive(Z, lambda p: gz.at[p], s_gz, r_gz)
    row = gz[0]
    for k in range(1, nz):
        row = row + gz[k]
    ggain[...] = row[0:1]
    gskip[...] = head_sums(jnp.concatenate([row, jnp.zeros((6, width), F32)], axis=0))[1:2, 0:heads]
    for i in later[3:4]:
        weight_relay(i)
    for i in later[:2]:
        weight_rows(i)
    for i in later[4:]:
        weight_relay(i)
    for i in later[2:]:
        weight_rows(i)
    reduce_3(gread, 0, s_c2, r_c2)
    reduce_3(gwrite, 1, s_w2, r_w2)
    weight_finish()
    for copy in pending:
        copy.wait_send()


def copy_out(*refs):
    count = 8
    sources, targets, scratch, sem_in, sem_out = (
        refs[:count],
        refs[count : 2 * count],
        refs[2 * count : -2],
        refs[-2],
        refs[-1],
    )
    large = [k for k in range(count) if k not in (5, 6)]
    loads = [
        pltpu.make_async_copy(sources[k], scratch[i], sem_in.at[i]) for i, k in enumerate(large)
    ]
    stores = [
        pltpu.make_async_copy(scratch[i], targets[k], sem_out.at[i]) for i, k in enumerate(large)
    ]
    for load in loads:
        load.start()
    for k in (5, 6):
        targets[k][...] = sources[k][...].reshape(targets[k].shape)
    for load, store in zip(loads, stores):
        load.wait()
        store.start()
    for store in stores:
        store.wait()


def hand_out(outs):
    vmem = pl.BlockSpec(memory_space=pltpu.VMEM)
    hbm = pl.BlockSpec(memory_space=pl.ANY)
    specs = [vmem if k in (5, 6) else hbm for k in range(8)]
    shapes = [
        jax.ShapeDtypeStruct(o.shape[1:] if k in (5, 6) else o.shape, o.dtype)
        for k, o in enumerate(outs)
    ]
    large = [o for k, o in enumerate(outs) if k not in (5, 6)]
    done = pl.pallas_call(
        copy_out,
        out_shape=shapes,
        in_specs=specs,
        out_specs=specs,
        scratch_shapes=[pltpu.VMEM(o.shape, o.dtype) for o in large]
        + [pltpu.SemaphoreType.DMA((6,)), pltpu.SemaphoreType.DMA((6,))],
        name="hand_out",
    )(*outs)
    return (*done[:7], done[7].T)


def on_device(nx, nz, ntp, packed, expo, gate, write, read, decay, skip, gain, weight, cotangent):
    cot = cotangent.T
    tokens, width = gate.shape
    heads = decay.shape[0]
    model = weight.shape[1]
    shard = cot.shape[0]
    chunks = tokens // L
    n = write.shape[1]
    columns = model // (nx * nz)
    qrows, erows = n // nx, n // (nx * nz)
    share = tokens // ntp

    def wide(kind=F32):
        return pltpu.VMEM((tokens, width), kind)

    def exchange(kind):
        return [
            pltpu.VMEM((n, width), kind),
            pltpu.VMEM((nx, qrows, width), kind),
            pltpu.VMEM((nz, erows, width), F32),
            pltpu.VMEM((nz, erows, width), F32),
            pltpu.VMEM((nz, erows, width), F32),
            pltpu.VMEM((nz, erows, width), F32),
            pltpu.VMEM((nx, qrows, width), kind),
            pltpu.VMEM((n, width), kind),
        ]

    def sems(*shape):
        return [pltpu.SemaphoreType.DMA(shape), pltpu.SemaphoreType.DMA(shape)]

    scratch = [
        pltpu.VMEM((tokens, width), BF16),
        pltpu.VMEM((width, model), BF16),
        pltpu.VMEM((model, tokens), BF16),
        wide(BF16),
        *[wide() for _ in range(7)],
        wide(BF16),
        pltpu.VMEM((chunks, SLOT, L), F32),
        pltpu.VMEM((chunks, L, SLOT), F32),
        pltpu.VMEM((chunks, 1, width), F32),
        pltpu.VMEM((chunks, heads, L, L), F32),
        pltpu.VMEM((chunks, L, L), F32),
        pltpu.VMEM((chunks, n, width), F32),
        pltpu.VMEM((chunks, n, width), F32),
        pltpu.VMEM((chunks, n, width), F32),
        pltpu.VMEM((chunks, n, width), F32),
        pltpu.VMEM((chunks, L, L), F32),
        pltpu.VMEM((chunks, SLOT, L), F32),
        pltpu.VMEM((chunks, L, SLOT), F32),
        wide(),
        *exchange(F32),
        *exchange(BF16),
        pltpu.VMEM((qrows, width), F32),
        pltpu.VMEM((nx, 1, width), F32),
        pltpu.VMEM((nz, 1, width), F32),
        pltpu.VMEM((ntp, chunks, 8, L), F32),
        pltpu.VMEM((nx, 2, width), F32),
        pltpu.VMEM((nz, 2, width), F32),
        pltpu.VMEM((nz, shard, width), BF16),
        *[pltpu.VMEM((nz, columns, width), BF16) for _ in range(6)],
        pltpu.VMEM((tokens, n), F32),
        pltpu.VMEM((tokens, n), F32),
        pltpu.VMEM((2, ntp, share, n), F32),
        pltpu.VMEM((2, ntp, share, n), F32),
        pltpu.SemaphoreType.DMA((3,)),
        *sems(10),
        *sems(nx),
        *sems(nz),
        *(sems(nx) + sems(nz) + sems(nz) + sems(nx)),
        *(sems(nx) + sems(nz) + sems(nz) + sems(nx)),
        *sems(ntp),
        *sems(nx),
        *sems(nz),
        *sems(3, nz),
        *sems(nz),
        *(sems(ntp) * 4),
    ]
    vmem = pl.BlockSpec(memory_space=pltpu.VMEM)
    hbm = pl.BlockSpec(memory_space=pl.ANY)
    outs = pl.pallas_call(
        functools.partial(core, nx, nz, ntp),
        out_shape=(
            jax.ShapeDtypeStruct((tokens, width), BF16),
            jax.ShapeDtypeStruct((tokens, width), BF16),
            jax.ShapeDtypeStruct((tokens, n), F32),
            jax.ShapeDtypeStruct((tokens, n), F32),
            jax.ShapeDtypeStruct((heads, tokens), F32),
            jax.ShapeDtypeStruct((1, heads), F32),
            jax.ShapeDtypeStruct((1, width), F32),
            jax.ShapeDtypeStruct((columns, width), F32),
        ),
        in_specs=[vmem, vmem, hbm, vmem, vmem, vmem, pl.BlockSpec(memory_space=pltpu.SMEM), vmem, hbm, hbm],
        out_specs=(vmem,) * 8,
        scratch_shapes=scratch,
        compiler_params=pltpu.CompilerParams(
            collective_id=0, has_side_effects=True, vmem_limit_bytes=60 * 1024 * 1024
        ),
        name="layer_backward",
    )(packed, expo, gate, write, read, decay, skip[None, :], gain, weight, cot)
    return hand_out(outs)


def solution(mesh):
    ntp = mesh.shape["tp"]
    nz = mesh.shape["seq"] // NX
    return jax.shard_map(
        functools.partial(on_device, NX, nz, ntp),
        mesh=mesh,
        in_specs=(
            P("seq", "tp"),
            P("tp", "seq"),
            P("seq", "tp"),
            P("seq", None),
            P("seq", None),
            P("tp", "seq"),
            P("tp"),
            P("tp"),
            P("tp", None),
            P("seq", "tp"),
        ),
        out_specs=(
            P("seq", "tp"),
            P("seq", "tp"),
            P("seq", None),
            P("seq", None),
            P("tp", "seq"),
            P("tp"),
            P("tp"),
            P("tp", "seq"),
        ),
        check_vma=False,
    )
```

```python
import functools

import jax
import jax.numpy as jnp
from jax import lax
from jax.experimental import pallas as pl
from jax.experimental.pallas import tpu as pltpu
from jax.sharding import PartitionSpec as P

MESH = pl.DeviceIdType.MESH
F32, BF16 = jnp.float32, jnp.bfloat16
EXACT = lax.Precision.HIGHEST
NX = 4
L = 128
HEAD = 64
SLOT = 16


def dot(a, b, ca=1, cb=0, precision=None):
    return lax.dot_general(
        a, b, (((ca,), (cb,)), ((), ())), preferred_element_type=F32, precision=precision
    )


def pieces(v, count):
    out = []
    for _ in range(count):
        part = v.astype(BF16)
        out.append(part)
        v = v - part.astype(F32)
    return out


def iota(shape, dim):
    return lax.broadcasted_iota(jnp.int32, shape, dim)


def rcopy(src, dst, send, recv, dev):
    return pltpu.make_async_remote_copy(
        src_ref=src, dst_ref=dst, send_sem=send, recv_sem=recv, device_id=dev, device_id_type=MESH
    )


def core(nx, nz, ntp, packed, expo, gate_hbm, b_ref, c_ref, ld_ref, skip_ref, gain_ref, w_hbm, cot_hbm,
         gin, ggate, gwrite, gread, gdecay, gskip, ggain, gow, *scratch):
    (gate_v, w_v, cot, xb, yb, gvb, mixb, dyb, rsb, endb, startb,
     normed, csr, csc, totb, dec, cross, gb, stb, hcb, hst, sumd, segr, segc, dxi,
     sloc, lb, tb, ub, qs, qb, vs, s_in,
     rloc, lb2, tb2, ub2, qs2, qb2, vs2, h_in,
     vtop, dxs, dzs, sums, totc, gx, gz, pw, xa, xd, xm, xc, zs, zr, accw, accr, red, redo,
     cp_sem, s_ag, r_ag, s_dx, r_dx, s_dz, r_dz,
     s_p1, r_p1, s_p2, r_p2, s_p3, r_p3, s_p4, r_p4,
     s_h1, r_h1, s_h2, r_h2, s_h3, r_h3, s_h4, r_h4,
     s_tp, r_tp, s_gx, r_gx, s_gz, r_gz, s_rx, r_rx, s_rz, r_rz,
     s_w1, r_w1, s_w2, r_w2, s_c1, r_c1, s_c2, r_c2) = scratch
    tokens, width = xb.shape
    chunks = tokens // L
    pairs = width // 128
    heads = width // HEAD
    total_width = width * ntp
    ny = ntp // 2
    qrows, erows = 128 // nx, 128 // (nx * nz)
    s = lax.axis_index("seq")
    t = lax.axis_index("tp")
    z, x = lax.div(s, nx), lax.rem(s, nx)
    y, half = lax.div(t, 2), lax.rem(t, 2)
    shard = cot.shape[0] // ntp

    def dev_x(p):
        return {"seq": z * nx + p, "tp": t}

    def dev_z(p):
        return {"seq": p * nx + x, "tp": t}

    def dev_t(p):
        return {"seq": s, "tp": p}

    X, Z, TP = (nx, x, dev_x), (nz, z, dev_z), (ntp, t, dev_t)
    pending = []

    def send(group, src_of, dst, ssem, rsem):
        n, me, dev = group
        for d in range(1, n):
            p = lax.rem(me + d, n)
            copy = rcopy(src_of(p), dst, ssem.at[d], rsem.at[me], dev(p))
            copy.start()
            pending.append(copy)

    def arrive(group, dst_of, ssem, rsem):
        n, me, dev = group
        for d in range(1, n):
            p = lax.rem(me + d, n)
            rcopy(dst_of(p), dst_of(p), ssem.at[d], rsem.at[p], dev(p)).wait_recv()

    def cot_rows(p, first=0, count=shard):
        return cot.at[pl.ds(pl.multiple_of(p * shard + first, 16), count)]

    load_cot = pltpu.make_async_copy(cot_hbm, cot_rows(t), cp_sem.at[0])
    load_gate = pltpu.make_async_copy(gate_hbm, gate_v, cp_sem.at[1])
    load_w = pltpu.make_async_copy(w_hbm, w_v, cp_sem.at[2])
    load_cot.start()
    load_gate.start()
    load_w.start()

    barrier = pltpu.get_barrier_semaphore()
    for n, me, dev in (X, Z, TP):
        for d in range(1, n):
            pl.semaphore_signal(
                barrier, inc=1, device_id=dev(lax.rem(me + d, n)), device_id_type=MESH
            )

    spread = (iota((SLOT, width), 1) // HEAD == iota((SLOT, width), 0)).astype(BF16)
    gather = (iota((width, SLOT), 0) // HEAD == iota((width, SLOT), 1)).astype(BF16)
    upper = (iota((L, L), 0) <= iota((L, L), 1)).astype(BF16)
    causal = iota((L, L), 0) >= iota((L, L), 1)
    left = iota((L, 128), 1) < HEAD

    def spread_heads(v):
        return sum(dot(part, spread) for part in pieces(v, 3))

    def head_sums(v):
        return sum(dot(part, gather) for part in pieces(v, 2))

    csr[...] = jnp.zeros_like(csr)
    segr[...] = jnp.zeros_like(segr)
    for k in range(chunks):
        csr[k, 0:heads, :] = ld_ref[:, k * L : (k + 1) * L]
    rows = csr[...].reshape(chunks * SLOT, L)
    rows = sum(dot(part, upper) for part in pieces(rows, 3))
    log_total = jnp.zeros((1, width), F32)
    for k in range(chunks):
        csr[k] = rows[k * SLOT : (k + 1) * SLOT, :]
        cols = rows[k * SLOT : (k + 1) * SLOT, :].T
        csc[k] = cols
        logs = spread_heads(cols)
        last = logs[L - 1 : L, :]
        log_total = log_total + last
        totb[k] = jnp.exp(last)
        endb[k * L : (k + 1) * L, :] = jnp.exp(last - logs)
        startb[k * L : (k + 1) * L, :] = jnp.exp(logs)
    dxs[x] = jnp.exp(log_total)

    powers = lax.shift_left(jnp.ones_like(expo[...]), expo[...] + 5).astype(F32) * (1.0 / 32.0)
    nibble = 4 * iota((8, width), 0)
    for k in range(chunks):
        factor_rows = jnp.concatenate(
            [powers[:, k * L : (k + 1) * L], jnp.zeros((8 - pairs, L), F32)], axis=0
        )
        factor = factor_rows.T
        wide = jnp.concatenate(
            [jnp.broadcast_to(factor[:, p : p + 1], (L, 128)) for p in range(pairs)], axis=1
        )
        words = packed[k * (L // 8) : (k + 1) * (L // 8), :]
        fields = jnp.concatenate(
            [
                lax.bitwise_and(
                    lax.shift_right_arithmetic(
                        jnp.broadcast_to(words[r : r + 1, :], (8, width)), nibble
                    ),
                    15,
                )
                - 8
                for r in range(L // 8)
            ],
            axis=0,
        )
        xb[k * L : (k + 1) * L, :] = (fields.astype(F32) * wide).astype(BF16)

    run = jnp.zeros((128, width), F32)
    for k in range(chunks):
        rows = slice(k * L, (k + 1) * L)
        weighted = xb[rows, :].astype(F32) * endb[rows, :]
        gb[k] = sum(dot(b_ref[rows, :], part, 0, 0) for part in pieces(weighted, 2))
        run = totb[k] * run + gb[k]
    sloc[...] = run

    pl.semaphore_wait(barrier, (nx - 1) + (nz - 1) + (ntp - 1))
    send(X, lambda p: dxs.at[x], dxs.at[x], s_dx, r_dx)

    load_cot.wait()
    part = shard // 2
    sibling = 2 * y + 1 - half
    after = 2 * lax.rem(y + 1, ny) + half
    before = 2 * lax.rem(y + ny - 1, ny) + half
    across = 2 * lax.rem(y + 2, ny) + half

    def cot_copy(i, j, p, to, first=0, count=shard):
        return rcopy(cot_rows(p, first, count), cot_rows(p, first, count), s_ag.at[i], r_ag.at[j], dev_t(to))

    def cot_send(i, j, p, to, *rows):
        copy = cot_copy(i, j, p, to, *rows)
        copy.start()
        pending.append(copy)

    def cot_wait(j, p, *rows):
        cot_copy(0, j, p, sibling, *rows).wait_recv()

    cot_send(0, 0, t, sibling)
    if ny == 2:
        cot_send(1, 1, t, after)
    elif ny == 4:
        cot_send(1, 1, t, after, 0, part)
        cot_send(2, 3, t, before, part, part)
        cot_send(3, 2, t, after, part, part)
        cot_send(4, 4, t, before, 0, part)

    def relay_cot():
        if ny == 4:
            cot_wait(1, before, 0, part)
            cot_send(5, 5, before, after, 0, part)
            cot_wait(3, after, part, part)
            cot_send(6, 6, after, before, part, part)

    def near_cot():
        if ny == 2:
            cot_wait(1, after)
            cot_send(2, 7, after, sibling)
        elif ny == 4:
            cot_wait(2, before, part, part)
            cot_send(7, 7, before, sibling)
            cot_wait(4, after, 0, part)
            cot_send(8, 8, after, sibling)

    def far_cot():
        if ny == 4:
            cot_wait(5, across, 0, part)
            cot_wait(6, across, part, part)
            cot_send(9, 9, across, sibling)

    def project(chip, first=False):
        terms = dot(
            cot[pl.ds(pl.multiple_of(chip * 2 * shard, 128), 2 * shard), :],
            w_v[:, pl.ds(pl.multiple_of(chip * 2 * shard, 128), 2 * shard)],
            0,
            1,
        )
        gvb[...] = terms if first else gvb[...] + terms

    def other(p):
        return p + 1 - 2 * half

    def take_rows(ref, at, count):
        return ref[pl.ds(pl.multiple_of(at * count, count), count), :]

    def exchange_1(own, lbuf, ssem, rsem):
        send(
            X,
            lambda p: own.at[pl.ds(pl.multiple_of(p * qrows, qrows), qrows)],
            lbuf.at[x],
            ssem,
            rsem,
        )
        lbuf[x] = take_rows(own, x, qrows)

    def exchange_2(lbuf, tbuf, ubuf, s1, r1, ssem, rsem, backward):
        arrive(X, lambda p: lbuf.at[p], s1, r1)
        order = range(nx - 1, -1, -1) if backward else range(nx)
        row = None
        for k in order:
            add = lbuf[k].astype(F32)
            row = add if row is None else dxs[k] * row + add
        for k in range(nz):
            tbuf[k] = row[k * erows : (k + 1) * erows, :]
        send(Z, lambda p: tbuf.at[p], ubuf.at[z], ssem, rsem)
        ubuf[z] = tbuf[z]

    def exchange_3(ubuf, qsend, qbuf, s2, r2, ssem, rsem, backward):
        arrive(Z, lambda p: ubuf.at[p], s2, r2)
        order = range(nz - 1, -1, -1) if backward else range(nz)
        row = jnp.zeros((erows, width), F32)
        for k in order:
            qsend[k] = row
            row = dzs[k] * row + ubuf[k]
        send(Z, lambda p: qsend.at[p], qbuf.at[z], ssem, rsem)
        qbuf[z] = qsend[z]

    def exchange_4(qbuf, lbuf, vsend, result, s3, r3, ssem, rsem, backward):
        arrive(Z, lambda p: qbuf.at[p], s3, r3)
        for k in range(nz):
            vtop[k * erows : (k + 1) * erows, :] = qbuf[k]
        order = range(nx - 1, -1, -1) if backward else range(nx)
        row = vtop[...]
        for k in order:
            vsend[k] = row.astype(vsend.dtype)
            row = dxs[k] * row + lbuf[k].astype(F32)
        mine = result.at[pl.ds(pl.multiple_of(x * qrows, qrows), qrows)]
        send(X, lambda p: vsend.at[p], mine, ssem, rsem)
        result[pl.ds(pl.multiple_of(x * qrows, qrows), qrows), :] = vsend[x]

    def exchange_5(result, s4, r4):
        arrive(X, lambda p: result.at[pl.ds(pl.multiple_of(p * qrows, qrows), qrows)], s4, r4)

    exchange_1(sloc, lb, s_p1, r_p1)

    arrive(X, lambda p: dxs.at[p], s_dx, r_dx)
    row = dxs[0]
    for k in range(1, nx):
        row = row * dxs[k]
    dzs[z] = row
    send(Z, lambda p: dzs.at[z], dzs.at[z], s_dz, r_dz)

    skip_row = jnp.zeros((1, width), F32)
    head_of = iota((1, width), 1) // HEAD
    for h in range(heads):
        skip_row = jnp.where(head_of == h, skip_ref[0, h], skip_row)

    def at_chunk(k):
        return pl.ds(pl.multiple_of(k * L, L), L)

    def split_pair(v):
        zero = jnp.zeros_like(v)
        return jnp.concatenate([jnp.where(left, v, zero), jnp.where(left, zero, v)], axis=0)

    def inside(k, _):
        rows = at_chunk(k)
        both = dot(c_ref[rows, :], b_ref[rows, :], 1, 1)
        cross[k] = both
        for p in range(pairs):
            mixing = []
            for h in (2 * p, 2 * p + 1):
                spread_log = csc[k][:, h : h + 1] - csr[k][h : h + 1, :]
                decay = jnp.where(causal, jnp.exp(jnp.minimum(spread_log, 0.0)), 0.0)
                dec[k, h] = decay
                mixing.append(pieces(decay * both, 2))
            lanes = slice(128 * p, 128 * (p + 1))
            x_pair = xb[rows, lanes]
            x_split = split_pair(x_pair)
            yb[rows, lanes] = (
                dot(jnp.concatenate([m[0] for m in mixing], axis=1), x_split)
                + dot(jnp.concatenate([m[1] for m in mixing], axis=1), x_split)
                + skip_row[:, lanes] * x_pair.astype(F32)
            )
        return 0

    lax.fori_loop(0, chunks // 2, inside, 0)
    load_w.wait()
    cot_wait(0, sibling)
    project(y, True)
    exchange_2(lb, tb, ub, s_p1, r_p1, s_p2, r_p2, False)
    relay_cot()
    lax.fori_loop(chunks // 2, chunks, inside, 0)
    arrive(Z, lambda p: dzs.at[p], s_dz, r_dz)
    exchange_3(ub, qs, qb, s_p2, r_p2, s_p3, r_p3, False)
    near_cot()
    exchange_4(qb, lb, vs, s_in, s_p3, r_p3, s_p4, r_p4, False)
    far_cot()
    if ny == 2:
        cot_wait(7, other(after))
        project(lax.rem(y + 1, ny))
    elif ny == 4:
        cot_wait(7, other(before))
        project(lax.rem(y + 3, ny))
        cot_wait(8, other(after))
        project(lax.rem(y + 1, ny))
    load_gate.wait()
    exchange_5(s_in, s_p4, r_p4)
    gain_row = gain_ref[...].reshape(1, width)
    stb[0] = s_in[...].astype(F32)
    for k in range(1, chunks):
        stb[k] = totb[k - 1] * stb[k - 1] + gb[k - 1]

    def outputs_of(k, _):
        rows = at_chunk(k)
        start = sum(dot(c_ref[rows, :], part) for part in pieces(stb[k], 2))
        rsb[rows, :] = start
        y_now = yb[rows, :] + startb[rows, :] * start
        yb[rows, :] = y_now
        gate = gate_v[rows, :].astype(F32)
        mixed = y_now * gate * jax.nn.sigmoid(gate)
        mixb[rows, :] = mixed
        return 0

    lax.fori_loop(0, chunks, outputs_of, 0)
    if ny == 4:
        cot_wait(9, other(across))
        project(lax.rem(y + 2, ny))

    lane = iota((L, 128), 1)

    def sums_of(k, acc):
        rows = at_chunk(k)
        mixed = mixb[rows, :]
        square = jnp.sum(mixed * mixed, axis=1, keepdims=True)
        inner = jnp.sum(gvb[rows, :] * gain_row * mixed, axis=1, keepdims=True)
        return jnp.where(lane == 2 * k, square, jnp.where(lane == 2 * k + 1, inner, acc))

    packed_sums = lax.fori_loop(0, chunks, sums_of, jnp.zeros((L, 128), F32))
    sums[t] = packed_sums.T[0:8, :]
    send(TP, lambda p: sums.at[t], sums.at[t], s_tp, r_tp)
    arrive(TP, lambda p: sums.at[p], s_tp, r_tp)

    both = sums[0]
    for p in range(1, ntp):
        both = both + sums[p]
    totc[...] = jnp.concatenate([both, jnp.zeros((120, L), F32)], axis=0).T

    def token_scales(k):
        both = totc[...]
        square = jnp.sum(jnp.where(lane == 2 * k, both, 0.0), axis=1, keepdims=True)
        inner = jnp.sum(jnp.where(lane == 2 * k + 1, both, 0.0), axis=1, keepdims=True)
        return lax.rsqrt(square / total_width + 1e-05), inner

    def gradients(k, _):
        rows = at_chunk(k)
        scale, inner = token_scales(k)
        gate = gate_v[rows, :].astype(F32)
        grad_mixed = scale * (gvb[rows, :] * gain_row) - mixb[rows, :] * (
            (scale * scale * scale) * inner / total_width
        )
        grad_y = grad_mixed * gate * jax.nn.sigmoid(gate)
        dyb[rows, :] = grad_y
        scaled = grad_y * startb[rows, :]
        hcb[k] = sum(dot(c_ref[rows, :], part, 0, 0) for part in pieces(scaled, 2))
        return 0

    lax.fori_loop(0, chunks, gradients, 0)
    run = hcb[chunks - 1]
    for k in range(chunks - 2, -1, -1):
        run = totb[k] * run + hcb[k]
    rloc[...] = run.astype(BF16)
    exchange_1(rloc, lb2, s_h1, r_h1)

    def gate_gradients(k, carry):
        gain_sum, skip_sum = carry
        rows = at_chunk(k)
        scale, inner = token_scales(k)
        mixed = mixb[rows, :]
        grad_v = gvb[rows, :]
        gate = gate_v[rows, :].astype(F32)
        sigma = jax.nn.sigmoid(gate)
        scaled_mixed = mixed * scale
        normed[rows, :] = (scaled_mixed * gain_row).astype(BF16)
        grad_mixed = scale * (grad_v * gain_row) - mixed * (
            (scale * scale * scale) * inner / total_width
        )
        ggate[rows, :] = (
            grad_mixed * yb[rows, :] * sigma * (1.0 + gate * (1.0 - sigma))
        ).astype(BF16)
        gain_sum = gain_sum + jnp.sum(grad_v * scaled_mixed, axis=0, keepdims=True)
        skip_sum = skip_sum + jnp.sum(
            dyb[rows, :] * xb[rows, :].astype(F32), axis=0, keepdims=True
        )
        return gain_sum, skip_sum

    zero_row = jnp.zeros((1, width), F32)
    gain_sum, skip_sum = lax.fori_loop(0, chunks, gate_gradients, (zero_row, zero_row))
    gx[x, 0:1, :] = gain_sum
    gx[x, 1:2, :] = skip_sum
    send(X, lambda p: gx.at[x], gx.at[x], s_gx, r_gx)

    columns = shard // nx
    steps = sorted(range(1, nz), key=lambda i: -min(i, nz - i)) + [nz]

    def block_of(i):
        return lax.rem(z + i, nz)

    def mine_of(i, p):
        return pw.at[block_of(i), pl.ds(pl.multiple_of(p * columns, columns), columns)]

    def sides(i):
        one, two = lax.rem(x + 1, nx), lax.rem(x + nx - 1, nx)
        return (one, two) if steps.index(i) % 2 == 0 else (two, one)

    def weight_copy(kind, i, to):
        source = (mine_of(i, lax.rem(x + 2, nx)), mine_of(i, to), xm.at[i - 1])[kind]
        target = (xa, xd, xc)[kind].at[i - 1]
        return rcopy(source, target, s_rx.at[kind, i - 1], r_rx.at[kind, i - 1], dev_x(to))

    def weight_send(kind, i, to):
        copy = weight_copy(kind, i, to)
        copy.start()
        pending.append(copy)

    def weight_block(i):
        k = block_of(i)
        pw[k] = dot(cot[pl.ds(pl.multiple_of(k * shard, shard), shard), :], normed[...]).astype(BF16)
        near, far = sides(i)
        if nx == 4:
            weight_send(0, i, near)
        if nx > 1:
            weight_send(1, i, far)

    def weight_relay(i):
        near, _ = sides(i)
        if nx == 4:
            weight_copy(0, i, near).wait_recv()
            xm[i - 1] = (xa[i - 1].astype(F32) + mine_of(i, near)[...].astype(F32)).astype(BF16)
            weight_send(2, i, near)

    def weight_rows(i):
        near, far = sides(i)
        out = mine_of(i, x)[...].astype(F32)
        if nx > 1:
            weight_copy(1, i, far).wait_recv()
            out = out + xd[i - 1].astype(F32)
        if nx == 4:
            weight_copy(2, i, near).wait_recv()
            out = out + xc[i - 1].astype(F32)
        away = i % nz
        if away < middle:
            ring_copy(away + 1, True).wait_recv()
            out = add_part(out, away + 1, True)
        if i > middle:
            ring_copy(i - 1, False).wait_recv()
            out = add_part(out, i - 1, False)
        if i == nz:
            gow[...] = out
            return
        zs[i - 1] = out.astype(BF16)
        for up in (True, False):
            if i == middle or (i < middle) == up:
                copy = ring_copy(i, up)
                copy.start()
                pending.append(copy)

    middle = nz // 2
    cut = 16 * (3 * columns // 80)

    def ring_rows(i, up):
        return (0, columns) if i != middle else (0, cut) if up else (cut, columns)

    def ring_copy(i, up):
        first, end = ring_rows(i, up)
        slot = i - 1 if i != middle or up else nz - 1
        return rcopy(
            zs.at[i - 1, pl.ds(first, end - first)],
            zr.at[i - 1, pl.ds(first, end - first)],
            s_rz.at[slot],
            r_rz.at[slot],
            dev_z(lax.rem(z + (1 if up else nz - 1), nz)),
        )

    def add_part(out, i, up):
        first, end = ring_rows(i, up)
        part = zr[i - 1, first:end, :].astype(F32)
        parts = [out[:first]] if first else []
        parts.append(out[first:end] + part)
        if end < columns:
            parts.append(out[end:])
        return jnp.concatenate(parts, axis=0) if len(parts) > 1 else parts[0]

    early = steps[: (3 * nz) // 8]
    later = steps[(3 * nz) // 8 :]
    for i in early:
        weight_block(i)
    exchange_2(lb2, tb2, ub2, s_h1, r_h1, s_h2, r_h2, True)
    arrive(X, lambda p: gx.at[p], s_gx, r_gx)
    row = gx[0]
    for k in range(1, nx):
        row = row + gx[k]
    gz[z] = row
    send(Z, lambda p: gz.at[z], gz.at[z], s_gz, r_gz)

    def inside_back(k, _):
        rows = at_chunk(k)
        both = cross[k]
        summed = jnp.zeros((L, L), F32)
        lane = iota((L, SLOT), 1)
        row_sums = jnp.zeros((L, SLOT), F32)
        for p in range(pairs):
            lanes = slice(128 * p, 128 * (p + 1))
            x_pair = xb[rows, lanes]
            grads = split_pair(dyb[rows, lanes].astype(BF16))
            dots = dot(grads, x_pair, 1, 1)
            mixing = []
            for i in range(2):
                h = 2 * p + i
                decay = dec[k, h]
                weighted = dots[i * L : (i + 1) * L, :] * decay
                summed = summed + weighted
                terms = weighted * both
                row_sums = row_sums + jnp.where(
                    lane == h, jnp.sum(terms, axis=1, keepdims=True), 0.0
                )
                segr[k, h : h + 1, :] = jnp.sum(terms, axis=0, keepdims=True)
                mixing.append((decay * both).astype(BF16))
            dxi[rows, lanes] = dot(jnp.concatenate(mixing, axis=0), grads, 0, 0)
        sumd[k] = summed
        segc[k] = row_sums - segr[k].T
        scaled = dyb[rows, :] * startb[rows, :]
        accr[rows, :] = dot(summed.astype(BF16), b_ref[rows, :]) + dot(
            scaled.astype(BF16), stb[k].astype(BF16), 1, 1
        )
        return 0

    lax.fori_loop(0, chunks // 2, inside_back, 0)
    for i in early[:1]:
        weight_relay(i)
    exchange_3(ub2, qs2, qb2, s_h2, r_h2, s_h3, r_h3, True)
    lax.fori_loop(chunks // 2, chunks, inside_back, 0)
    for i in early[1:]:
        weight_relay(i)
    for i in early[:1]:
        weight_rows(i)
    exchange_4(qb2, lb2, vs2, h_in, s_h3, r_h3, s_h4, r_h4, True)

    share = tokens // ntp

    def reduce_1(acc, which, ssem, rsem):
        send(
            TP,
            lambda p: acc.at[pl.ds(pl.multiple_of(p * share, share), share)],
            red.at[which, t],
            ssem,
            rsem,
        )
        red[which, t] = take_rows(acc, t, share)

    def reduce_2(which, s1, r1, ssem, rsem):
        arrive(TP, lambda p: red.at[which, p], s1, r1)
        out = red[which, 0]
        for p in range(1, ntp):
            out = out + red[which, p]
        redo[which, t] = out
        send(TP, lambda p: redo.at[which, t], redo.at[which, t], ssem, rsem)

    def reduce_3(out_ref, which, ssem, rsem):
        arrive(TP, lambda p: redo.at[which, p], ssem, rsem)
        for p in range(ntp):
            out_ref[p * share : (p + 1) * share, :] = redo[which, p]

    for i in later:
        weight_block(i)
    reduce_1(accr, 0, s_c1, r_c1)
    for i in early[1:]:
        weight_rows(i)
    exchange_5(h_in, s_h4, r_h4)

    def states_back(i, run):
        k = chunks - 1 - i
        rows = at_chunk(k)
        hst[k] = run
        accw[rows, :] = dot(sumd[k].astype(BF16), c_ref[rows, :], 0, 0) + dot(
            (xb[rows, :].astype(F32) * endb[rows, :]).astype(BF16), run.astype(BF16), 1, 1
        )
        return totb[k] * run + hcb[k]

    lax.fori_loop(0, chunks, states_back, h_in[...].astype(F32))
    reduce_1(accw, 1, s_w1, r_w1)
    for i in later[:1]:
        weight_relay(i)

    def finish(k, _):
        rows = at_chunk(k)
        grad_y = dyb[rows, :]
        run = hst[k]
        write = endb[rows, :] * sum(dot(b_ref[rows, :], part) for part in pieces(run, 2))
        gin[rows, :] = (skip_row * grad_y + dxi[rows, :] + write).astype(BF16)
        leaving = xb[rows, :].astype(F32) * write
        arriving = grad_y * startb[rows, :] * rsb[rows, :]
        seg = segc[k] + head_sums(arriving - leaving)
        final = jnp.sum(leaving, axis=0, keepdims=True) + totb[k] * jnp.sum(
            run * stb[k], axis=0, keepdims=True
        )
        final = head_sums(jnp.broadcast_to(final, (8, width)))[0:1]
        whole = sum(dot(upper, part) for part in pieces(seg, 2)) + final
        sumd[k, 0:SLOT, :] = whole.T
        return 0

    lax.fori_loop(0, chunks // 2, finish, 0)
    for i in later[1:2]:
        weight_relay(i)
    lax.fori_loop(chunks // 2, chunks, finish, 0)
    for k in range(chunks):
        gdecay[:, k * L : (k + 1) * L] = sumd[k, 0:heads, :]
    for i in later[:1]:
        weight_rows(i)
    for i in later[2:3]:
        weight_relay(i)
    reduce_2(0, s_c1, r_c1, s_c2, r_c2)
    reduce_2(1, s_w1, r_w1, s_w2, r_w2)
    for i in later[3:4]:
        weight_relay(i)
    for i in later[1:2]:
        weight_rows(i)
    arrive(Z, lambda p: gz.at[p], s_gz, r_gz)
    row = gz[0]
    for k in range(1, nz):
        row = row + gz[k]
    ggain[...] = row[0:1]
    gskip[...] = head_sums(jnp.concatenate([row, jnp.zeros((6, width), F32)], axis=0))[1:2, 0:heads]
    for i in later[4:]:
        weight_relay(i)
    for i in later[2:-1]:
        weight_rows(i)
    reduce_3(gread, 0, s_c2, r_c2)
    reduce_3(gwrite, 1, s_w2, r_w2)
    weight_rows(nz)
    for copy in pending:
        copy.wait_send()


def copy_out(*refs):
    count = 8
    sources, targets, scratch, sem_in, sem_out = (
        refs[:count],
        refs[count : 2 * count],
        refs[2 * count : -2],
        refs[-2],
        refs[-1],
    )
    large = [k for k in range(count) if k not in (5, 6)]
    loads = [
        pltpu.make_async_copy(sources[k], scratch[i], sem_in.at[i]) for i, k in enumerate(large)
    ]
    stores = [
        pltpu.make_async_copy(scratch[i], targets[k], sem_out.at[i]) for i, k in enumerate(large)
    ]
    for load in loads:
        load.start()
    for k in (5, 6):
        targets[k][...] = sources[k][...].reshape(targets[k].shape)
    for load, store in zip(loads, stores):
        load.wait()
        store.start()
    for store in stores:
        store.wait()


def hand_out(outs):
    vmem = pl.BlockSpec(memory_space=pltpu.VMEM)
    hbm = pl.BlockSpec(memory_space=pl.ANY)
    specs = [vmem if k in (5, 6) else hbm for k in range(8)]
    shapes = [
        jax.ShapeDtypeStruct(o.shape[1:] if k in (5, 6) else o.shape, o.dtype)
        for k, o in enumerate(outs)
    ]
    large = [o for k, o in enumerate(outs) if k not in (5, 6)]
    done = pl.pallas_call(
        copy_out,
        out_shape=shapes,
        in_specs=specs,
        out_specs=specs,
        scratch_shapes=[pltpu.VMEM(o.shape, o.dtype) for o in large]
        + [pltpu.SemaphoreType.DMA((6,)), pltpu.SemaphoreType.DMA((6,))],
        name="hand_out",
    )(*outs)
    return (*done[:7], done[7].T)


def on_device(nx, nz, ntp, packed, expo, gate, write, read, decay, skip, gain, weight, cotangent):
    cot = cotangent.T
    tokens, width = gate.shape
    heads = decay.shape[0]
    model = weight.shape[1]
    shard = cot.shape[0]
    chunks = tokens // L
    n = write.shape[1]
    columns = model // (nx * nz)
    qrows, erows = n // nx, n // (nx * nz)
    share = tokens // ntp

    def wide(kind=F32):
        return pltpu.VMEM((tokens, width), kind)

    def exchange(kind):
        return [
            pltpu.VMEM((n, width), kind),
            pltpu.VMEM((nx, qrows, width), kind),
            pltpu.VMEM((nz, erows, width), F32),
            pltpu.VMEM((nz, erows, width), F32),
            pltpu.VMEM((nz, erows, width), F32),
            pltpu.VMEM((nz, erows, width), F32),
            pltpu.VMEM((nx, qrows, width), kind),
            pltpu.VMEM((n, width), kind),
        ]

    def sems(*shape):
        return [pltpu.SemaphoreType.DMA(shape), pltpu.SemaphoreType.DMA(shape)]

    scratch = [
        pltpu.VMEM((tokens, width), BF16),
        pltpu.VMEM((width, model), BF16),
        pltpu.VMEM((model, tokens), BF16),
        wide(BF16),
        *[wide() for _ in range(7)],
        wide(BF16),
        pltpu.VMEM((chunks, SLOT, L), F32),
        pltpu.VMEM((chunks, L, SLOT), F32),
        pltpu.VMEM((chunks, 1, width), F32),
        pltpu.VMEM((chunks, heads, L, L), F32),
        pltpu.VMEM((chunks, L, L), F32),
        pltpu.VMEM((chunks, n, width), F32),
        pltpu.VMEM((chunks, n, width), F32),
        pltpu.VMEM((chunks, n, width), F32),
        pltpu.VMEM((chunks, n, width), F32),
        pltpu.VMEM((chunks, L, L), F32),
        pltpu.VMEM((chunks, SLOT, L), F32),
        pltpu.VMEM((chunks, L, SLOT), F32),
        wide(),
        *exchange(F32),
        *exchange(BF16),
        pltpu.VMEM((qrows, width), F32),
        pltpu.VMEM((nx, 1, width), F32),
        pltpu.VMEM((nz, 1, width), F32),
        pltpu.VMEM((ntp, 8, L), F32),
        pltpu.VMEM((L, 128), F32),
        pltpu.VMEM((nx, 2, width), F32),
        pltpu.VMEM((nz, 2, width), F32),
        pltpu.VMEM((nz, shard, width), BF16),
        *[pltpu.VMEM((nz, columns, width), BF16) for _ in range(6)],
        pltpu.VMEM((tokens, n), F32),
        pltpu.VMEM((tokens, n), F32),
        pltpu.VMEM((2, ntp, share, n), F32),
        pltpu.VMEM((2, ntp, share, n), F32),
        pltpu.SemaphoreType.DMA((3,)),
        *sems(10),
        *sems(nx),
        *sems(nz),
        *(sems(nx) + sems(nz) + sems(nz) + sems(nx)),
        *(sems(nx) + sems(nz) + sems(nz) + sems(nx)),
        *sems(ntp),
        *sems(nx),
        *sems(nz),
        *sems(3, nz),
        *sems(nz),
        *(sems(ntp) * 4),
    ]
    vmem = pl.BlockSpec(memory_space=pltpu.VMEM)
    hbm = pl.BlockSpec(memory_space=pl.ANY)
    outs = pl.pallas_call(
        functools.partial(core, nx, nz, ntp),
        out_shape=(
            jax.ShapeDtypeStruct((tokens, width), BF16),
            jax.ShapeDtypeStruct((tokens, width), BF16),
            jax.ShapeDtypeStruct((tokens, n), F32),
            jax.ShapeDtypeStruct((tokens, n), F32),
            jax.ShapeDtypeStruct((heads, tokens), F32),
            jax.ShapeDtypeStruct((1, heads), F32),
            jax.ShapeDtypeStruct((1, width), F32),
            jax.ShapeDtypeStruct((columns, width), F32),
        ),
        in_specs=[vmem, vmem, hbm, vmem, vmem, vmem, pl.BlockSpec(memory_space=pltpu.SMEM), vmem, hbm, hbm],
        out_specs=(vmem,) * 8,
        scratch_shapes=scratch,
        compiler_params=pltpu.CompilerParams(
            collective_id=0, has_side_effects=True, vmem_limit_bytes=60 * 1024 * 1024
        ),
        name="layer_backward",
    )(packed, expo, gate, write, read, decay, skip[None, :], gain, weight, cot)
    return hand_out(outs)


def solution(mesh):
    ntp = mesh.shape["tp"]
    nz = mesh.shape["seq"] // NX
    return jax.shard_map(
        functools.partial(on_device, NX, nz, ntp),
        mesh=mesh,
        in_specs=(
            P("seq", "tp"),
            P("tp", "seq"),
            P("seq", "tp"),
            P("seq", None),
            P("seq", None),
            P("tp", "seq"),
            P("tp"),
            P("tp"),
            P("tp", None),
            P("seq", "tp"),
        ),
        out_specs=(
            P("seq", "tp"),
            P("seq", "tp"),
            P("seq", None),
            P("seq", None),
            P("tp", "seq"),
            P("tp"),
            P("tp"),
            P("tp", "seq"),
        ),
        check_vma=False,
    )
```

```python
import functools

import jax
import jax.numpy as jnp
from jax import lax
from jax.experimental import pallas as pl
from jax.experimental.pallas import tpu as pltpu
from jax.sharding import PartitionSpec as P

MESH = pl.DeviceIdType.MESH
F32, BF16 = jnp.float32, jnp.bfloat16
EXACT = lax.Precision.HIGHEST
NX = 4
L = 128
HEAD = 64
SLOT = 16
FRONT = 384


def dot(a, b, ca=1, cb=0, precision=None):
    return lax.dot_general(
        a, b, (((ca,), (cb,)), ((), ())), preferred_element_type=F32, precision=precision
    )


def pieces(v, count):
    out = []
    for _ in range(count):
        part = v.astype(BF16)
        out.append(part)
        v = v - part.astype(F32)
    return out


def iota(shape, dim):
    return lax.broadcasted_iota(jnp.int32, shape, dim)


def rcopy(src, dst, send, recv, dev):
    return pltpu.make_async_remote_copy(
        src_ref=src, dst_ref=dst, send_sem=send, recv_sem=recv, device_id=dev, device_id_type=MESH
    )


def core(nx, nz, ntp, packed, expo, gate_hbm, b_ref, c_ref, ld_ref, skip_ref, gain_ref, w_hbm, cot_hbm,
         gin, ggate, gwrite, gread, gdecay, gskip, ggain, gow, *scratch):
    (gate_v, w_v, cot, xb, yb, gvb, mixb, dyb, rsb, endb, startb,
     normed, csr, csc, totb, dec, cross, gb, stb, hcb, hst, sumd, segr, segc, dxi,
     sloc, lb, tb, ub, qs, qb, vs, s_in,
     rloc, lb2, tb2, ub2, qs2, qb2, vs2, h_in,
     vtop, dxs, dzs, sums, totc, gx, gz, pwa, pwb, xa, xd, xm, xc, zsa, zra, zsb, zrb, xsb, xrb, accw, accr, red, redo,
     cp_sem, s_ag, r_ag, s_dx, r_dx, s_dz, r_dz,
     s_p1, r_p1, s_p2, r_p2, s_p3, r_p3, s_p4, r_p4,
     s_h1, r_h1, s_h2, r_h2, s_h3, r_h3, s_h4, r_h4,
     s_tp, r_tp, s_gx, r_gx, s_gz, r_gz, s_rx, r_rx, s_za, r_za, s_zb, r_zb, s_xb, r_xb,
     s_w1, r_w1, s_w2, r_w2, s_c1, r_c1, s_c2, r_c2) = scratch
    tokens, width = xb.shape
    chunks = tokens // L
    pairs = width // 128
    heads = width // HEAD
    total_width = width * ntp
    ny = ntp // 2
    qrows, erows = 128 // nx, 128 // (nx * nz)
    s = lax.axis_index("seq")
    t = lax.axis_index("tp")
    z, x = lax.div(s, nx), lax.rem(s, nx)
    y, half = lax.div(t, 2), lax.rem(t, 2)
    shard = cot.shape[0] // ntp

    def dev_x(p):
        return {"seq": z * nx + p, "tp": t}

    def dev_z(p):
        return {"seq": p * nx + x, "tp": t}

    def dev_t(p):
        return {"seq": s, "tp": p}

    X, Z, TP = (nx, x, dev_x), (nz, z, dev_z), (ntp, t, dev_t)
    pending = []

    def send(group, src_of, dst, ssem, rsem):
        n, me, dev = group
        for d in range(1, n):
            p = lax.rem(me + d, n)
            copy = rcopy(src_of(p), dst, ssem.at[d], rsem.at[me], dev(p))
            copy.start()
            pending.append(copy)

    def arrive(group, dst_of, ssem, rsem):
        n, me, dev = group
        for d in range(1, n):
            p = lax.rem(me + d, n)
            rcopy(dst_of(p), dst_of(p), ssem.at[d], rsem.at[p], dev(p)).wait_recv()

    def cot_rows(p, first=0, count=shard):
        return cot.at[pl.ds(pl.multiple_of(p * shard + first, 16), count)]

    load_cot = pltpu.make_async_copy(cot_hbm, cot_rows(t), cp_sem.at[0])
    load_gate = pltpu.make_async_copy(gate_hbm, gate_v, cp_sem.at[1])
    load_w = pltpu.make_async_copy(w_hbm, w_v, cp_sem.at[2])
    load_cot.start()
    load_gate.start()
    load_w.start()

    barrier = pltpu.get_barrier_semaphore()
    for n, me, dev in (X, Z, TP):
        for d in range(1, n):
            pl.semaphore_signal(
                barrier, inc=1, device_id=dev(lax.rem(me + d, n)), device_id_type=MESH
            )

    spread = (iota((SLOT, width), 1) // HEAD == iota((SLOT, width), 0)).astype(BF16)
    gather = (iota((width, SLOT), 0) // HEAD == iota((width, SLOT), 1)).astype(BF16)
    upper = (iota((L, L), 0) <= iota((L, L), 1)).astype(BF16)
    causal = iota((L, L), 0) >= iota((L, L), 1)
    left = iota((L, 128), 1) < HEAD

    def spread_heads(v):
        return sum(dot(part, spread) for part in pieces(v, 3))

    def head_sums(v):
        return sum(dot(part, gather) for part in pieces(v, 2))

    csr[...] = jnp.zeros_like(csr)
    segr[...] = jnp.zeros_like(segr)
    for k in range(chunks):
        csr[k, 0:heads, :] = ld_ref[:, k * L : (k + 1) * L]
    rows = csr[...].reshape(chunks * SLOT, L)
    rows = sum(dot(part, upper) for part in pieces(rows, 3))
    log_total = jnp.zeros((1, width), F32)
    for k in range(chunks):
        csr[k] = rows[k * SLOT : (k + 1) * SLOT, :]
        cols = rows[k * SLOT : (k + 1) * SLOT, :].T
        csc[k] = cols
        logs = spread_heads(cols)
        last = logs[L - 1 : L, :]
        log_total = log_total + last
        totb[k] = jnp.exp(last)
        endb[k * L : (k + 1) * L, :] = jnp.exp(last - logs)
        startb[k * L : (k + 1) * L, :] = jnp.exp(logs)
    dxs[x] = jnp.exp(log_total)

    powers = lax.shift_left(jnp.ones_like(expo[...]), expo[...] + 5).astype(F32) * (1.0 / 32.0)
    nibble = 4 * iota((8, width), 0)
    for k in range(chunks):
        factor_rows = jnp.concatenate(
            [powers[:, k * L : (k + 1) * L], jnp.zeros((8 - pairs, L), F32)], axis=0
        )
        factor = factor_rows.T
        wide = jnp.concatenate(
            [jnp.broadcast_to(factor[:, p : p + 1], (L, 128)) for p in range(pairs)], axis=1
        )
        words = packed[k * (L // 8) : (k + 1) * (L // 8), :]
        fields = jnp.concatenate(
            [
                lax.bitwise_and(
                    lax.shift_right_arithmetic(
                        jnp.broadcast_to(words[r : r + 1, :], (8, width)), nibble
                    ),
                    15,
                )
                - 8
                for r in range(L // 8)
            ],
            axis=0,
        )
        xb[k * L : (k + 1) * L, :] = (fields.astype(F32) * wide).astype(BF16)

    run = jnp.zeros((128, width), F32)
    for k in range(chunks):
        rows = slice(k * L, (k + 1) * L)
        weighted = xb[rows, :].astype(F32) * endb[rows, :]
        gb[k] = sum(dot(b_ref[rows, :], part, 0, 0) for part in pieces(weighted, 2))
        run = totb[k] * run + gb[k]
    sloc[...] = run

    pl.semaphore_wait(barrier, (nx - 1) + (nz - 1) + (ntp - 1))
    send(X, lambda p: dxs.at[x], dxs.at[x], s_dx, r_dx)

    load_cot.wait()
    part = shard // 2
    sibling = 2 * y + 1 - half
    after = 2 * lax.rem(y + 1, ny) + half
    before = 2 * lax.rem(y + ny - 1, ny) + half
    across = 2 * lax.rem(y + 2, ny) + half

    def cot_copy(i, j, p, to, first=0, count=shard):
        return rcopy(cot_rows(p, first, count), cot_rows(p, first, count), s_ag.at[i], r_ag.at[j], dev_t(to))

    def cot_send(i, j, p, to, *rows):
        copy = cot_copy(i, j, p, to, *rows)
        copy.start()
        pending.append(copy)

    def cot_wait(j, p, *rows):
        cot_copy(0, j, p, sibling, *rows).wait_recv()

    cot_send(0, 0, t, sibling)
    if ny == 2:
        cot_send(1, 1, t, after)
    elif ny == 4:
        cot_send(1, 1, t, after, 0, part)
        cot_send(2, 3, t, before, part, part)
        cot_send(3, 2, t, after, part, part)
        cot_send(4, 4, t, before, 0, part)

    def relay_cot():
        if ny == 4:
            cot_wait(1, before, 0, part)
            cot_send(5, 5, before, after, 0, part)
            cot_wait(3, after, part, part)
            cot_send(6, 6, after, before, part, part)

    def near_cot():
        if ny == 2:
            cot_wait(1, after)
            cot_send(2, 7, after, sibling)
        elif ny == 4:
            cot_wait(2, before, part, part)
            cot_send(7, 7, before, sibling)
            cot_wait(4, after, 0, part)
            cot_send(8, 8, after, sibling)

    def far_cot():
        if ny == 4:
            cot_wait(5, across, 0, part)
            cot_wait(6, across, part, part)
            cot_send(9, 9, across, sibling)

    def project(chip, first=False):
        terms = dot(
            cot[pl.ds(pl.multiple_of(chip * 2 * shard, 128), 2 * shard), :],
            w_v[:, pl.ds(pl.multiple_of(chip * 2 * shard, 128), 2 * shard)],
            0,
            1,
        )
        gvb[...] = terms if first else gvb[...] + terms

    def other(p):
        return p + 1 - 2 * half

    def take_rows(ref, at, count):
        return ref[pl.ds(pl.multiple_of(at * count, count), count), :]

    def exchange_1(own, lbuf, ssem, rsem):
        send(
            X,
            lambda p: own.at[pl.ds(pl.multiple_of(p * qrows, qrows), qrows)],
            lbuf.at[x],
            ssem,
            rsem,
        )
        lbuf[x] = take_rows(own, x, qrows)

    def exchange_2(lbuf, tbuf, ubuf, s1, r1, ssem, rsem, backward):
        arrive(X, lambda p: lbuf.at[p], s1, r1)
        order = range(nx - 1, -1, -1) if backward else range(nx)
        row = None
        for k in order:
            add = lbuf[k].astype(F32)
            row = add if row is None else dxs[k] * row + add
        for k in range(nz):
            tbuf[k] = row[k * erows : (k + 1) * erows, :]
        send(Z, lambda p: tbuf.at[p], ubuf.at[z], ssem, rsem)
        ubuf[z] = tbuf[z]

    def exchange_3(ubuf, qsend, qbuf, s2, r2, ssem, rsem, backward):
        arrive(Z, lambda p: ubuf.at[p], s2, r2)
        order = range(nz - 1, -1, -1) if backward else range(nz)
        row = jnp.zeros((erows, width), F32)
        for k in order:
            qsend[k] = row
            row = dzs[k] * row + ubuf[k]
        send(Z, lambda p: qsend.at[p], qbuf.at[z], ssem, rsem)
        qbuf[z] = qsend[z]

    def exchange_4(qbuf, lbuf, vsend, result, s3, r3, ssem, rsem, backward):
        arrive(Z, lambda p: qbuf.at[p], s3, r3)
        for k in range(nz):
            vtop[k * erows : (k + 1) * erows, :] = qbuf[k]
        order = range(nx - 1, -1, -1) if backward else range(nx)
        row = vtop[...]
        for k in order:
            vsend[k] = row.astype(vsend.dtype)
            row = dxs[k] * row + lbuf[k].astype(F32)
        mine = result.at[pl.ds(pl.multiple_of(x * qrows, qrows), qrows)]
        send(X, lambda p: vsend.at[p], mine, ssem, rsem)
        result[pl.ds(pl.multiple_of(x * qrows, qrows), qrows), :] = vsend[x]

    def exchange_5(result, s4, r4):
        arrive(X, lambda p: result.at[pl.ds(pl.multiple_of(p * qrows, qrows), qrows)], s4, r4)

    exchange_1(sloc, lb, s_p1, r_p1)

    skip_row = jnp.zeros((1, width), F32)
    head_of = iota((1, width), 1) // HEAD
    for h in range(heads):
        skip_row = jnp.where(head_of == h, skip_ref[0, h], skip_row)

    def at_chunk(k):
        return pl.ds(pl.multiple_of(k * L, L), L)

    def split_pair(v):
        zero = jnp.zeros_like(v)
        return jnp.concatenate([jnp.where(left, v, zero), jnp.where(left, zero, v)], axis=0)

    def inside(k, _):
        rows = at_chunk(k)
        both = dot(c_ref[rows, :], b_ref[rows, :], 1, 1)
        cross[k] = both
        for p in range(pairs):
            mixing = []
            for h in (2 * p, 2 * p + 1):
                spread_log = csc[k][:, h : h + 1] - csr[k][h : h + 1, :]
                decay = jnp.where(causal, jnp.exp(jnp.minimum(spread_log, 0.0)), 0.0)
                dec[k, h] = decay
                mixing.append(pieces(decay * both, 2))
            lanes = slice(128 * p, 128 * (p + 1))
            x_pair = xb[rows, lanes]
            x_split = split_pair(x_pair)
            yb[rows, lanes] = (
                dot(jnp.concatenate([m[0] for m in mixing], axis=1), x_split)
                + dot(jnp.concatenate([m[1] for m in mixing], axis=1), x_split)
                + skip_row[:, lanes] * x_pair.astype(F32)
            )
        return 0

    lax.fori_loop(0, chunks // 2, inside, 0)
    load_w.wait()
    cot_wait(0, sibling)
    project(y, True)
    arrive(X, lambda p: dxs.at[p], s_dx, r_dx)
    row = dxs[0]
    for k in range(1, nx):
        row = row * dxs[k]
    dzs[z] = row
    send(Z, lambda p: dzs.at[z], dzs.at[z], s_dz, r_dz)

    exchange_2(lb, tb, ub, s_p1, r_p1, s_p2, r_p2, False)
    relay_cot()
    lax.fori_loop(chunks // 2, chunks, inside, 0)
    arrive(Z, lambda p: dzs.at[p], s_dz, r_dz)
    exchange_3(ub, qs, qb, s_p2, r_p2, s_p3, r_p3, False)
    near_cot()
    exchange_4(qb, lb, vs, s_in, s_p3, r_p3, s_p4, r_p4, False)
    far_cot()
    if ny == 2:
        cot_wait(7, other(after))
        project(lax.rem(y + 1, ny))
    elif ny == 4:
        cot_wait(7, other(before))
        project(lax.rem(y + 3, ny))
        cot_wait(8, other(after))
        project(lax.rem(y + 1, ny))
    load_gate.wait()
    exchange_5(s_in, s_p4, r_p4)
    gain_row = gain_ref[...].reshape(1, width)
    stb[0] = s_in[...].astype(F32)
    for k in range(1, chunks):
        stb[k] = totb[k - 1] * stb[k - 1] + gb[k - 1]

    def outputs_of(k, _):
        rows = at_chunk(k)
        start = sum(dot(c_ref[rows, :], part) for part in pieces(stb[k], 2))
        rsb[rows, :] = start
        y_now = yb[rows, :] + startb[rows, :] * start
        yb[rows, :] = y_now
        gate = gate_v[rows, :].astype(F32)
        mixed = y_now * gate * jax.nn.sigmoid(gate)
        mixb[rows, :] = mixed
        return 0

    lax.fori_loop(0, chunks, outputs_of, 0)
    if ny == 4:
        cot_wait(9, other(across))
        project(lax.rem(y + 2, ny))

    lane = iota((L, 128), 1)

    def sums_of(k, acc):
        rows = at_chunk(k)
        mixed = mixb[rows, :]
        square = jnp.sum(mixed * mixed, axis=1, keepdims=True)
        inner = jnp.sum(gvb[rows, :] * gain_row * mixed, axis=1, keepdims=True)
        return jnp.where(lane == 2 * k, square, jnp.where(lane == 2 * k + 1, inner, acc))

    packed_sums = lax.fori_loop(0, chunks, sums_of, jnp.zeros((L, 128), F32))
    sums[t] = packed_sums.T[0:8, :]
    send(TP, lambda p: sums.at[t], sums.at[t], s_tp, r_tp)
    arrive(TP, lambda p: sums.at[p], s_tp, r_tp)

    both = sums[0]
    for p in range(1, ntp):
        both = both + sums[p]
    totc[...] = jnp.concatenate([both, jnp.zeros((120, L), F32)], axis=0).T

    def token_scales(k):
        both = totc[...]
        square = jnp.sum(jnp.where(lane == 2 * k, both, 0.0), axis=1, keepdims=True)
        inner = jnp.sum(jnp.where(lane == 2 * k + 1, both, 0.0), axis=1, keepdims=True)
        return lax.rsqrt(square / total_width + 1e-05), inner

    def gradients(k, _):
        rows = at_chunk(k)
        scale, inner = token_scales(k)
        gate = gate_v[rows, :].astype(F32)
        grad_mixed = scale * (gvb[rows, :] * gain_row) - mixb[rows, :] * (
            (scale * scale * scale) * inner / total_width
        )
        grad_y = grad_mixed * gate * jax.nn.sigmoid(gate)
        dyb[rows, :] = grad_y
        scaled = grad_y * startb[rows, :]
        hcb[k] = sum(dot(c_ref[rows, :], part, 0, 0) for part in pieces(scaled, 2))
        return 0

    lax.fori_loop(0, chunks, gradients, 0)
    run = hcb[chunks - 1]
    for k in range(chunks - 2, -1, -1):
        run = totb[k] * run + hcb[k]
    rloc[...] = run.astype(BF16)
    exchange_1(rloc, lb2, s_h1, r_h1)

    def gate_gradients(k, carry):
        gain_sum, skip_sum = carry
        rows = at_chunk(k)
        scale, inner = token_scales(k)
        mixed = mixb[rows, :]
        grad_v = gvb[rows, :]
        gate = gate_v[rows, :].astype(F32)
        sigma = jax.nn.sigmoid(gate)
        scaled_mixed = mixed * scale
        normed[rows, :] = (scaled_mixed * gain_row).astype(BF16)
        grad_mixed = scale * (grad_v * gain_row) - mixed * (
            (scale * scale * scale) * inner / total_width
        )
        ggate[rows, :] = (
            grad_mixed * yb[rows, :] * sigma * (1.0 + gate * (1.0 - sigma))
        ).astype(BF16)
        gain_sum = gain_sum + jnp.sum(grad_v * scaled_mixed, axis=0, keepdims=True)
        skip_sum = skip_sum + jnp.sum(
            dyb[rows, :] * xb[rows, :].astype(F32), axis=0, keepdims=True
        )
        return gain_sum, skip_sum

    zero_row = jnp.zeros((1, width), F32)
    gain_sum, skip_sum = lax.fori_loop(0, chunks, gate_gradients, (zero_row, zero_row))
    gx[x, 0:1, :] = gain_sum
    gx[x, 1:2, :] = skip_sum
    send(X, lambda p: gx.at[x], gx.at[x], s_gx, r_gx)

    columns = shard // nx
    front = pwa.shape[2]
    middle = nz // 2
    steps = sorted(range(1, nz), key=lambda i: -min(i, nz - i)) + [nz]

    def block_of(i):
        return lax.rem(z + i, nz)

    def mine_of(i, p):
        return pwa.at[block_of(i), pl.ds(pl.multiple_of(p * columns, columns), columns)]

    def sides(i):
        one, two = lax.rem(x + 1, nx), lax.rem(x + nx - 1, nx)
        return (one, two) if steps.index(i) % 2 == 0 else (two, one)

    def weight_copy(kind, i, to):
        source = (mine_of(i, lax.rem(x + 2, nx)), mine_of(i, to), xm.at[i - 1])[kind]
        target = (xa, xd, xc)[kind].at[i - 1]
        return rcopy(source, target, s_rx.at[kind, i - 1], r_rx.at[kind, i - 1], dev_x(to))

    def weight_send(kind, i, to):
        copy = weight_copy(kind, i, to)
        copy.start()
        pending.append(copy)

    def weight_block(i):
        k = block_of(i)
        terms = dot(cot[pl.ds(pl.multiple_of(k * shard, shard), shard), :], normed[...]).astype(BF16)
        pwa[k] = terms[:, :front]
        pwb[k] = terms[:, front:]
        near, far = sides(i)
        if nx == 4:
            weight_send(0, i, near)
        if nx > 1:
            weight_send(1, i, far)

    def weight_relay(i):
        near, _ = sides(i)
        if nx == 4:
            weight_copy(0, i, near).wait_recv()
            xm[i - 1] = (xa[i - 1].astype(F32) + mine_of(i, near)[...].astype(F32)).astype(BF16)
            weight_send(2, i, near)

    def ring_part(kind, i, up):
        rows = (columns, shard)[kind]
        cut = 16 * (3 * rows // 80)
        return (0, rows) if i != middle else (0, cut) if up else (cut, rows)

    def ring_copy(kind, i, up):
        first, end = ring_part(kind, i, up)
        slot = i - 1 if i != middle or up else nz - 1
        sends, lands, s_z, r_z = ((zsa, zra, s_za, r_za), (zsb, zrb, s_zb, r_zb))[kind]
        return rcopy(
            sends.at[i - 1, pl.ds(first, end - first)],
            lands.at[i - 1, pl.ds(first, end - first)],
            s_z.at[slot],
            r_z.at[slot],
            dev_z(lax.rem(z + (1 if up else nz - 1), nz)),
        )

    def ring_add(kind, out, i, up):
        ring_copy(kind, i, up).wait_recv()
        first, end = ring_part(kind, i, up)
        part = (zra, zrb)[kind][i - 1, first:end, :].astype(F32)
        parts = [out[:first]] if first else []
        parts.append(out[first:end] + part)
        if end < out.shape[0]:
            parts.append(out[end:])
        return jnp.concatenate(parts, axis=0) if len(parts) > 1 else parts[0]

    def ring_step(kind, i, out):
        if i % nz < middle:
            out = ring_add(kind, out, i % nz + 1, True)
        if i > middle:
            out = ring_add(kind, out, i - 1, False)
        if i < nz:
            (zsa, zsb)[kind][i - 1] = out.astype(BF16)
            for up in (True, False):
                if i == middle or (i < middle) == up:
                    copy = ring_copy(kind, i, up)
                    copy.start()
                    pending.append(copy)
        return out

    def weight_rows(i):
        near, far = sides(i)
        out = mine_of(i, x)[...].astype(F32)
        if nx > 1:
            weight_copy(1, i, far).wait_recv()
            out = out + xd[i - 1].astype(F32)
        if nx == 4:
            weight_copy(2, i, near).wait_recv()
            out = out + xc[i - 1].astype(F32)
        out = ring_step(0, i, out)
        if i == nz:
            gow[:, :front] = out

    def back_rows(i):
        out = ring_step(1, i, pwb[block_of(i)].astype(F32))
        if i == nz:
            for p in range(nx):
                xsb[p] = out[p * columns : (p + 1) * columns, :].astype(BF16)
            send(X, lambda p: xsb.at[p], xrb.at[x], s_xb, r_xb)
            xrb[x] = xsb[x]

    def back_finish():
        arrive(X, lambda p: xrb.at[p], s_xb, r_xb)
        out = xrb[0].astype(F32)
        for p in range(1, nx):
            out = out + xrb[p].astype(F32)
        gow[:, front:] = out

    early = steps[: (5 * nz) // 8]
    later = steps[(5 * nz) // 8 :]
    order = iter(steps)

    def back_steps(count):
        for _ in range(count):
            i = next(order, None)
            if i is not None:
                back_rows(i)

    for n, i in enumerate(early):
        weight_block(i)
        if n == 0:
            back_steps(1)
    exchange_2(lb2, tb2, ub2, s_h1, r_h1, s_h2, r_h2, True)
    arrive(X, lambda p: gx.at[p], s_gx, r_gx)
    row = gx[0]
    for k in range(1, nx):
        row = row + gx[k]
    gz[z] = row
    send(Z, lambda p: gz.at[z], gz.at[z], s_gz, r_gz)

    def inside_back(k, _):
        rows = at_chunk(k)
        both = cross[k]
        summed = jnp.zeros((L, L), F32)
        lane = iota((L, SLOT), 1)
        row_sums = jnp.zeros((L, SLOT), F32)
        for p in range(pairs):
            lanes = slice(128 * p, 128 * (p + 1))
            x_pair = xb[rows, lanes]
            grads = split_pair(dyb[rows, lanes].astype(BF16))
            dots = dot(grads, x_pair, 1, 1)
            mixing = []
            for i in range(2):
                h = 2 * p + i
                decay = dec[k, h]
                weighted = dots[i * L : (i + 1) * L, :] * decay
                summed = summed + weighted
                terms = weighted * both
                row_sums = row_sums + jnp.where(
                    lane == h, jnp.sum(terms, axis=1, keepdims=True), 0.0
                )
                segr[k, h : h + 1, :] = jnp.sum(terms, axis=0, keepdims=True)
                mixing.append((decay * both).astype(BF16))
            dxi[rows, lanes] = dot(jnp.concatenate(mixing, axis=0), grads, 0, 0)
        sumd[k] = summed
        segc[k] = row_sums - segr[k].T
        scaled = dyb[rows, :] * startb[rows, :]
        accr[rows, :] = dot(summed.astype(BF16), b_ref[rows, :]) + dot(
            scaled.astype(BF16), stb[k].astype(BF16), 1, 1
        )
        return 0

    lax.fori_loop(0, chunks // 2, inside_back, 0)
    for i in early[:1]:
        weight_relay(i)
    back_steps(2 if nz == 8 else 0)
    exchange_3(ub2, qs2, qb2, s_h2, r_h2, s_h3, r_h3, True)
    lax.fori_loop(chunks // 2, chunks, inside_back, 0)
    for i in early[1:3]:
        weight_relay(i)
    for i in early[:1]:
        weight_rows(i)
    exchange_4(qb2, lb2, vs2, h_in, s_h3, r_h3, s_h4, r_h4, True)

    share = tokens // ntp

    def reduce_1(acc, which, ssem, rsem):
        send(
            TP,
            lambda p: acc.at[pl.ds(pl.multiple_of(p * share, share), share)],
            red.at[which, t],
            ssem,
            rsem,
        )
        red[which, t] = take_rows(acc, t, share)

    def reduce_2(which, s1, r1, ssem, rsem):
        arrive(TP, lambda p: red.at[which, p], s1, r1)
        out = red[which, 0]
        for p in range(1, ntp):
            out = out + red[which, p]
        redo[which, t] = out
        send(TP, lambda p: redo.at[which, t], redo.at[which, t], ssem, rsem)

    def reduce_3(out_ref, which, ssem, rsem):
        arrive(TP, lambda p: redo.at[which, p], ssem, rsem)
        for p in range(ntp):
            out_ref[p * share : (p + 1) * share, :] = redo[which, p]

    for i in later:
        weight_block(i)
    reduce_1(accr, 0, s_c1, r_c1)
    for i in early[3:4]:
        weight_relay(i)
    for i in early[1:3]:
        weight_rows(i)
    back_steps(2 if nz == 8 else 0)
    exchange_5(h_in, s_h4, r_h4)

    def states_back(i, run):
        k = chunks - 1 - i
        rows = at_chunk(k)
        hst[k] = run
        accw[rows, :] = dot(sumd[k].astype(BF16), c_ref[rows, :], 0, 0) + dot(
            (xb[rows, :].astype(F32) * endb[rows, :]).astype(BF16), run.astype(BF16), 1, 1
        )
        return totb[k] * run + hcb[k]

    lax.fori_loop(0, chunks, states_back, h_in[...].astype(F32))
    reduce_1(accw, 1, s_w1, r_w1)
    for i in early[4:]:
        weight_relay(i)

    def finish(k, _):
        rows = at_chunk(k)
        grad_y = dyb[rows, :]
        run = hst[k]
        write = endb[rows, :] * sum(dot(b_ref[rows, :], part) for part in pieces(run, 2))
        gin[rows, :] = (skip_row * grad_y + dxi[rows, :] + write).astype(BF16)
        leaving = xb[rows, :].astype(F32) * write
        arriving = grad_y * startb[rows, :] * rsb[rows, :]
        seg = segc[k] + head_sums(arriving - leaving)
        final = jnp.sum(leaving, axis=0, keepdims=True) + totb[k] * jnp.sum(
            run * stb[k], axis=0, keepdims=True
        )
        final = head_sums(jnp.broadcast_to(final, (8, width)))[0:1]
        whole = sum(dot(upper, part) for part in pieces(seg, 2)) + final
        sumd[k, 0:SLOT, :] = whole.T
        return 0

    lax.fori_loop(0, chunks // 2, finish, 0)
    for i in later[:1]:
        weight_relay(i)
    for i in early[3:4]:
        weight_rows(i)
    back_steps(2 if nz == 8 else 0)
    lax.fori_loop(chunks // 2, chunks, finish, 0)
    for k in range(chunks):
        gdecay[:, k * L : (k + 1) * L] = sumd[k, 0:heads, :]
    for i in later[1:2]:
        weight_relay(i)
    for i in early[4:]:
        weight_rows(i)
    reduce_2(0, s_c1, r_c1, s_c2, r_c2)
    reduce_2(1, s_w1, r_w1, s_w2, r_w2)
    for i in later[2:]:
        weight_relay(i)
    arrive(Z, lambda p: gz.at[p], s_gz, r_gz)
    row = gz[0]
    for k in range(1, nz):
        row = row + gz[k]
    ggain[...] = row[0:1]
    gskip[...] = head_sums(jnp.concatenate([row, jnp.zeros((6, width), F32)], axis=0))[1:2, 0:heads]
    back_steps(nz)
    for i in later[:-1]:
        weight_rows(i)
    reduce_3(gread, 0, s_c2, r_c2)
    reduce_3(gwrite, 1, s_w2, r_w2)
    weight_rows(nz)
    back_finish()
    for copy in pending:
        copy.wait_send()


def copy_out(*refs):
    count = 8
    sources, targets, scratch, sem_in, sem_out = (
        refs[:count],
        refs[count : 2 * count],
        refs[2 * count : -2],
        refs[-2],
        refs[-1],
    )
    large = [k for k in range(count) if k not in (5, 6)]
    loads = [
        pltpu.make_async_copy(sources[k], scratch[i], sem_in.at[i]) for i, k in enumerate(large)
    ]
    stores = [
        pltpu.make_async_copy(scratch[i], targets[k], sem_out.at[i]) for i, k in enumerate(large)
    ]
    for load in loads:
        load.start()
    for k in (5, 6):
        targets[k][...] = sources[k][...].reshape(targets[k].shape)
    for load, store in zip(loads, stores):
        load.wait()
        store.start()
    for store in stores:
        store.wait()


def hand_out(outs):
    vmem = pl.BlockSpec(memory_space=pltpu.VMEM)
    hbm = pl.BlockSpec(memory_space=pl.ANY)
    specs = [vmem if k in (5, 6) else hbm for k in range(8)]
    shapes = [
        jax.ShapeDtypeStruct(o.shape[1:] if k in (5, 6) else o.shape, o.dtype)
        for k, o in enumerate(outs)
    ]
    large = [o for k, o in enumerate(outs) if k not in (5, 6)]
    done = pl.pallas_call(
        copy_out,
        out_shape=shapes,
        in_specs=specs,
        out_specs=specs,
        scratch_shapes=[pltpu.VMEM(o.shape, o.dtype) for o in large]
        + [pltpu.SemaphoreType.DMA((6,)), pltpu.SemaphoreType.DMA((6,))],
        name="hand_out",
    )(*outs)
    return (*done[:7], done[7].T)


def on_device(nx, nz, ntp, packed, expo, gate, write, read, decay, skip, gain, weight, cotangent):
    cot = cotangent.T
    tokens, width = gate.shape
    heads = decay.shape[0]
    model = weight.shape[1]
    shard = cot.shape[0]
    chunks = tokens // L
    n = write.shape[1]
    columns = model // (nx * nz)
    qrows, erows = n // nx, n // (nx * nz)
    share = tokens // ntp
    front = FRONT

    def wide(kind=F32):
        return pltpu.VMEM((tokens, width), kind)

    def exchange(kind):
        return [
            pltpu.VMEM((n, width), kind),
            pltpu.VMEM((nx, qrows, width), kind),
            pltpu.VMEM((nz, erows, width), F32),
            pltpu.VMEM((nz, erows, width), F32),
            pltpu.VMEM((nz, erows, width), F32),
            pltpu.VMEM((nz, erows, width), F32),
            pltpu.VMEM((nx, qrows, width), kind),
            pltpu.VMEM((n, width), kind),
        ]

    def sems(*shape):
        return [pltpu.SemaphoreType.DMA(shape), pltpu.SemaphoreType.DMA(shape)]

    scratch = [
        pltpu.VMEM((tokens, width), BF16),
        pltpu.VMEM((width, model), BF16),
        pltpu.VMEM((model, tokens), BF16),
        wide(BF16),
        *[wide() for _ in range(7)],
        wide(BF16),
        pltpu.VMEM((chunks, SLOT, L), F32),
        pltpu.VMEM((chunks, L, SLOT), F32),
        pltpu.VMEM((chunks, 1, width), F32),
        pltpu.VMEM((chunks, heads, L, L), F32),
        pltpu.VMEM((chunks, L, L), F32),
        pltpu.VMEM((chunks, n, width), F32),
        pltpu.VMEM((chunks, n, width), F32),
        pltpu.VMEM((chunks, n, width), F32),
        pltpu.VMEM((chunks, n, width), F32),
        pltpu.VMEM((chunks, L, L), F32),
        pltpu.VMEM((chunks, SLOT, L), F32),
        pltpu.VMEM((chunks, L, SLOT), F32),
        wide(),
        *exchange(F32),
        *exchange(BF16),
        pltpu.VMEM((qrows, width), F32),
        pltpu.VMEM((nx, 1, width), F32),
        pltpu.VMEM((nz, 1, width), F32),
        pltpu.VMEM((ntp, 8, L), F32),
        pltpu.VMEM((L, 128), F32),
        pltpu.VMEM((nx, 2, width), F32),
        pltpu.VMEM((nz, 2, width), F32),
        pltpu.VMEM((nz, shard, front), BF16),
        pltpu.VMEM((nz, shard, width - front), BF16),
        *[pltpu.VMEM((nz, columns, front), BF16) for _ in range(6)],
        *[pltpu.VMEM((nz, shard, width - front), BF16) for _ in range(2)],
        *[pltpu.VMEM((nx, columns, width - front), BF16) for _ in range(2)],
        pltpu.VMEM((tokens, n), F32),
        pltpu.VMEM((tokens, n), F32),
        pltpu.VMEM((2, ntp, share, n), F32),
        pltpu.VMEM((2, ntp, share, n), F32),
        pltpu.SemaphoreType.DMA((3,)),
        *sems(10),
        *sems(nx),
        *sems(nz),
        *(sems(nx) + sems(nz) + sems(nz) + sems(nx)),
        *(sems(nx) + sems(nz) + sems(nz) + sems(nx)),
        *sems(ntp),
        *sems(nx),
        *sems(nz),
        *sems(3, nz),
        *sems(nz),
        *sems(nz),
        *sems(nx),
        *(sems(ntp) * 4),
    ]
    vmem = pl.BlockSpec(memory_space=pltpu.VMEM)
    hbm = pl.BlockSpec(memory_space=pl.ANY)
    outs = pl.pallas_call(
        functools.partial(core, nx, nz, ntp),
        out_shape=(
            jax.ShapeDtypeStruct((tokens, width), BF16),
            jax.ShapeDtypeStruct((tokens, width), BF16),
            jax.ShapeDtypeStruct((tokens, n), F32),
            jax.ShapeDtypeStruct((tokens, n), F32),
            jax.ShapeDtypeStruct((heads, tokens), F32),
            jax.ShapeDtypeStruct((1, heads), F32),
            jax.ShapeDtypeStruct((1, width), F32),
            jax.ShapeDtypeStruct((columns, width), F32),
        ),
        in_specs=[vmem, vmem, hbm, vmem, vmem, vmem, pl.BlockSpec(memory_space=pltpu.SMEM), vmem, hbm, hbm],
        out_specs=(vmem,) * 8,
        scratch_shapes=scratch,
        compiler_params=pltpu.CompilerParams(
            collective_id=0, has_side_effects=True, vmem_limit_bytes=60 * 1024 * 1024
        ),
        name="layer_backward",
    )(packed, expo, gate, write, read, decay, skip[None, :], gain, weight, cot)
    return hand_out(outs)


def solution(mesh):
    ntp = mesh.shape["tp"]
    nz = mesh.shape["seq"] // NX
    return jax.shard_map(
        functools.partial(on_device, NX, nz, ntp),
        mesh=mesh,
        in_specs=(
            P("seq", "tp"),
            P("tp", "seq"),
            P("seq", "tp"),
            P("seq", None),
            P("seq", None),
            P("tp", "seq"),
            P("tp"),
            P("tp"),
            P("tp", None),
            P("seq", "tp"),
        ),
        out_specs=(
            P("seq", "tp"),
            P("seq", "tp"),
            P("seq", None),
            P("seq", None),
            P("tp", "seq"),
            P("tp"),
            P("tp"),
            P("tp", "seq"),
        ),
        check_vma=False,
    )
```

```python
import functools

import jax
import jax.numpy as jnp
from jax import lax
from jax.experimental import pallas as pl
from jax.experimental.pallas import tpu as pltpu
from jax.sharding import PartitionSpec as P

MESH = pl.DeviceIdType.MESH
F32, BF16 = jnp.float32, jnp.bfloat16
EXACT = lax.Precision.HIGHEST
NX = 4
L = 128
HEAD = 64
SLOT = 16
FRONT = 384


def dot(a, b, ca=1, cb=0, precision=None):
    return lax.dot_general(
        a, b, (((ca,), (cb,)), ((), ())), preferred_element_type=F32, precision=precision
    )


def pieces(v, count):
    out = []
    for _ in range(count):
        part = v.astype(BF16)
        out.append(part)
        v = v - part.astype(F32)
    return out


def iota(shape, dim):
    return lax.broadcasted_iota(jnp.int32, shape, dim)


def rcopy(src, dst, send, recv, dev):
    return pltpu.make_async_remote_copy(
        src_ref=src, dst_ref=dst, send_sem=send, recv_sem=recv, device_id=dev, device_id_type=MESH
    )


def core(nx, nz, ntp, packed, expo, gate_hbm, b_ref, c_ref, ld_ref, skip_ref, gain_ref, w_hbm, cot_hbm,
         gin, ggate, gwrite, gread, gdecay, gskip, ggain, gow, *scratch):
    (gate_v, w_v, cot, xb, yb, gvb, mixb, dyb, rsb, endb, startb,
     normed, act, gvg, xe, accp, csr, csc, totb, dec, cross, gb, stb, hcb, hst, sumd, segr, segc, dxi,
     sloc, lb, tb, ub, qs, qb, vs, s_in,
     rloc, lb2, tb2, ub2, qs2, qb2, vs2, h_in,
     vtop, dxs, dzs, sums, totc, gx, gz, pwa, pwb, xa, xd, xm, xc, zsa, zra, zsb, zrb, xsb, xrb, accw, accr, red, redo,
     cp_sem, s_ag, r_ag, s_dx, r_dx, s_dz, r_dz,
     s_p1, r_p1, s_p2, r_p2, s_p3, r_p3, s_p4, r_p4,
     s_h1, r_h1, s_h2, r_h2, s_h3, r_h3, s_h4, r_h4,
     s_tp, r_tp, s_gx, r_gx, s_gz, r_gz, s_rx, r_rx, s_za, r_za, s_zb, r_zb, s_xb, r_xb,
     s_w1, r_w1, s_w2, r_w2, s_c1, r_c1, s_c2, r_c2) = scratch
    tokens, width = xb.shape
    chunks = tokens // L
    pairs = width // 128
    heads = width // HEAD
    total_width = width * ntp
    ny = ntp // 2
    qrows, erows = 128 // nx, 128 // (nx * nz)
    s = lax.axis_index("seq")
    t = lax.axis_index("tp")
    z, x = lax.div(s, nx), lax.rem(s, nx)
    y, half = lax.div(t, 2), lax.rem(t, 2)
    shard = cot.shape[0] // ntp

    def dev_x(p):
        return {"seq": z * nx + p, "tp": t}

    def dev_z(p):
        return {"seq": p * nx + x, "tp": t}

    def dev_t(p):
        return {"seq": s, "tp": p}

    X, Z, TP = (nx, x, dev_x), (nz, z, dev_z), (ntp, t, dev_t)
    pending = []

    def send(group, src_of, dst, whole, ssem, rsem):
        n, me, dev = group
        for d in range(1, n):
            p = lax.rem(me + d, n)
            rcopy(src_of(p), dst, ssem.at[0], rsem.at[0], dev(p)).start()
        if n > 1:
            pending.append(rcopy(whole, whole, ssem.at[0], rsem.at[0], dev(me)))

    def arrive(group, whole, ssem, rsem):
        n, me, dev = group
        if n > 1:
            rcopy(whole, whole, ssem.at[0], rsem.at[0], dev(me)).wait_recv()

    def slots(ref, n):
        return ref.at[pl.ds(0, n - 1)]

    def cot_rows(p, first=0, count=shard):
        return cot.at[pl.ds(pl.multiple_of(p * shard + first, 16), count)]

    load_cot = pltpu.make_async_copy(cot_hbm, cot_rows(t), cp_sem.at[0])
    load_gate = pltpu.make_async_copy(gate_hbm, gate_v, cp_sem.at[1])
    load_w = pltpu.make_async_copy(w_hbm, w_v, cp_sem.at[2])
    load_cot.start()
    load_gate.start()
    load_w.start()

    barrier = pltpu.get_barrier_semaphore()
    for n, me, dev in (X, Z, TP):
        for d in range(1, n):
            pl.semaphore_signal(
                barrier, inc=1, device_id=dev(lax.rem(me + d, n)), device_id_type=MESH
            )

    spread = (iota((SLOT, width), 1) // HEAD == iota((SLOT, width), 0)).astype(BF16)
    gather = (iota((width, SLOT), 0) // HEAD == iota((width, SLOT), 1)).astype(BF16)
    upper = (iota((L, L), 0) <= iota((L, L), 1)).astype(BF16)
    causal = iota((L, L), 0) >= iota((L, L), 1)
    left = iota((L, 128), 1) < HEAD

    def spread_heads(v):
        return sum(dot(part, spread) for part in pieces(v, 3))

    def head_sums(v):
        return sum(dot(part, gather) for part in pieces(v, 2))

    csr[...] = jnp.zeros_like(csr)
    segr[...] = jnp.zeros_like(segr)
    for k in range(chunks):
        csr[k, 0:heads, :] = ld_ref[:, k * L : (k + 1) * L]
    rows = csr[...].reshape(chunks * SLOT, L)
    rows = sum(dot(part, upper) for part in pieces(rows, 3))
    log_total = jnp.zeros((1, width), F32)
    for k in range(chunks):
        csr[k] = rows[k * SLOT : (k + 1) * SLOT, :]
        cols = rows[k * SLOT : (k + 1) * SLOT, :].T
        csc[k] = cols
        logs = spread_heads(cols)
        last = logs[L - 1 : L, :]
        log_total = log_total + last
        totb[k] = jnp.exp(last)
        endb[k * L : (k + 1) * L, :] = jnp.exp(last - logs)
        startb[k * L : (k + 1) * L, :] = jnp.exp(logs)
    dxs[x] = jnp.exp(log_total)

    powers = lax.shift_left(jnp.ones_like(expo[...]), expo[...] + 5).astype(F32) * (1.0 / 32.0)
    nibble = 4 * iota((8, width), 0)
    for k in range(chunks):
        factor_rows = jnp.concatenate(
            [powers[:, k * L : (k + 1) * L], jnp.zeros((8 - pairs, L), F32)], axis=0
        )
        factor = factor_rows.T
        wide = jnp.concatenate(
            [jnp.broadcast_to(factor[:, p : p + 1], (L, 128)) for p in range(pairs)], axis=1
        )
        words = packed[k * (L // 8) : (k + 1) * (L // 8), :]
        fields = jnp.concatenate(
            [
                lax.bitwise_and(
                    lax.shift_right_arithmetic(
                        jnp.broadcast_to(words[r : r + 1, :], (8, width)), nibble
                    ),
                    15,
                )
                - 8
                for r in range(L // 8)
            ],
            axis=0,
        )
        xb[k * L : (k + 1) * L, :] = (fields.astype(F32) * wide).astype(BF16)

    run = jnp.zeros((128, width), F32)
    for k in range(chunks):
        rows = slice(k * L, (k + 1) * L)
        weighted = xb[rows, :].astype(F32) * endb[rows, :]
        parts = pieces(weighted, 2)
        xe[rows, :] = parts[0]
        gb[k] = sum(dot(b_ref[rows, :], part, 0, 0) for part in parts)
        run = totb[k] * run + gb[k]
    sloc[...] = run

    def take_rows(ref, at, count):
        return ref[pl.ds(pl.multiple_of(at * count, count), count), :]

    def exchange_1(own, lbuf, ssem, rsem):
        send(
            X,
            lambda p: own.at[pl.ds(pl.multiple_of(p * qrows, qrows), qrows)],
            lbuf.at[x],
            slots(lbuf, nx),
            ssem,
            rsem,
        )
        lbuf[x] = take_rows(own, x, qrows)

    pl.semaphore_wait(barrier, (nx - 1) + (nz - 1) + (ntp - 1))
    send(X, lambda p: dxs.at[x], dxs.at[x], slots(dxs, nx), s_dx, r_dx)
    exchange_1(sloc, lb, s_p1, r_p1)

    load_cot.wait()
    part = shard // 2
    sibling = 2 * y + 1 - half
    after = 2 * lax.rem(y + 1, ny) + half
    before = 2 * lax.rem(y + ny - 1, ny) + half
    across = 2 * lax.rem(y + 2, ny) + half

    def cot_copy(j, p, to, first=0, count=shard):
        return rcopy(cot_rows(p, first, count), cot_rows(p, first, count), s_ag.at[0], r_ag.at[j], dev_t(to))

    def cot_send(j, p, to, *rows):
        cot_copy(j, p, to, *rows).start()

    def cot_wait(j, p, *rows):
        cot_copy(j, p, sibling, *rows).wait_recv()

    cot_send(0, t, sibling)
    if ny == 2:
        cot_send(1, t, after)
    elif ny == 4:
        cot_send(1, t, after, 0, part)
        cot_send(3, t, before, part, part)
        cot_send(2, t, after, part, part)
        cot_send(4, t, before, 0, part)

    def relay_cot():
        if ny == 4:
            cot_wait(1, before, 0, part)
            cot_send(5, before, after, 0, part)
            cot_wait(3, after, part, part)
            cot_send(6, after, before, part, part)

    def near_cot():
        if ny == 2:
            cot_wait(1, after)
            cot_send(7, after, sibling)
        elif ny == 4:
            cot_wait(2, before, part, part)
            cot_send(7, before, sibling)
            cot_wait(4, after, 0, part)
            cot_send(8, after, sibling)

    def far_cot():
        if ny == 4:
            cot_wait(5, across, 0, part)
            cot_wait(6, across, part, part)
            cot_send(9, across, sibling)

    def project(chip, first=False):
        terms = dot(
            cot[pl.ds(pl.multiple_of(chip * 2 * shard, 128), 2 * shard), :],
            w_v[:, pl.ds(pl.multiple_of(chip * 2 * shard, 128), 2 * shard)],
            0,
            1,
        )
        gvb[...] = terms if first else gvb[...] + terms

    def other(p):
        return p + 1 - 2 * half

    def exchange_2(lbuf, tbuf, ubuf, s1, r1, ssem, rsem, backward):
        arrive(X, slots(lbuf, nx), s1, r1)
        order = range(nx - 1, -1, -1) if backward else range(nx)
        row = None
        for k in order:
            add = lbuf[k].astype(F32)
            row = add if row is None else dxs[k] * row + add
        for k in range(nz):
            tbuf[k] = row[k * erows : (k + 1) * erows, :]
        send(Z, lambda p: tbuf.at[p], ubuf.at[z], slots(ubuf, nz), ssem, rsem)
        ubuf[z] = tbuf[z]

    def exchange_3(ubuf, qsend, qbuf, s2, r2, ssem, rsem, backward):
        arrive(Z, slots(ubuf, nz), s2, r2)
        order = range(nz - 1, -1, -1) if backward else range(nz)
        row = jnp.zeros((erows, width), F32)
        for k in order:
            qsend[k] = row
            row = dzs[k] * row + ubuf[k]
        send(Z, lambda p: qsend.at[p], qbuf.at[z], slots(qbuf, nz), ssem, rsem)
        qbuf[z] = qsend[z]

    def exchange_4(qbuf, lbuf, vsend, result, s3, r3, ssem, rsem, backward):
        arrive(Z, slots(qbuf, nz), s3, r3)
        for k in range(nz):
            vtop[k * erows : (k + 1) * erows, :] = qbuf[k]
        order = range(nx - 1, -1, -1) if backward else range(nx)
        row = vtop[...]
        for k in order:
            vsend[k] = row.astype(vsend.dtype)
            row = dxs[k] * row + lbuf[k].astype(F32)
        mine = result.at[pl.ds(pl.multiple_of(x * qrows, qrows), qrows)]
        send(X, lambda p: vsend.at[p], mine, result.at[pl.ds(0, (nx - 1) * qrows)], ssem, rsem)
        result[pl.ds(pl.multiple_of(x * qrows, qrows), qrows), :] = vsend[x]

    def exchange_5(result, s4, r4):
        arrive(X, result.at[pl.ds(0, (nx - 1) * qrows)], s4, r4)


    skip_row = jnp.zeros((1, width), F32)
    head_of = iota((1, width), 1) // HEAD
    for h in range(heads):
        skip_row = jnp.where(head_of == h, skip_ref[0, h], skip_row)

    def at_chunk(k):
        return pl.ds(pl.multiple_of(k * L, L), L)

    def split_pair(v):
        zero = jnp.zeros_like(v)
        return jnp.concatenate([jnp.where(left, v, zero), jnp.where(left, zero, v)], axis=0)

    def inside(k, _):
        rows = at_chunk(k)
        both = dot(c_ref[rows, :], b_ref[rows, :], 1, 1)
        cross[k] = both
        for p in range(pairs):
            mixing = []
            for h in (2 * p, 2 * p + 1):
                spread_log = csc[k][:, h : h + 1] - csr[k][h : h + 1, :]
                decay = jnp.where(causal, jnp.exp(jnp.minimum(spread_log, 0.0)), 0.0)
                dec[k, h] = decay
                mixing.append(pieces(decay * both, 2))
            lanes = slice(128 * p, 128 * (p + 1))
            x_pair = xb[rows, lanes]
            x_split = split_pair(x_pair)
            yb[rows, lanes] = (
                dot(jnp.concatenate([m[0] for m in mixing], axis=1), x_split)
                + dot(jnp.concatenate([m[1] for m in mixing], axis=1), x_split)
                + skip_row[:, lanes] * x_pair.astype(F32)
            )
        return 0

    lax.fori_loop(0, chunks // 2, inside, 0)
    load_w.wait()
    cot_wait(0, sibling)
    project(y, True)
    arrive(X, slots(dxs, nx), s_dx, r_dx)
    row = dxs[0]
    for k in range(1, nx):
        row = row * dxs[k]
    dzs[z] = row
    send(Z, lambda p: dzs.at[z], dzs.at[z], slots(dzs, nz), s_dz, r_dz)

    exchange_2(lb, tb, ub, s_p1, r_p1, s_p2, r_p2, False)
    relay_cot()
    lax.fori_loop(chunks // 2, chunks, inside, 0)
    arrive(Z, slots(dzs, nz), s_dz, r_dz)
    exchange_3(ub, qs, qb, s_p2, r_p2, s_p3, r_p3, False)
    near_cot()
    exchange_4(qb, lb, vs, s_in, s_p3, r_p3, s_p4, r_p4, False)
    far_cot()
    if ny == 2:
        cot_wait(7, other(after))
        project(lax.rem(y + 1, ny))
    elif ny == 4:
        cot_wait(7, other(before))
        project(lax.rem(y + 3, ny))
        cot_wait(8, other(after))
        project(lax.rem(y + 1, ny))
    load_gate.wait()
    if ny == 4:
        cot_wait(9, other(across))
        project(lax.rem(y + 2, ny))
    gain_row = gain_ref[...].reshape(1, width)

    def prepare(k, _):
        rows = at_chunk(k)
        gate = gate_v[rows, :].astype(F32)
        act[rows, :] = gate * jax.nn.sigmoid(gate)
        gvg[rows, :] = gvb[rows, :] * gain_row
        return 0

    lax.fori_loop(0, chunks, prepare, 0)
    exchange_5(s_in, s_p4, r_p4)
    stb[0] = s_in[...].astype(F32)
    for k in range(1, chunks):
        stb[k] = totb[k - 1] * stb[k - 1] + gb[k - 1]
    lane = iota((L, 128), 1)

    def sums_of(k, acc):
        rows = at_chunk(k)
        start = sum(dot(c_ref[rows, :], part) for part in pieces(stb[k], 2))
        rsb[rows, :] = start
        y_now = yb[rows, :] + startb[rows, :] * start
        yb[rows, :] = y_now
        mixed = y_now * act[rows, :]
        mixb[rows, :] = mixed
        square = jnp.sum(mixed * mixed, axis=1, keepdims=True)
        inner = jnp.sum(gvg[rows, :] * mixed, axis=1, keepdims=True)
        return jnp.where(lane == 2 * k, square, jnp.where(lane == 2 * k + 1, inner, acc))

    packed_sums = lax.fori_loop(0, chunks, sums_of, jnp.zeros((L, 128), F32))
    sums[t] = packed_sums.T[0:8, :]
    send(TP, lambda p: sums.at[t], sums.at[t], slots(sums, ntp), s_tp, r_tp)
    arrive(TP, slots(sums, ntp), s_tp, r_tp)

    both = sums[0]
    for p in range(1, ntp):
        both = both + sums[p]
    totc[...] = jnp.concatenate([both, jnp.zeros((120, L), F32)], axis=0).T

    def token_scales(k):
        both = totc[...]
        square = jnp.sum(jnp.where(lane == 2 * k, both, 0.0), axis=1, keepdims=True)
        inner = jnp.sum(jnp.where(lane == 2 * k + 1, both, 0.0), axis=1, keepdims=True)
        return lax.rsqrt(square / total_width + 1e-05), inner

    def gradients(k, _):
        rows = at_chunk(k)
        scale, inner = token_scales(k)
        grad_mixed = scale * gvg[rows, :] - mixb[rows, :] * (
            (scale * scale * scale) * inner / total_width
        )
        grad_y = grad_mixed * act[rows, :]
        dyb[rows, :] = grad_y
        scaled = grad_y * startb[rows, :]
        hcb[k] = sum(dot(c_ref[rows, :], part, 0, 0) for part in pieces(scaled, 2))
        return 0

    lax.fori_loop(0, chunks, gradients, 0)
    run = hcb[chunks - 1]
    for k in range(chunks - 2, -1, -1):
        run = totb[k] * run + hcb[k]
    rloc[...] = run.astype(BF16)
    exchange_1(rloc, lb2, s_h1, r_h1)

    def gate_gradients(k, carry):
        gain_sum, skip_sum = carry
        rows = at_chunk(k)
        scale, inner = token_scales(k)
        mixed = mixb[rows, :]
        gate = gate_v[rows, :].astype(F32)
        sigma = jax.nn.sigmoid(gate)
        scaled_mixed = mixed * scale
        normed[rows, :] = (scaled_mixed * gain_row).astype(BF16)
        grad_mixed = scale * gvg[rows, :] - mixed * (
            (scale * scale * scale) * inner / total_width
        )
        ggate[rows, :] = (
            grad_mixed * yb[rows, :] * sigma * (1.0 + gate * (1.0 - sigma))
        ).astype(BF16)
        gain_sum = gain_sum + jnp.sum(gvb[rows, :] * scaled_mixed, axis=0, keepdims=True)
        skip_sum = skip_sum + jnp.sum(
            dyb[rows, :] * xb[rows, :].astype(F32), axis=0, keepdims=True
        )
        return gain_sum, skip_sum

    zero_row = jnp.zeros((1, width), F32)
    gain_sum, skip_sum = lax.fori_loop(0, chunks, gate_gradients, (zero_row, zero_row))
    gx[x, 0:1, :] = gain_sum
    gx[x, 1:2, :] = skip_sum
    send(X, lambda p: gx.at[x], gx.at[x], slots(gx, nx), s_gx, r_gx)

    columns = shard // nx
    front = pwa.shape[2]
    middle = nz // 2
    steps = sorted(range(1, nz), key=lambda i: -min(i, nz - i)) + [nz]

    def block_of(i):
        return lax.rem(z + i, nz)

    def mine_of(i, p):
        return pwa.at[block_of(i), pl.ds(pl.multiple_of(p * columns, columns), columns)]

    def sides(i):
        one, two = lax.rem(x + 1, nx), lax.rem(x + nx - 1, nx)
        return (one, two) if steps.index(i) % 2 == 0 else (two, one)

    def weight_copy(kind, i, to):
        source = (mine_of(i, lax.rem(x + 2, nx)), mine_of(i, to), xm.at[i - 1])[kind]
        target = (xa, xd, xc)[kind].at[i - 1]
        return rcopy(source, target, s_rx.at[kind], r_rx.at[kind, i - 1], dev_x(to))

    def weight_send(kind, i, to):
        weight_copy(kind, i, to).start()

    def weight_block(i):
        k = block_of(i)
        terms = dot(cot[pl.ds(pl.multiple_of(k * shard, shard), shard), :], normed[...]).astype(BF16)
        pwa[k] = terms[:, :front]
        pwb[k] = terms[:, front:]
        near, far = sides(i)
        if nx == 4:
            weight_send(0, i, near)
        if nx > 1:
            weight_send(1, i, far)

    def weight_relay(i):
        near, _ = sides(i)
        if nx == 4:
            weight_copy(0, i, near).wait_recv()
            xm[i - 1] = (xa[i - 1].astype(F32) + mine_of(i, near)[...].astype(F32)).astype(BF16)
            weight_send(2, i, near)

    def ring_part(kind, i, up):
        rows = (columns, shard)[kind]
        cut = 16 * (3 * rows // 80)
        return (0, rows) if i != middle else (0, cut) if up else (cut, rows)

    def ring_copy(kind, i, up):
        first, end = ring_part(kind, i, up)
        slot = i - 1 if i != middle or up else nz - 1
        sends, lands, s_z, r_z = ((zsa, zra, s_za, r_za), (zsb, zrb, s_zb, r_zb))[kind]
        return rcopy(
            sends.at[i - 1, pl.ds(first, end - first)],
            lands.at[i - 1, pl.ds(first, end - first)],
            s_z.at[0],
            r_z.at[slot],
            dev_z(lax.rem(z + (1 if up else nz - 1), nz)),
        )

    def ring_add(kind, out, i, up):
        ring_copy(kind, i, up).wait_recv()
        first, end = ring_part(kind, i, up)
        part = (zra, zrb)[kind][i - 1, first:end, :].astype(F32)
        parts = [out[:first]] if first else []
        parts.append(out[first:end] + part)
        if end < out.shape[0]:
            parts.append(out[end:])
        return jnp.concatenate(parts, axis=0) if len(parts) > 1 else parts[0]

    def ring_step(kind, i, out):
        if i % nz < middle:
            out = ring_add(kind, out, i % nz + 1, True)
        if i > middle:
            out = ring_add(kind, out, i - 1, False)
        if i < nz:
            (zsa, zsb)[kind][i - 1] = out.astype(BF16)
            for up in (True, False):
                if i == middle or (i < middle) == up:
                    ring_copy(kind, i, up).start()
        return out

    def weight_rows(i):
        near, far = sides(i)
        out = mine_of(i, x)[...].astype(F32)
        if nx > 1:
            weight_copy(1, i, far).wait_recv()
            out = out + xd[i - 1].astype(F32)
        if nx == 4:
            weight_copy(2, i, near).wait_recv()
            out = out + xc[i - 1].astype(F32)
        out = ring_step(0, i, out)
        if i == nz:
            gow[:, :front] = out

    def back_rows(i):
        out = ring_step(1, i, pwb[block_of(i)].astype(F32))
        if i == nz:
            for p in range(nx):
                xsb[p] = out[p * columns : (p + 1) * columns, :].astype(BF16)
            send(X, lambda p: xsb.at[p], xrb.at[x], slots(xrb, nx), s_xb, r_xb)
            xrb[x] = xsb[x]

    def back_finish():
        arrive(X, slots(xrb, nx), s_xb, r_xb)
        out = xrb[0].astype(F32)
        for p in range(1, nx):
            out = out + xrb[p].astype(F32)
        gow[:, front:] = out

    early, later = steps[: (5 * nz) // 8], steps[(5 * nz) // 8 :]
    order = iter(steps)

    def back_steps(count):
        for _ in range(count):
            i = next(order, None)
            if i is not None:
                back_rows(i)

    for n, i in enumerate(steps):
        weight_block(i)
        if n == 0:
            back_steps(1)
    exchange_2(lb2, tb2, ub2, s_h1, r_h1, s_h2, r_h2, True)
    arrive(X, slots(gx, nx), s_gx, r_gx)
    row = gx[0]
    for k in range(1, nx):
        row = row + gx[k]
    gz[z] = row
    send(Z, lambda p: gz.at[z], gz.at[z], slots(gz, nz), s_gz, r_gz)

    def inside_back(k, _):
        rows = at_chunk(k)
        both = cross[k]
        summed = jnp.zeros((L, L), F32)
        lane = iota((L, SLOT), 1)
        row_sums = jnp.zeros((L, SLOT), F32)
        for p in range(pairs):
            lanes = slice(128 * p, 128 * (p + 1))
            x_pair = xb[rows, lanes]
            high, low = pieces(dyb[rows, lanes], 2)
            grads = split_pair(high)
            dots = dot(grads, x_pair, 1, 1) + dot(split_pair(low), x_pair, 1, 1)
            mixing = []
            for i in range(2):
                h = 2 * p + i
                decay = dec[k, h]
                weighted = dots[i * L : (i + 1) * L, :] * decay
                summed = summed + weighted
                terms = weighted * both
                row_sums = row_sums + jnp.where(
                    lane == h, jnp.sum(terms, axis=1, keepdims=True), 0.0
                )
                segr[k, h : h + 1, :] = jnp.sum(terms, axis=0, keepdims=True)
                mixing.append((decay * both).astype(BF16))
            dxi[rows, lanes] = dot(jnp.concatenate(mixing, axis=0), grads, 0, 0)
        accp[rows, :] = dot(summed.astype(BF16), c_ref[rows, :], 0, 0)
        segc[k] = row_sums - segr[k].T
        scaled = dyb[rows, :] * startb[rows, :]
        accr[rows, :] = (
            dot(summed.astype(BF16), b_ref[rows, :])
            + dot(scaled.astype(BF16), stb[k].astype(BF16), 1, 1)
        ).astype(BF16)
        return 0

    lax.fori_loop(0, chunks // 2, inside_back, 0)
    back_steps(2 if nz == 8 else 0)
    exchange_3(ub2, qs2, qb2, s_h2, r_h2, s_h3, r_h3, True)
    lax.fori_loop(chunks // 2, chunks, inside_back, 0)
    back_steps(2 if nz == 8 else 0)
    for i in early[:3]:
        weight_relay(i)
    exchange_4(qb2, lb2, vs2, h_in, s_h3, r_h3, s_h4, r_h4, True)

    share = tokens // ntp

    def reduce_1(acc, which, ssem, rsem):
        send(
            TP,
            lambda p: acc.at[pl.ds(pl.multiple_of(p * share, share), share)],
            red.at[which, t],
            red.at[which, pl.ds(0, ntp - 1)],
            ssem,
            rsem,
        )
        red[which, t] = take_rows(acc, t, share)

    def reduce_2(which, s1, r1, ssem, rsem):
        arrive(TP, red.at[which, pl.ds(0, ntp - 1)], s1, r1)
        out = red[which, 0].astype(F32)
        for p in range(1, ntp):
            out = out + red[which, p].astype(F32)
        redo[which, t] = out
        send(TP, lambda p: redo.at[which, t], redo.at[which, t], redo.at[which, pl.ds(0, ntp - 1)], ssem, rsem)

    def reduce_3(out_ref, which, ssem, rsem):
        arrive(TP, redo.at[which, pl.ds(0, ntp - 1)], ssem, rsem)
        for p in range(ntp):
            out_ref[p * share : (p + 1) * share, :] = redo[which, p]

    reduce_1(accr, 0, s_c1, r_c1)
    for i in early[:1]:
        weight_rows(i)
    for i in early[3:]:
        weight_relay(i)
    for i in early[1:3]:
        weight_rows(i)
    for i in later:
        weight_relay(i)
    back_steps(2 if nz == 8 else 0)
    exchange_5(h_in, s_h4, r_h4)

    def states_back(i, run):
        k = chunks - 1 - i
        rows = at_chunk(k)
        hst[k] = run
        accw[rows, :] = (accp[rows, :] + dot(xe[rows, :], run.astype(BF16), 1, 1)).astype(BF16)
        return totb[k] * run + hcb[k]

    lax.fori_loop(0, chunks, states_back, h_in[...].astype(F32))
    reduce_1(accw, 1, s_w1, r_w1)
    for i in early[3:]:
        weight_rows(i)

    def finish(k, _):
        rows = at_chunk(k)
        grad_y = dyb[rows, :]
        run = hst[k]
        write = endb[rows, :] * sum(dot(b_ref[rows, :], part) for part in pieces(run, 2))
        gin[rows, :] = (skip_row * grad_y + dxi[rows, :] + write).astype(BF16)
        leaving = xb[rows, :].astype(F32) * write
        arriving = grad_y * startb[rows, :] * rsb[rows, :]
        seg = segc[k] + head_sums(arriving - leaving)
        final = jnp.sum(leaving, axis=0, keepdims=True) + totb[k] * jnp.sum(
            run * stb[k], axis=0, keepdims=True
        )
        final = head_sums(jnp.broadcast_to(final, (8, width)))[0:1]
        whole = sum(dot(upper, part) for part in pieces(seg, 2)) + final
        sumd[k] = whole.T
        return 0

    lax.fori_loop(0, chunks // 2, finish, 0)
    reduce_2(0, s_c1, r_c1, s_c2, r_c2)
    back_steps(nz)
    lax.fori_loop(chunks // 2, chunks, finish, 0)
    for k in range(chunks):
        gdecay[:, k * L : (k + 1) * L] = sumd[k, 0:heads, :]
    reduce_2(1, s_w1, r_w1, s_w2, r_w2)
    for i in later[:-1]:
        weight_rows(i)
    arrive(Z, slots(gz, nz), s_gz, r_gz)
    row = gz[0]
    for k in range(1, nz):
        row = row + gz[k]
    ggain[...] = row[0:1]
    gskip[...] = head_sums(jnp.concatenate([row, jnp.zeros((6, width), F32)], axis=0))[1:2, 0:heads]
    reduce_3(gread, 0, s_c2, r_c2)
    back_finish()
    weight_rows(nz)
    reduce_3(gwrite, 1, s_w2, r_w2)
    for copy in pending:
        copy.wait_send()

    def all_left(whole, sem):
        rcopy(whole, whole, sem, r_ag.at[0], dev_t(sibling)).wait_send()

    all_left(cot.at[pl.ds(0, (2 * ny - 1) * shard)], s_ag.at[0])
    for kind in range(3):
        if nx == 4 or (nx > 1 and kind == 1):
            all_left(xa, s_rx.at[kind])
    all_left(slots(zra, nz), s_za.at[0])
    all_left(slots(zrb, nz), s_zb.at[0])


def copy_out(*refs):
    count = 8
    sources, targets, sem = refs[:count], refs[count : 2 * count], refs[-1]
    stores = [
        pltpu.make_async_copy(sources[k], targets[k], sem.at[k])
        for k in range(count)
        if k not in (5, 6)
    ]
    for store in stores:
        store.start()
    for k in (5, 6):
        targets[k][...] = sources[k][...].reshape(targets[k].shape)
    for store in stores:
        store.wait()


def hand_out(outs):
    vmem = pl.BlockSpec(memory_space=pltpu.VMEM)
    hbm = pl.BlockSpec(memory_space=pl.ANY)
    shapes = [
        jax.ShapeDtypeStruct(o.shape[1:] if k in (5, 6) else o.shape, o.dtype)
        for k, o in enumerate(outs)
    ]
    done = pl.pallas_call(
        copy_out,
        out_shape=shapes,
        in_specs=[vmem] * 8,
        out_specs=[vmem if k in (5, 6) else hbm for k in range(8)],
        scratch_shapes=[pltpu.SemaphoreType.DMA((8,))],
        name="hand_out",
    )(*[pltpu.with_memory_space_constraint(o, pltpu.VMEM) for o in outs])
    return (*done[:7], done[7].T)


def on_device(nx, nz, ntp, packed, expo, gate, write, read, decay, skip, gain, weight, cotangent):
    cot = cotangent.T
    tokens, width = gate.shape
    heads = decay.shape[0]
    model = weight.shape[1]
    shard = cot.shape[0]
    chunks = tokens // L
    n = write.shape[1]
    columns = model // (nx * nz)
    qrows, erows = n // nx, n // (nx * nz)
    share = tokens // ntp
    front = FRONT

    def wide(kind=F32):
        return pltpu.VMEM((tokens, width), kind)

    def exchange(kind):
        return [
            pltpu.VMEM((n, width), kind),
            pltpu.VMEM((nx, qrows, width), kind),
            pltpu.VMEM((nz, erows, width), F32),
            pltpu.VMEM((nz, erows, width), F32),
            pltpu.VMEM((nz, erows, width), F32),
            pltpu.VMEM((nz, erows, width), F32),
            pltpu.VMEM((nx, qrows, width), F32),
            pltpu.VMEM((n, width), F32),
        ]

    def sems(sends, lands):
        return [pltpu.SemaphoreType.DMA((sends,)), pltpu.SemaphoreType.DMA((lands,))]

    scratch = [
        pltpu.VMEM((tokens, width), BF16),
        pltpu.VMEM((width, model), BF16),
        pltpu.VMEM((model, tokens), BF16),
        wide(BF16),
        *[wide() for _ in range(7)],
        wide(BF16),
        wide(),
        wide(),
        wide(BF16),
        pltpu.VMEM((tokens, n), F32),
        pltpu.VMEM((chunks, SLOT, L), F32),
        pltpu.VMEM((chunks, L, SLOT), F32),
        pltpu.VMEM((chunks, 1, width), F32),
        pltpu.VMEM((chunks, heads, L, L), F32),
        pltpu.VMEM((chunks, L, L), F32),
        pltpu.VMEM((chunks, n, width), F32),
        pltpu.VMEM((chunks, n, width), F32),
        pltpu.VMEM((chunks, n, width), F32),
        pltpu.VMEM((chunks, n, width), F32),
        pltpu.VMEM((chunks, SLOT, L), F32),
        pltpu.VMEM((chunks, SLOT, L), F32),
        pltpu.VMEM((chunks, L, SLOT), F32),
        wide(),
        *exchange(F32),
        *exchange(BF16),
        pltpu.VMEM((qrows, width), F32),
        pltpu.VMEM((nx, 1, width), F32),
        pltpu.VMEM((nz, 1, width), F32),
        pltpu.VMEM((ntp, 8, L), F32),
        pltpu.VMEM((L, 128), F32),
        pltpu.VMEM((nx, 2, width), F32),
        pltpu.VMEM((nz, 2, width), F32),
        pltpu.VMEM((nz, shard, front), BF16),
        pltpu.VMEM((nz, shard, width - front), BF16),
        *[pltpu.VMEM((nz, columns, front), BF16) for _ in range(6)],
        *[pltpu.VMEM((nz, shard, width - front), BF16) for _ in range(2)],
        *[pltpu.VMEM((nx, columns, width - front), BF16) for _ in range(2)],
        pltpu.VMEM((tokens, n), BF16),
        pltpu.VMEM((tokens, n), BF16),
        pltpu.VMEM((2, ntp, share, n), BF16),
        pltpu.VMEM((2, ntp, share, n), F32),
        pltpu.SemaphoreType.DMA((3,)),
        *sems(1, 10),
        *(sems(1, 1) * 2),
        *(sems(1, 1) * 8),
        *(sems(1, 1) * 3),
        pltpu.SemaphoreType.DMA((3,)),
        pltpu.SemaphoreType.DMA((3, nz)),
        *(sems(1, nz) * 2),
        *(sems(1, 1) * 5),
    ]
    vmem = pl.BlockSpec(memory_space=pltpu.VMEM)
    hbm = pl.BlockSpec(memory_space=pl.ANY)
    outs = pl.pallas_call(
        functools.partial(core, nx, nz, ntp),
        out_shape=(
            pltpu.VMEM((tokens, width), BF16),
            pltpu.VMEM((tokens, width), BF16),
            pltpu.VMEM((tokens, n), F32),
            pltpu.VMEM((tokens, n), F32),
            pltpu.VMEM((heads, tokens), F32),
            pltpu.VMEM((1, heads), F32),
            pltpu.VMEM((1, width), F32),
            pltpu.VMEM((columns, width), F32),
        ),
        in_specs=[vmem, vmem, hbm, vmem, vmem, vmem, pl.BlockSpec(memory_space=pltpu.SMEM), vmem, hbm, hbm],
        out_specs=(vmem,) * 8,
        scratch_shapes=scratch,
        compiler_params=pltpu.CompilerParams(
            collective_id=0, has_side_effects=True, vmem_limit_bytes=54 * 1024 * 1024
        ),
        name="layer_backward",
    )(packed, expo, gate, write, read, decay, skip[None, :], gain, weight, cot)
    return hand_out(outs)


def solution(mesh):
    ntp = mesh.shape["tp"]
    nz = mesh.shape["seq"] // NX
    return jax.shard_map(
        functools.partial(on_device, NX, nz, ntp),
        mesh=mesh,
        in_specs=(
            P("seq", "tp"),
            P("tp", "seq"),
            P("seq", "tp"),
            P("seq", None),
            P("seq", None),
            P("tp", "seq"),
            P("tp"),
            P("tp"),
            P("tp", None),
            P("seq", "tp"),
        ),
        out_specs=(
            P("seq", "tp"),
            P("seq", "tp"),
            P("seq", None),
            P("seq", None),
            P("tp", "seq"),
            P("tp"),
            P("tp"),
            P("tp", "seq"),
        ),
        check_vma=False,
    )
```

```python
import functools

import jax
import jax.numpy as jnp
from jax import lax
from jax.experimental import pallas as pl
from jax.experimental.pallas import tpu as pltpu
from jax.sharding import PartitionSpec as P

MESH = pl.DeviceIdType.MESH
F32, BF16 = jnp.float32, jnp.bfloat16
EXACT = lax.Precision.HIGHEST
NX = 4
L = 128
HEAD = 64
SLOT = 16
FRONT = 384


def dot(a, b, ca=1, cb=0, precision=None):
    return lax.dot_general(
        a, b, (((ca,), (cb,)), ((), ())), preferred_element_type=F32, precision=precision
    )


def pieces(v, count):
    out = []
    for _ in range(count):
        part = v.astype(BF16)
        out.append(part)
        v = v - part.astype(F32)
    return out


def iota(shape, dim):
    return lax.broadcasted_iota(jnp.int32, shape, dim)


def rcopy(src, dst, send, recv, dev):
    return pltpu.make_async_remote_copy(
        src_ref=src, dst_ref=dst, send_sem=send, recv_sem=recv, device_id=dev, device_id_type=MESH
    )


def core(nx, nz, ntp, packed, expo, gate_hbm, b_ref, c_ref, ld_ref, skip_ref, gain_ref, w_hbm, cot_hbm,
         gin, ggate, gwrite, gread, gdecay, gskip, ggain, gow, *scratch):
    (gate_v, w_v, cot, xb, yb, gvb, mixb, dyb, rsb, endb, startb,
     normed, act, gvg, xe, xl, accp, csr, csc, totb, dec, cross, gb, stb, hcb, sumd, segr, segc, dxi,
     sloc, lb, tb, ub, qs, qb, vs, s_in,
     rloc, lb2, tb2, ub2, qs2, qb2, vs2, h_in, vl2, h_low,
     vtop, dxs, dzs, sums, totc, gx, gz, pwa, pwb, xa, xd, xm, xc, zsa, zra, zsb, zrb, xsb, xrb, accw, accr, red, redo,
     cp_sem, s_ag, r_ag, s_dx, r_dx, s_dz, r_dz,
     s_p1, r_p1, s_p2, r_p2, s_p3, r_p3, s_p4, r_p4,
     s_h1, r_h1, s_h2, r_h2, s_h3, r_h3, s_h4, r_h4, s_hl, r_hl,
     s_tp, r_tp, s_gx, r_gx, s_gz, r_gz, s_rx, r_rx, s_za, r_za, s_zb, r_zb, s_xb, r_xb,
     s_w1, r_w1, s_w2, r_w2, s_c1, r_c1, s_c2, r_c2) = scratch
    tokens, width = xb.shape
    chunks = tokens // L
    pairs = width // 128
    heads = width // HEAD
    total_width = width * ntp
    ny = ntp // 2
    qrows, erows = 128 // nx, 128 // (nx * nz)
    s = lax.axis_index("seq")
    t = lax.axis_index("tp")
    z, x = lax.div(s, nx), lax.rem(s, nx)
    y, half = lax.div(t, 2), lax.rem(t, 2)
    shard = cot.shape[0] // ntp

    def dev_x(p):
        return {"seq": z * nx + p, "tp": t}

    def dev_z(p):
        return {"seq": p * nx + x, "tp": t}

    def dev_t(p):
        return {"seq": s, "tp": p}

    X, Z, TP = (nx, x, dev_x), (nz, z, dev_z), (ntp, t, dev_t)
    pending = []

    def send(group, src_of, dst, whole, ssem, rsem):
        n, me, dev = group
        for d in sorted(range(1, n), key=lambda d: -min(d, n - d)):
            p = lax.rem(me + d, n)
            rcopy(src_of(p), dst, ssem.at[0], rsem.at[0], dev(p)).start()
        if n > 1:
            pending.append(rcopy(whole, whole, ssem.at[0], rsem.at[0], dev(me)))

    def arrive(group, whole, ssem, rsem):
        n, me, dev = group
        if n > 1:
            rcopy(whole, whole, ssem.at[0], rsem.at[0], dev(me)).wait_recv()

    def slots(ref, n):
        return ref.at[pl.ds(0, n - 1)]

    def cot_rows(p, first=0, count=shard):
        return cot.at[pl.ds(pl.multiple_of(p * shard + first, 16), count)]

    load_cot = pltpu.make_async_copy(cot_hbm, cot_rows(t), cp_sem.at[0])
    load_gate = pltpu.make_async_copy(gate_hbm, gate_v, cp_sem.at[1])
    load_w = pltpu.make_async_copy(w_hbm, w_v, cp_sem.at[2])
    load_cot.start()
    load_gate.start()
    load_w.start()

    barrier = pltpu.get_barrier_semaphore()
    for n, me, dev in (X, Z, TP):
        for d in range(1, n):
            pl.semaphore_signal(
                barrier, inc=1, device_id=dev(lax.rem(me + d, n)), device_id_type=MESH
            )

    spread = (iota((SLOT, width), 1) // HEAD == iota((SLOT, width), 0)).astype(BF16)
    gather = (iota((width, SLOT), 0) // HEAD == iota((width, SLOT), 1)).astype(BF16)
    upper = (iota((L, L), 0) <= iota((L, L), 1)).astype(BF16)
    causal = iota((L, L), 0) >= iota((L, L), 1)
    left = iota((L, 128), 1) < HEAD

    def spread_heads(v):
        return sum(dot(part, spread) for part in pieces(v, 3))

    def head_sums(v):
        return sum(dot(part, gather) for part in pieces(v, 2))

    csr[...] = jnp.zeros_like(csr)
    segr[...] = jnp.zeros_like(segr)
    for k in range(chunks):
        csr[k, 0:heads, :] = ld_ref[:, k * L : (k + 1) * L]
    rows = csr[...].reshape(chunks * SLOT, L)
    rows = sum(dot(part, upper) for part in pieces(rows, 3))
    log_total = jnp.zeros((1, width), F32)
    for k in range(chunks):
        csr[k] = rows[k * SLOT : (k + 1) * SLOT, :]
        cols = rows[k * SLOT : (k + 1) * SLOT, :].T
        csc[k] = cols
        logs = spread_heads(cols)
        last = logs[L - 1 : L, :]
        log_total = log_total + last
        totb[k] = jnp.exp(last)
        endb[k * L : (k + 1) * L, :] = jnp.exp(last - logs)
        startb[k * L : (k + 1) * L, :] = jnp.exp(logs)
    dxs[x] = jnp.exp(log_total)

    powers = lax.shift_left(jnp.ones_like(expo[...]), expo[...] + 5).astype(F32) * (1.0 / 32.0)
    nibble = 4 * iota((8, width), 0)
    for k in range(chunks):
        factor_rows = jnp.concatenate(
            [powers[:, k * L : (k + 1) * L], jnp.zeros((8 - pairs, L), F32)], axis=0
        )
        factor = factor_rows.T
        wide = jnp.concatenate(
            [jnp.broadcast_to(factor[:, p : p + 1], (L, 128)) for p in range(pairs)], axis=1
        )
        words = packed[k * (L // 8) : (k + 1) * (L // 8), :]
        fields = jnp.concatenate(
            [
                lax.bitwise_and(
                    lax.shift_right_arithmetic(
                        jnp.broadcast_to(words[r : r + 1, :], (8, width)), nibble
                    ),
                    15,
                )
                - 8
                for r in range(L // 8)
            ],
            axis=0,
        )
        xb[k * L : (k + 1) * L, :] = (fields.astype(F32) * wide).astype(BF16)

    run = jnp.zeros((128, width), F32)
    for k in range(chunks):
        rows = slice(k * L, (k + 1) * L)
        weighted = xb[rows, :].astype(F32) * endb[rows, :]
        parts = pieces(weighted, 2)
        xe[rows, :], xl[rows, :] = parts
        gb[k] = sum(dot(b_ref[rows, :], part, 0, 0) for part in parts)
        run = totb[k] * run + gb[k]
    sloc[...] = run

    def take_rows(ref, at, count):
        return ref[pl.ds(pl.multiple_of(at * count, count), count), :]

    def exchange_1(own, lbuf, ssem, rsem):
        send(
            X,
            lambda p: own.at[pl.ds(pl.multiple_of(p * qrows, qrows), qrows)],
            lbuf.at[x],
            slots(lbuf, nx),
            ssem,
            rsem,
        )
        lbuf[x] = take_rows(own, x, qrows)

    pl.semaphore_wait(barrier, (nx - 1) + (nz - 1) + (ntp - 1))
    send(X, lambda p: dxs.at[x], dxs.at[x], slots(dxs, nx), s_dx, r_dx)
    exchange_1(sloc, lb, s_p1, r_p1)

    load_cot.wait()
    part = shard // 2
    sibling = 2 * y + 1 - half
    after = 2 * lax.rem(y + 1, ny) + half
    before = 2 * lax.rem(y + ny - 1, ny) + half
    across = 2 * lax.rem(y + 2, ny) + half

    def cot_copy(j, p, to, first=0, count=shard):
        return rcopy(cot_rows(p, first, count), cot_rows(p, first, count), s_ag.at[0], r_ag.at[j], dev_t(to))

    def cot_send(j, p, to, *rows):
        cot_copy(j, p, to, *rows).start()

    def cot_wait(j, p, *rows):
        cot_copy(j, p, sibling, *rows).wait_recv()

    cot_send(0, t, sibling)
    if ny == 2:
        cot_send(1, t, after)
    elif ny == 4:
        cot_send(1, t, after, 0, part)
        cot_send(3, t, before, part, part)
        cot_send(2, t, after, part, part)
        cot_send(4, t, before, 0, part)

    def relay_cot():
        if ny == 4:
            cot_wait(1, before, 0, part)
            cot_send(5, before, after, 0, part)
            cot_wait(3, after, part, part)
            cot_send(6, after, before, part, part)

    def near_cot():
        if ny == 2:
            cot_wait(1, after)
            cot_send(7, after, sibling)
        elif ny == 4:
            cot_wait(2, before, part, part)
            cot_send(7, before, sibling)
            cot_wait(4, after, 0, part)
            cot_send(8, after, sibling)

    def far_cot():
        if ny == 4:
            cot_wait(5, across, 0, part)
            cot_wait(6, across, part, part)
            cot_send(9, across, sibling)

    def project(chip, first=False):
        terms = dot(
            cot[pl.ds(pl.multiple_of(chip * 2 * shard, 128), 2 * shard), :],
            w_v[:, pl.ds(pl.multiple_of(chip * 2 * shard, 128), 2 * shard)],
            0,
            1,
        )
        gvb[...] = terms if first else gvb[...] + terms

    def other(p):
        return p + 1 - 2 * half

    def exchange_2(lbuf, tbuf, ubuf, s1, r1, ssem, rsem, backward):
        arrive(X, slots(lbuf, nx), s1, r1)
        order = range(nx - 1, -1, -1) if backward else range(nx)
        row = None
        for k in order:
            add = lbuf[k].astype(F32)
            row = add if row is None else dxs[k] * row + add
        for k in range(nz):
            tbuf[k] = row[k * erows : (k + 1) * erows, :]
        send(Z, lambda p: tbuf.at[p], ubuf.at[z], slots(ubuf, nz), ssem, rsem)
        ubuf[z] = tbuf[z]

    def exchange_3(ubuf, qsend, qbuf, s2, r2, ssem, rsem, backward):
        arrive(Z, slots(ubuf, nz), s2, r2)
        order = range(nz - 1, -1, -1) if backward else range(nz)
        row = jnp.zeros((erows, width), F32)
        for k in order:
            qsend[k] = row
            row = dzs[k] * row + ubuf[k]
        send(Z, lambda p: qsend.at[p], qbuf.at[z], slots(qbuf, nz), ssem, rsem)
        qbuf[z] = qsend[z]

    def exchange_4(qbuf, lbuf, vsend, result, s3, r3, ssem, rsem, backward):
        arrive(Z, slots(qbuf, nz), s3, r3)
        for k in range(nz):
            vtop[k * erows : (k + 1) * erows, :] = qbuf[k]
        order = range(nx - 1, -1, -1) if backward else range(nx)
        row = vtop[...]
        for k in order:
            if backward:
                vsend[k], vl2[k] = pieces(row, 2)
            else:
                vsend[k] = row
            row = dxs[k] * row + lbuf[k].astype(F32)
        mine = pl.ds(pl.multiple_of(x * qrows, qrows), qrows)
        rest = pl.ds(0, (nx - 1) * qrows)
        send(X, lambda p: vsend.at[p], result.at[mine], result.at[rest], ssem, rsem)
        result[mine, :] = vsend[x]
        if backward:
            send(X, lambda p: vl2.at[p], h_low.at[mine], h_low.at[rest], s_hl, r_hl)
            h_low[mine, :] = vl2[x]

    def exchange_5(result, s4, r4):
        arrive(X, result.at[pl.ds(0, (nx - 1) * qrows)], s4, r4)


    skip_row = jnp.zeros((1, width), F32)
    head_of = iota((1, width), 1) // HEAD
    for h in range(heads):
        skip_row = jnp.where(head_of == h, skip_ref[0, h], skip_row)

    def at_chunk(k):
        return pl.ds(pl.multiple_of(k * L, L), L)

    def split_pair(v):
        zero = jnp.zeros_like(v)
        return jnp.concatenate([jnp.where(left, v, zero), jnp.where(left, zero, v)], axis=0)

    def inside(k, _):
        rows = at_chunk(k)
        both = dot(c_ref[rows, :], b_ref[rows, :], 1, 1)
        cross[k] = both
        for p in range(pairs):
            mixing = []
            for h in (2 * p, 2 * p + 1):
                spread_log = csc[k][:, h : h + 1] - csr[k][h : h + 1, :]
                decay = jnp.where(causal, jnp.exp(jnp.minimum(spread_log, 0.0)), 0.0)
                dec[k, h] = decay
                mixing.append(pieces(decay * both, 2))
            lanes = slice(128 * p, 128 * (p + 1))
            x_pair = xb[rows, lanes]
            x_split = split_pair(x_pair)
            yb[rows, lanes] = (
                dot(jnp.concatenate([m[0] for m in mixing], axis=1), x_split)
                + dot(jnp.concatenate([m[1] for m in mixing], axis=1), x_split)
                + skip_row[:, lanes] * x_pair.astype(F32)
            )
        return 0

    lax.fori_loop(0, chunks // 2, inside, 0)
    load_w.wait()
    cot_wait(0, sibling)
    project(y, True)
    arrive(X, slots(dxs, nx), s_dx, r_dx)
    row = dxs[0]
    for k in range(1, nx):
        row = row * dxs[k]
    dzs[z] = row
    send(Z, lambda p: dzs.at[z], dzs.at[z], slots(dzs, nz), s_dz, r_dz)

    exchange_2(lb, tb, ub, s_p1, r_p1, s_p2, r_p2, False)
    relay_cot()
    lax.fori_loop(chunks // 2, chunks, inside, 0)
    arrive(Z, slots(dzs, nz), s_dz, r_dz)
    exchange_3(ub, qs, qb, s_p2, r_p2, s_p3, r_p3, False)
    near_cot()
    exchange_4(qb, lb, vs, s_in, s_p3, r_p3, s_p4, r_p4, False)
    far_cot()
    if ny == 2:
        cot_wait(7, other(after))
        project(lax.rem(y + 1, ny))
    elif ny == 4:
        cot_wait(7, other(before))
        project(lax.rem(y + 3, ny))
        cot_wait(8, other(after))
        project(lax.rem(y + 1, ny))
    load_gate.wait()
    if ny == 4:
        cot_wait(9, other(across))
        project(lax.rem(y + 2, ny))
    gain_row = gain_ref[...].reshape(1, width)

    def prepare(k, _):
        rows = at_chunk(k)
        gate = gate_v[rows, :].astype(F32)
        act[rows, :] = gate * jax.nn.sigmoid(gate)
        gvg[rows, :] = gvb[rows, :] * gain_row
        return 0

    lax.fori_loop(0, chunks, prepare, 0)
    exchange_5(s_in, s_p4, r_p4)
    stb[0] = s_in[...].astype(F32)
    for k in range(1, chunks):
        stb[k] = totb[k - 1] * stb[k - 1] + gb[k - 1]
    lane = iota((L, 128), 1)

    def sums_of(k, acc):
        rows = at_chunk(k)
        start = sum(dot(c_ref[rows, :], part) for part in pieces(stb[k], 2))
        rsb[rows, :] = start
        y_now = yb[rows, :] + startb[rows, :] * start
        yb[rows, :] = y_now
        mixed = y_now * act[rows, :]
        mixb[rows, :] = mixed
        square = jnp.sum(mixed * mixed, axis=1, keepdims=True)
        inner = jnp.sum(gvg[rows, :] * mixed, axis=1, keepdims=True)
        return jnp.where(lane == 2 * k, square, jnp.where(lane == 2 * k + 1, inner, acc))

    packed_sums = lax.fori_loop(0, chunks, sums_of, jnp.zeros((L, 128), F32))
    sums[t] = packed_sums.T[0:8, :]
    send(TP, lambda p: sums.at[t], sums.at[t], slots(sums, ntp), s_tp, r_tp)
    arrive(TP, slots(sums, ntp), s_tp, r_tp)

    both = sums[0]
    for p in range(1, ntp):
        both = both + sums[p]
    totc[...] = jnp.concatenate([both, jnp.zeros((120, L), F32)], axis=0).T

    def token_scales(k):
        both = totc[...]
        square = jnp.sum(jnp.where(lane == 2 * k, both, 0.0), axis=1, keepdims=True)
        inner = jnp.sum(jnp.where(lane == 2 * k + 1, both, 0.0), axis=1, keepdims=True)
        return lax.rsqrt(square / total_width + 1e-05), inner

    def gradients(k, _):
        rows = at_chunk(k)
        scale, inner = token_scales(k)
        grad_mixed = scale * gvg[rows, :] - mixb[rows, :] * (
            (scale * scale * scale) * inner / total_width
        )
        grad_y = grad_mixed * act[rows, :]
        dyb[rows, :] = grad_y
        scaled = grad_y * startb[rows, :]
        hcb[k] = sum(dot(c_ref[rows, :], part, 0, 0) for part in pieces(scaled, 2))
        return 0

    lax.fori_loop(0, chunks, gradients, 0)
    run = hcb[chunks - 1]
    for k in range(chunks - 2, -1, -1):
        run = totb[k] * run + hcb[k]
    rloc[...] = run.astype(BF16)
    exchange_1(rloc, lb2, s_h1, r_h1)

    def gate_gradients(k, carry):
        gain_sum, skip_sum = carry
        rows = at_chunk(k)
        scale, inner = token_scales(k)
        mixed = mixb[rows, :]
        gate = gate_v[rows, :].astype(F32)
        sigma = jax.nn.sigmoid(gate)
        scaled_mixed = mixed * scale
        normed[rows, :] = (scaled_mixed * gain_row).astype(BF16)
        grad_mixed = scale * gvg[rows, :] - mixed * (
            (scale * scale * scale) * inner / total_width
        )
        ggate[rows, :] = (
            grad_mixed * yb[rows, :] * sigma * (1.0 + gate * (1.0 - sigma))
        ).astype(BF16)
        gain_sum = gain_sum + jnp.sum(gvb[rows, :] * scaled_mixed, axis=0, keepdims=True)
        skip_sum = skip_sum + jnp.sum(
            dyb[rows, :] * xb[rows, :].astype(F32), axis=0, keepdims=True
        )
        return gain_sum, skip_sum

    zero_row = jnp.zeros((1, width), F32)
    gain_sum, skip_sum = lax.fori_loop(0, chunks, gate_gradients, (zero_row, zero_row))
    gx[x, 0:1, :] = gain_sum
    gx[x, 1:2, :] = skip_sum
    send(X, lambda p: gx.at[x], gx.at[x], slots(gx, nx), s_gx, r_gx)

    columns = shard // nx
    front = pwa.shape[2]
    middle = nz // 2
    steps = sorted(range(1, nz), key=lambda i: -min(i, nz - i)) + [nz]

    def block_of(i):
        return lax.rem(z + i, nz)

    def mine_of(i, p):
        return pwa.at[block_of(i), pl.ds(pl.multiple_of(p * columns, columns), columns)]

    def sides(i):
        one, two = lax.rem(x + 1, nx), lax.rem(x + nx - 1, nx)
        return (one, two) if steps.index(i) % 2 == 0 else (two, one)

    def weight_copy(kind, i, to):
        source = (mine_of(i, lax.rem(x + 2, nx)), mine_of(i, to), xm.at[i - 1])[kind]
        target = (xa, xd, xc)[kind].at[i - 1]
        return rcopy(source, target, s_rx.at[kind], r_rx.at[kind, i - 1], dev_x(to))

    def weight_send(kind, i, to):
        weight_copy(kind, i, to).start()

    def weight_block(i):
        k = block_of(i)
        terms = dot(cot[pl.ds(pl.multiple_of(k * shard, shard), shard), :], normed[...]).astype(BF16)
        pwa[k] = terms[:, :front]
        pwb[k] = terms[:, front:]

    def block_send(i):
        near, far = sides(i)
        if nx == 4:
            weight_send(0, i, near)
        if nx > 1:
            weight_send(1, i, far)

    def weight_relay(i):
        near, _ = sides(i)
        if nx == 4:
            weight_copy(0, i, near).wait_recv()
            xm[i - 1] = (xa[i - 1].astype(F32) + mine_of(i, near)[...].astype(F32)).astype(BF16)
            weight_send(2, i, near)

    def ring_part(kind, i, up):
        rows = (columns, shard)[kind]
        cut = 16 * (3 * rows // 80)
        return (0, rows) if i != middle else (0, cut) if up else (cut, rows)

    def ring_copy(kind, i, up):
        first, end = ring_part(kind, i, up)
        slot = i - 1 if i != middle or up else nz - 1
        sends, lands, s_z, r_z = ((zsa, zra, s_za, r_za), (zsb, zrb, s_zb, r_zb))[kind]
        return rcopy(
            sends.at[i - 1, pl.ds(first, end - first)],
            lands.at[i - 1, pl.ds(first, end - first)],
            s_z.at[0],
            r_z.at[slot],
            dev_z(lax.rem(z + (1 if up else nz - 1), nz)),
        )

    def ring_add(kind, out, i, up):
        ring_copy(kind, i, up).wait_recv()
        first, end = ring_part(kind, i, up)
        part = (zra, zrb)[kind][i - 1, first:end, :].astype(F32)
        parts = [out[:first]] if first else []
        parts.append(out[first:end] + part)
        if end < out.shape[0]:
            parts.append(out[end:])
        return jnp.concatenate(parts, axis=0) if len(parts) > 1 else parts[0]

    def ring_step(kind, i, out):
        if i % nz < middle:
            out = ring_add(kind, out, i % nz + 1, True)
        if i > middle:
            out = ring_add(kind, out, i - 1, False)
        if i < nz:
            (zsa, zsb)[kind][i - 1] = out.astype(BF16)
            for up in (True, False):
                if i == middle or (i < middle) == up:
                    ring_copy(kind, i, up).start()
        return out

    def weight_rows(i):
        near, far = sides(i)
        out = mine_of(i, x)[...].astype(F32)
        if nx > 1:
            weight_copy(1, i, far).wait_recv()
            out = out + xd[i - 1].astype(F32)
        if nx == 4:
            weight_copy(2, i, near).wait_recv()
            out = out + xc[i - 1].astype(F32)
        out = ring_step(0, i, out)
        if i == nz:
            gow[:, :front] = out

    def back_rows(i):
        out = ring_step(1, i, pwb[block_of(i)].astype(F32))
        if i == nz:
            for p in range(nx):
                xsb[p] = out[p * columns : (p + 1) * columns, :].astype(BF16)
            send(X, lambda p: xsb.at[p], xrb.at[x], slots(xrb, nx), s_xb, r_xb)
            xrb[x] = xsb[x]

    def back_finish():
        arrive(X, slots(xrb, nx), s_xb, r_xb)
        out = xrb[0].astype(F32)
        for p in range(1, nx):
            out = out + xrb[p].astype(F32)
        gow[:, front:] = out

    def batch(first, end):
        return steps[(first * nz) // 8 : (end * nz) // 8]

    order = iter(steps)

    def back_steps(count):
        for _ in range(count):
            i = next(order, None)
            if i is not None:
                back_rows(i)

    for n, i in enumerate(steps):
        weight_block(i)
        if i in batch(0, 4):
            block_send(i)
        if n == 0:
            back_steps(1)
    exchange_2(lb2, tb2, ub2, s_h1, r_h1, s_h2, r_h2, True)
    arrive(X, slots(gx, nx), s_gx, r_gx)
    row = gx[0]
    for k in range(1, nx):
        row = row + gx[k]
    gz[z] = row
    send(Z, lambda p: gz.at[z], gz.at[z], slots(gz, nz), s_gz, r_gz)

    def inside_back(k, _):
        rows = at_chunk(k)
        both = cross[k]
        summed = jnp.zeros((L, L), F32)
        lane = iota((L, SLOT), 1)
        row_sums = jnp.zeros((L, SLOT), F32)
        for p in range(pairs):
            lanes = slice(128 * p, 128 * (p + 1))
            x_pair = xb[rows, lanes]
            high, low = pieces(dyb[rows, lanes], 2)
            grads = split_pair(high)
            dots = dot(grads, x_pair, 1, 1) + dot(split_pair(low), x_pair, 1, 1)
            mixing = []
            for i in range(2):
                h = 2 * p + i
                decay = dec[k, h]
                weighted = dots[i * L : (i + 1) * L, :] * decay
                summed = summed + weighted
                terms = weighted * both
                row_sums = row_sums + jnp.where(
                    lane == h, jnp.sum(terms, axis=1, keepdims=True), 0.0
                )
                segr[k, h : h + 1, :] = jnp.sum(terms, axis=0, keepdims=True)
                mixing.append((decay * both).astype(BF16))
            dxi[rows, lanes] = dot(jnp.concatenate(mixing, axis=0), grads, 0, 0)
        sum_parts = pieces(summed, 2)
        accp[rows, :] = sum(dot(part, c_ref[rows, :], 0, 0) for part in sum_parts)
        segc[k] = row_sums - segr[k].T
        scaled = dyb[rows, :] * startb[rows, :]
        accr[rows, :] = (
            sum(dot(part, b_ref[rows, :]) for part in sum_parts)
            + sum(dot(part, stb[k].astype(BF16), 1, 1) for part in pieces(scaled, 2))
        ).astype(BF16)
        return 0

    lax.fori_loop(0, chunks // 2, inside_back, 0)
    for i in batch(0, 1):
        weight_relay(i)
    back_steps(2 if nz == 8 else 0)
    exchange_3(ub2, qs2, qb2, s_h2, r_h2, s_h3, r_h3, True)
    for i in batch(4, 8):
        block_send(i)
    lax.fori_loop(chunks // 2, chunks, inside_back, 0)
    for i in batch(1, 3):
        weight_relay(i)
    for i in batch(0, 1):
        weight_rows(i)
    back_steps(2 if nz == 8 else 0)
    exchange_4(qb2, lb2, vs2, h_in, s_h3, r_h3, s_h4, r_h4, True)

    share = tokens // ntp

    def reduce_1(acc, which, ssem, rsem):
        send(
            TP,
            lambda p: acc.at[pl.ds(pl.multiple_of(p * share, share), share)],
            red.at[which, t],
            red.at[which, pl.ds(0, ntp - 1)],
            ssem,
            rsem,
        )
        red[which, t] = take_rows(acc, t, share)

    def reduce_2(which, s1, r1, ssem, rsem):
        arrive(TP, red.at[which, pl.ds(0, ntp - 1)], s1, r1)
        out = red[which, 0].astype(F32)
        for p in range(1, ntp):
            out = out + red[which, p].astype(F32)
        redo[which, t] = out.astype(BF16)
        send(TP, lambda p: redo.at[which, t], redo.at[which, t], redo.at[which, pl.ds(0, ntp - 1)], ssem, rsem)

    def reduce_3(out_ref, which, ssem, rsem):
        arrive(TP, redo.at[which, pl.ds(0, ntp - 1)], ssem, rsem)
        for p in range(ntp):
            out_ref[p * share : (p + 1) * share, :] = redo[which, p].astype(F32)

    reduce_1(accr, 0, s_c1, r_c1)
    for i in batch(3, 4):
        weight_relay(i)
    for i in batch(1, 3):
        weight_rows(i)
    for i in batch(4, 6):
        weight_relay(i)
    back_steps(2 if nz == 8 else 0)
    exchange_5(h_in, s_h4, r_h4)

    def states_back(i, run):
        k = chunks - 1 - i
        rows = at_chunk(k)
        state = run.astype(BF16)
        late = dot(xe[rows, :], state, 1, 1) + dot(xl[rows, :], state, 1, 1)
        accw[rows, :] = (accp[rows, :] + late).astype(BF16)
        return totb[k] * run + hcb[k]

    lax.fori_loop(0, chunks, states_back, h_in[...].astype(F32))
    reduce_1(accw, 1, s_w1, r_w1)
    def finish(i, run):
        k = chunks - 1 - i
        rows = at_chunk(k)
        grad_y = dyb[rows, :]
        write = endb[rows, :] * sum(dot(b_ref[rows, :], part) for part in pieces(run, 2))
        gin[rows, :] = (skip_row * grad_y + dxi[rows, :] + write).astype(BF16)
        leaving = xb[rows, :].astype(F32) * write
        arriving = grad_y * startb[rows, :] * rsb[rows, :]
        seg = segc[k] + head_sums(arriving - leaving)
        final = jnp.sum(leaving, axis=0, keepdims=True) + totb[k] * jnp.sum(
            run * stb[k], axis=0, keepdims=True
        )
        final = head_sums(jnp.broadcast_to(final, (8, width)))[0:1]
        whole = sum(dot(upper, part) for part in pieces(seg, 2)) + final
        sumd[k] = whole.T
        return totb[k] * run + hcb[k]

    exchange_5(h_low, s_hl, r_hl)
    run = lax.fori_loop(0, 3 * chunks // 4, finish, h_in[...].astype(F32) + h_low[...].astype(F32))
    for i in batch(3, 5):
        weight_rows(i)
    for i in batch(6, 8):
        weight_relay(i)

    reduce_2(1, s_w1, r_w1, s_w2, r_w2)
    reduce_2(0, s_c1, r_c1, s_c2, r_c2)
    lax.fori_loop(3 * chunks // 4, chunks, finish, run)
    for k in range(chunks):
        gdecay[:, k * L : (k + 1) * L] = sumd[k, 0:heads, :]
    back_steps(nz)
    for i in batch(5, 8)[:-1]:
        weight_rows(i)
    arrive(Z, slots(gz, nz), s_gz, r_gz)
    row = gz[0]
    for k in range(1, nz):
        row = row + gz[k]
    ggain[...] = row[0:1]
    gskip[...] = head_sums(jnp.concatenate([row, jnp.zeros((6, width), F32)], axis=0))[1:2, 0:heads]
    reduce_3(gread, 0, s_c2, r_c2)
    back_finish()
    weight_rows(nz)
    reduce_3(gwrite, 1, s_w2, r_w2)
    for copy in pending:
        copy.wait_send()

    def all_left(whole, sem):
        rcopy(whole, whole, sem, r_ag.at[0], dev_t(sibling)).wait_send()

    all_left(cot.at[pl.ds(0, (2 * ny - 1) * shard)], s_ag.at[0])
    for kind in range(3):
        if nx == 4 or (nx > 1 and kind == 1):
            all_left(xa, s_rx.at[kind])
    all_left(slots(zra, nz), s_za.at[0])
    all_left(slots(zrb, nz), s_zb.at[0])


def copy_out(*refs):
    count = 8
    sources, targets, sem = refs[:count], refs[count : 2 * count], refs[-1]
    stores = [
        pltpu.make_async_copy(sources[k], targets[k], sem.at[k])
        for k in range(count)
        if k not in (5, 6)
    ]
    for store in stores:
        store.start()
    for k in (5, 6):
        targets[k][...] = sources[k][...].reshape(targets[k].shape)
    for store in stores:
        store.wait()


def hand_out(outs):
    vmem = pl.BlockSpec(memory_space=pltpu.VMEM)
    hbm = pl.BlockSpec(memory_space=pl.ANY)
    shapes = [
        jax.ShapeDtypeStruct(o.shape[1:] if k in (5, 6) else o.shape, o.dtype)
        for k, o in enumerate(outs)
    ]
    done = pl.pallas_call(
        copy_out,
        out_shape=shapes,
        in_specs=[vmem] * 8,
        out_specs=[vmem if k in (5, 6) else hbm for k in range(8)],
        scratch_shapes=[pltpu.SemaphoreType.DMA((8,))],
        name="hand_out",
    )(*[pltpu.with_memory_space_constraint(o, pltpu.VMEM) for o in outs])
    return (*done[:7], done[7].T)


def on_device(nx, nz, ntp, packed, expo, gate, write, read, decay, skip, gain, weight, cotangent):
    cot = cotangent.T
    tokens, width = gate.shape
    heads = decay.shape[0]
    model = weight.shape[1]
    shard = cot.shape[0]
    chunks = tokens // L
    n = write.shape[1]
    columns = model // (nx * nz)
    qrows, erows = n // nx, n // (nx * nz)
    share = tokens // ntp
    front = FRONT

    def wide(kind=F32):
        return pltpu.VMEM((tokens, width), kind)

    def exchange(kind):
        return [
            pltpu.VMEM((n, width), kind),
            pltpu.VMEM((nx, qrows, width), kind),
            pltpu.VMEM((nz, erows, width), F32),
            pltpu.VMEM((nz, erows, width), F32),
            pltpu.VMEM((nz, erows, width), F32),
            pltpu.VMEM((nz, erows, width), F32),
            pltpu.VMEM((nx, qrows, width), kind),
            pltpu.VMEM((n, width), kind),
        ]

    def sems(sends, lands):
        return [pltpu.SemaphoreType.DMA((sends,)), pltpu.SemaphoreType.DMA((lands,))]

    scratch = [
        pltpu.VMEM((tokens, width), BF16),
        pltpu.VMEM((width, model), BF16),
        pltpu.VMEM((model, tokens), BF16),
        wide(BF16),
        *[wide() for _ in range(7)],
        wide(BF16),
        wide(),
        wide(),
        wide(BF16),
        wide(BF16),
        pltpu.VMEM((tokens, n), F32),
        pltpu.VMEM((chunks, SLOT, L), F32),
        pltpu.VMEM((chunks, L, SLOT), F32),
        pltpu.VMEM((chunks, 1, width), F32),
        pltpu.VMEM((chunks, heads, L, L), F32),
        pltpu.VMEM((chunks, L, L), F32),
        pltpu.VMEM((chunks, n, width), F32),
        pltpu.VMEM((chunks, n, width), F32),
        pltpu.VMEM((chunks, n, width), F32),
        pltpu.VMEM((chunks, SLOT, L), F32),
        pltpu.VMEM((chunks, SLOT, L), F32),
        pltpu.VMEM((chunks, L, SLOT), F32),
        wide(),
        *exchange(F32),
        *exchange(BF16),
        *exchange(BF16)[-2:],
        pltpu.VMEM((qrows, width), F32),
        pltpu.VMEM((nx, 1, width), F32),
        pltpu.VMEM((nz, 1, width), F32),
        pltpu.VMEM((ntp, 8, L), F32),
        pltpu.VMEM((L, 128), F32),
        pltpu.VMEM((nx, 2, width), F32),
        pltpu.VMEM((nz, 2, width), F32),
        pltpu.VMEM((nz, shard, front), BF16),
        pltpu.VMEM((nz, shard, width - front), BF16),
        *[pltpu.VMEM((nz, columns, front), BF16) for _ in range(6)],
        *[pltpu.VMEM((nz, shard, width - front), BF16) for _ in range(2)],
        *[pltpu.VMEM((nx, columns, width - front), BF16) for _ in range(2)],
        pltpu.VMEM((tokens, n), BF16),
        pltpu.VMEM((tokens, n), BF16),
        pltpu.VMEM((2, ntp, share, n), BF16),
        pltpu.VMEM((2, ntp, share, n), BF16),
        pltpu.SemaphoreType.DMA((3,)),
        *sems(1, 10),
        *(sems(1, 1) * 2),
        *(sems(1, 1) * 9),
        *(sems(1, 1) * 3),
        pltpu.SemaphoreType.DMA((3,)),
        pltpu.SemaphoreType.DMA((3, nz)),
        *(sems(1, nz) * 2),
        *(sems(1, 1) * 5),
    ]
    vmem = pl.BlockSpec(memory_space=pltpu.VMEM)
    hbm = pl.BlockSpec(memory_space=pl.ANY)
    outs = pl.pallas_call(
        functools.partial(core, nx, nz, ntp),
        out_shape=(
            pltpu.VMEM((tokens, width), BF16),
            pltpu.VMEM((tokens, width), BF16),
            pltpu.VMEM((tokens, n), F32),
            pltpu.VMEM((tokens, n), F32),
            pltpu.VMEM((heads, tokens), F32),
            pltpu.VMEM((1, heads), F32),
            pltpu.VMEM((1, width), F32),
            pltpu.VMEM((columns, width), F32),
        ),
        in_specs=[vmem, vmem, hbm, vmem, vmem, vmem, pl.BlockSpec(memory_space=pltpu.SMEM), vmem, hbm, hbm],
        out_specs=(vmem,) * 8,
        scratch_shapes=scratch,
        compiler_params=pltpu.CompilerParams(
            collective_id=0, has_side_effects=True, vmem_limit_bytes=54 * 1024 * 1024
        ),
        name="layer_backward",
    )(packed, expo, gate, write, read, decay, skip[None, :], gain, weight, cot)
    return hand_out(outs)


def solution(mesh):
    ntp = mesh.shape["tp"]
    nz = mesh.shape["seq"] // NX
    return jax.shard_map(
        functools.partial(on_device, NX, nz, ntp),
        mesh=mesh,
        in_specs=(
            P("seq", "tp"),
            P("tp", "seq"),
            P("seq", "tp"),
            P("seq", None),
            P("seq", None),
            P("tp", "seq"),
            P("tp"),
            P("tp"),
            P("tp", None),
            P("seq", "tp"),
        ),
        out_specs=(
            P("seq", "tp"),
            P("seq", "tp"),
            P("seq", None),
            P("seq", None),
            P("tp", "seq"),
            P("tp"),
            P("tp"),
            P("tp", "seq"),
        ),
        check_vma=False,
    )
```

```python
import functools

import jax
import jax.numpy as jnp
from jax import lax
from jax.experimental import pallas as pl
from jax.experimental.pallas import tpu as pltpu
from jax.sharding import PartitionSpec as P

MESH = pl.DeviceIdType.MESH
F32, BF16 = jnp.float32, jnp.bfloat16
EXACT = lax.Precision.HIGHEST
NX = 4
L = 128
HEAD = 64
SLOT = 16
FRONT = 384


def dot(a, b, ca=1, cb=0, precision=None):
    return lax.dot_general(
        a, b, (((ca,), (cb,)), ((), ())), preferred_element_type=F32, precision=precision
    )


def pieces(v, count):
    out = []
    for _ in range(count):
        part = v.astype(BF16)
        out.append(part)
        v = v - part.astype(F32)
    return out


def iota(shape, dim):
    return lax.broadcasted_iota(jnp.int32, shape, dim)


def rcopy(src, dst, send, recv, dev):
    return pltpu.make_async_remote_copy(
        src_ref=src, dst_ref=dst, send_sem=send, recv_sem=recv, device_id=dev, device_id_type=MESH
    )


def core(nx, nz, ntp, packed_hbm, expo_hbm, gate_hbm, b_hbm, c_hbm, ld_hbm, skip_hbm, gain_hbm, w_hbm, cot_hbm,
         gin, ggate, gwrite, gread, gdecay, gskip, ggain, gow, *scratch):
    (packed, expo, b_ref, c_ref, ld_ref, skip_ref, gain_ref, gate_v, w_v, cot, xb, yb, gvb, mixb, dyb, rsb, endb, startb,
     normed, act, gvg, xe, xl, accp, csr, csc, totb, dec, cross, gb, stb, hcb, sumd, segr, segc, dxi,
     sloc, lb, tb, ub, qs, qb, vs, s_in,
     rloc, lb2, tb2, ub2, qs2, qb2, vs2, h_in, vl2, h_low,
     vtop, dxs, dzs, sums, totc, gx, gz, pwa, pwb, xa, xd, xm, xc, zsa, zra, zsb, zrb, xsb, xrb, accw, accr, red, redo,
     cp_sem, s_ag, r_ag, s_dx, r_dx, s_dz, r_dz,
     s_p1, r_p1, s_p2, r_p2, s_p3, r_p3, s_p4, r_p4,
     s_h1, r_h1, s_h2, r_h2, s_h3, r_h3, s_h4, r_h4, s_hl, r_hl,
     s_tp, r_tp, s_gx, r_gx, s_gz, r_gz, s_rx, r_rx, s_za, r_za, s_zb, r_zb, s_xb, r_xb,
     s_w1, r_w1, s_w2, r_w2, s_c1, r_c1, s_c2, r_c2) = scratch
    tokens, width = xb.shape
    chunks = tokens // L
    pairs = width // 128
    heads = width // HEAD
    total_width = width * ntp
    ny = ntp // 2
    qrows, erows = 128 // nx, 128 // (nx * nz)
    s = lax.axis_index("seq")
    t = lax.axis_index("tp")
    z, x = lax.div(s, nx), lax.rem(s, nx)
    y, half = lax.div(t, 2), lax.rem(t, 2)
    shard = cot.shape[0] // ntp

    def dev_x(p):
        return {"seq": z * nx + p, "tp": t}

    def dev_z(p):
        return {"seq": p * nx + x, "tp": t}

    def dev_t(p):
        return {"seq": s, "tp": p}

    X, Z, TP = (nx, x, dev_x), (nz, z, dev_z), (ntp, t, dev_t)
    pending = []

    def send(group, src_of, dst, whole, ssem, rsem):
        n, me, dev = group
        for d in sorted(range(1, n), key=lambda d: -min(d, n - d)):
            p = lax.rem(me + d, n)
            rcopy(src_of(p), dst, ssem.at[0], rsem.at[0], dev(p)).start()
        if n > 1:
            pending.append(rcopy(whole, whole, ssem.at[0], rsem.at[0], dev(me)))

    def arrive(group, whole, ssem, rsem):
        n, me, dev = group
        if n > 1:
            rcopy(whole, whole, ssem.at[0], rsem.at[0], dev(me)).wait_recv()

    def slots(ref, n):
        return ref.at[pl.ds(0, n - 1)]

    def cot_rows(p, first=0, count=shard):
        return cot.at[pl.ds(pl.multiple_of(p * shard + first, 16), count)]

    load_cot = pltpu.make_async_copy(cot_hbm, cot_rows(t), cp_sem.at[0])
    load_gate = pltpu.make_async_copy(gate_hbm, gate_v, cp_sem.at[1])
    load_w = pltpu.make_async_copy(w_hbm, w_v, cp_sem.at[2])
    small = [
        pltpu.make_async_copy(source, target, cp_sem.at[3 + i])
        for i, (source, target) in enumerate(
            (
                (ld_hbm, ld_ref),
                (packed_hbm, packed),
                (expo_hbm, expo),
                (b_hbm, b_ref),
                (c_hbm, c_ref),
                (skip_hbm, skip_ref),
                (gain_hbm, gain_ref),
            )
        )
    ]
    load_ld, load_packed, load_expo, *load_rest = small
    for load in small:
        load.start()
    load_cot.start()
    load_gate.start()
    load_w.start()

    barrier = pltpu.get_barrier_semaphore()
    for n, me, dev in (X, Z, TP):
        for d in range(1, n):
            pl.semaphore_signal(
                barrier, inc=1, device_id=dev(lax.rem(me + d, n)), device_id_type=MESH
            )

    spread = (iota((SLOT, width), 1) // HEAD == iota((SLOT, width), 0)).astype(BF16)
    gather = (iota((width, SLOT), 0) // HEAD == iota((width, SLOT), 1)).astype(BF16)
    upper = (iota((L, L), 0) <= iota((L, L), 1)).astype(BF16)
    causal = iota((L, L), 0) >= iota((L, L), 1)
    left = iota((L, 128), 1) < HEAD

    def spread_heads(v):
        return sum(dot(part, spread) for part in pieces(v, 3))

    def head_sums(v):
        return sum(dot(part, gather) for part in pieces(v, 2))

    csr[...] = jnp.zeros_like(csr)
    segr[...] = jnp.zeros_like(segr)
    load_ld.wait()
    for k in range(chunks):
        csr[k, 0:heads, :] = ld_ref[:, k * L : (k + 1) * L]
    rows = csr[...].reshape(chunks * SLOT, L)
    rows = sum(dot(part, upper) for part in pieces(rows, 3))
    log_total = jnp.zeros((1, width), F32)
    for k in range(chunks):
        csr[k] = rows[k * SLOT : (k + 1) * SLOT, :]
        cols = rows[k * SLOT : (k + 1) * SLOT, :].T
        csc[k] = cols
        logs = spread_heads(cols)
        last = logs[L - 1 : L, :]
        log_total = log_total + last
        totb[k] = jnp.exp(last)
        endb[k * L : (k + 1) * L, :] = jnp.exp(last - logs)
        startb[k * L : (k + 1) * L, :] = jnp.exp(logs)
    dxs[x] = jnp.exp(log_total)

    load_packed.wait()
    load_expo.wait()
    powers = lax.shift_left(jnp.ones_like(expo[...]), expo[...] + 5).astype(F32) * (1.0 / 32.0)
    nibble = 4 * iota((8, width), 0)
    for k in range(chunks):
        factor_rows = jnp.concatenate(
            [powers[:, k * L : (k + 1) * L], jnp.zeros((8 - pairs, L), F32)], axis=0
        )
        factor = factor_rows.T
        wide = jnp.concatenate(
            [jnp.broadcast_to(factor[:, p : p + 1], (L, 128)) for p in range(pairs)], axis=1
        )
        words = packed[k * (L // 8) : (k + 1) * (L // 8), :]
        fields = jnp.concatenate(
            [
                lax.bitwise_and(
                    lax.shift_right_arithmetic(
                        jnp.broadcast_to(words[r : r + 1, :], (8, width)), nibble
                    ),
                    15,
                )
                - 8
                for r in range(L // 8)
            ],
            axis=0,
        )
        xb[k * L : (k + 1) * L, :] = (fields.astype(F32) * wide).astype(BF16)

    for load in load_rest:
        load.wait()
    run = jnp.zeros((128, width), F32)
    for k in range(chunks):
        rows = slice(k * L, (k + 1) * L)
        weighted = xb[rows, :].astype(F32) * endb[rows, :]
        parts = pieces(weighted, 2)
        xe[rows, :], xl[rows, :] = parts
        gb[k] = sum(dot(b_ref[rows, :], part, 0, 0) for part in parts)
        run = totb[k] * run + gb[k]
    sloc[...] = run

    def take_rows(ref, at, count):
        return ref[pl.ds(pl.multiple_of(at * count, count), count), :]

    def exchange_1(own, lbuf, ssem, rsem):
        send(
            X,
            lambda p: own.at[pl.ds(pl.multiple_of(p * qrows, qrows), qrows)],
            lbuf.at[x],
            slots(lbuf, nx),
            ssem,
            rsem,
        )
        lbuf[x] = take_rows(own, x, qrows)

    pl.semaphore_wait(barrier, (nx - 1) + (nz - 1) + (ntp - 1))
    send(X, lambda p: dxs.at[x], dxs.at[x], slots(dxs, nx), s_dx, r_dx)
    exchange_1(sloc, lb, s_p1, r_p1)

    load_cot.wait()
    part = shard // 2
    sibling = 2 * y + 1 - half
    after = 2 * lax.rem(y + 1, ny) + half
    before = 2 * lax.rem(y + ny - 1, ny) + half
    across = 2 * lax.rem(y + 2, ny) + half

    def cot_copy(j, p, to, first=0, count=shard):
        return rcopy(cot_rows(p, first, count), cot_rows(p, first, count), s_ag.at[0], r_ag.at[j], dev_t(to))

    def cot_send(j, p, to, *rows):
        cot_copy(j, p, to, *rows).start()

    def cot_wait(j, p, *rows):
        cot_copy(j, p, sibling, *rows).wait_recv()

    cot_send(0, t, sibling)
    if ny == 2:
        cot_send(1, t, after)
    elif ny == 4:
        cot_send(1, t, after, 0, part)
        cot_send(3, t, before, part, part)
        cot_send(2, t, after, part, part)
        cot_send(4, t, before, 0, part)

    def relay_cot():
        if ny == 4:
            cot_wait(1, before, 0, part)
            cot_send(5, before, after, 0, part)
            cot_wait(3, after, part, part)
            cot_send(6, after, before, part, part)

    def near_cot():
        if ny == 2:
            cot_wait(1, after)
            cot_send(7, after, sibling)
        elif ny == 4:
            cot_wait(2, before, part, part)
            cot_send(7, before, sibling)
            cot_wait(4, after, 0, part)
            cot_send(8, after, sibling)

    def far_cot():
        if ny == 4:
            cot_wait(5, across, 0, part)
            cot_wait(6, across, part, part)
            cot_send(9, across, sibling)

    def project(chip, first=False):
        terms = dot(
            cot[pl.ds(pl.multiple_of(chip * 2 * shard, 128), 2 * shard), :],
            w_v[:, pl.ds(pl.multiple_of(chip * 2 * shard, 128), 2 * shard)],
            0,
            1,
        )
        gvb[...] = terms if first else gvb[...] + terms

    def other(p):
        return p + 1 - 2 * half

    def exchange_2(lbuf, tbuf, ubuf, s1, r1, ssem, rsem, backward):
        arrive(X, slots(lbuf, nx), s1, r1)
        order = range(nx - 1, -1, -1) if backward else range(nx)
        row = None
        for k in order:
            add = lbuf[k].astype(F32)
            row = add if row is None else dxs[k] * row + add
        for k in range(nz):
            tbuf[k] = row[k * erows : (k + 1) * erows, :]
        send(Z, lambda p: tbuf.at[p], ubuf.at[z], slots(ubuf, nz), ssem, rsem)
        ubuf[z] = tbuf[z]

    def exchange_3(ubuf, qsend, qbuf, s2, r2, ssem, rsem, backward):
        arrive(Z, slots(ubuf, nz), s2, r2)
        order = range(nz - 1, -1, -1) if backward else range(nz)
        row = jnp.zeros((erows, width), F32)
        for k in order:
            qsend[k] = row
            row = dzs[k] * row + ubuf[k]
        send(Z, lambda p: qsend.at[p], qbuf.at[z], slots(qbuf, nz), ssem, rsem)
        qbuf[z] = qsend[z]

    def exchange_4(qbuf, lbuf, vsend, result, s3, r3, ssem, rsem, backward):
        arrive(Z, slots(qbuf, nz), s3, r3)
        for k in range(nz):
            vtop[k * erows : (k + 1) * erows, :] = qbuf[k]
        order = range(nx - 1, -1, -1) if backward else range(nx)
        row = vtop[...]
        for k in order:
            if backward:
                vsend[k], vl2[k] = pieces(row, 2)
            else:
                vsend[k] = row
            row = dxs[k] * row + lbuf[k].astype(F32)
        mine = pl.ds(pl.multiple_of(x * qrows, qrows), qrows)
        rest = pl.ds(0, (nx - 1) * qrows)
        send(X, lambda p: vsend.at[p], result.at[mine], result.at[rest], ssem, rsem)
        result[mine, :] = vsend[x]
        if backward:
            send(X, lambda p: vl2.at[p], h_low.at[mine], h_low.at[rest], s_hl, r_hl)
            h_low[mine, :] = vl2[x]

    def exchange_5(result, s4, r4):
        arrive(X, result.at[pl.ds(0, (nx - 1) * qrows)], s4, r4)


    skip_row = jnp.zeros((1, width), F32)
    head_of = iota((1, width), 1) // HEAD
    for h in range(heads):
        skip_row = jnp.where(head_of == h, skip_ref[0, h], skip_row)

    def at_chunk(k):
        return pl.ds(pl.multiple_of(k * L, L), L)

    def split_pair(v):
        zero = jnp.zeros_like(v)
        return jnp.concatenate([jnp.where(left, v, zero), jnp.where(left, zero, v)], axis=0)

    def inside(k, _):
        rows = at_chunk(k)
        both = dot(c_ref[rows, :], b_ref[rows, :], 1, 1)
        cross[k] = both
        for p in range(pairs):
            mixing = []
            for h in (2 * p, 2 * p + 1):
                spread_log = csc[k][:, h : h + 1] - csr[k][h : h + 1, :]
                decay = jnp.where(causal, jnp.exp(jnp.minimum(spread_log, 0.0)), 0.0)
                dec[k, h] = decay
                mixing.append(pieces(decay * both, 2))
            lanes = slice(128 * p, 128 * (p + 1))
            x_pair = xb[rows, lanes]
            x_split = split_pair(x_pair)
            yb[rows, lanes] = (
                dot(jnp.concatenate([m[0] for m in mixing], axis=1), x_split)
                + dot(jnp.concatenate([m[1] for m in mixing], axis=1), x_split)
                + skip_row[:, lanes] * x_pair.astype(F32)
            )
        return 0

    lax.fori_loop(0, chunks // 2, inside, 0)
    load_w.wait()
    cot_wait(0, sibling)
    project(y, True)
    arrive(X, slots(dxs, nx), s_dx, r_dx)
    row = dxs[0]
    for k in range(1, nx):
        row = row * dxs[k]
    dzs[z] = row
    send(Z, lambda p: dzs.at[z], dzs.at[z], slots(dzs, nz), s_dz, r_dz)

    exchange_2(lb, tb, ub, s_p1, r_p1, s_p2, r_p2, False)
    relay_cot()
    lax.fori_loop(chunks // 2, chunks, inside, 0)
    arrive(Z, slots(dzs, nz), s_dz, r_dz)
    exchange_3(ub, qs, qb, s_p2, r_p2, s_p3, r_p3, False)
    near_cot()
    exchange_4(qb, lb, vs, s_in, s_p3, r_p3, s_p4, r_p4, False)
    far_cot()
    if ny == 2:
        cot_wait(7, other(after))
        project(lax.rem(y + 1, ny))
    elif ny == 4:
        cot_wait(7, other(before))
        project(lax.rem(y + 3, ny))
        cot_wait(8, other(after))
        project(lax.rem(y + 1, ny))
    load_gate.wait()
    if ny == 4:
        cot_wait(9, other(across))
        project(lax.rem(y + 2, ny))
    gain_row = gain_ref[...].reshape(1, width)

    def prepare(k, _):
        rows = at_chunk(k)
        gate = gate_v[rows, :].astype(F32)
        act[rows, :] = gate * jax.nn.sigmoid(gate)
        gvg[rows, :] = gvb[rows, :] * gain_row
        return 0

    lax.fori_loop(0, chunks, prepare, 0)
    exchange_5(s_in, s_p4, r_p4)
    stb[0] = s_in[...].astype(F32)
    for k in range(1, chunks):
        stb[k] = totb[k - 1] * stb[k - 1] + gb[k - 1]
    lane = iota((L, 128), 1)

    def sums_of(k, acc):
        rows = at_chunk(k)
        start = sum(dot(c_ref[rows, :], part) for part in pieces(stb[k], 2))
        rsb[rows, :] = start
        y_now = yb[rows, :] + startb[rows, :] * start
        yb[rows, :] = y_now
        mixed = y_now * act[rows, :]
        mixb[rows, :] = mixed
        square = jnp.sum(mixed * mixed, axis=1, keepdims=True)
        inner = jnp.sum(gvg[rows, :] * mixed, axis=1, keepdims=True)
        return jnp.where(lane == 2 * k, square, jnp.where(lane == 2 * k + 1, inner, acc))

    packed_sums = lax.fori_loop(0, chunks, sums_of, jnp.zeros((L, 128), F32))
    sums[t] = packed_sums.T[0:8, :]
    send(TP, lambda p: sums.at[t], sums.at[t], slots(sums, ntp), s_tp, r_tp)
    arrive(TP, slots(sums, ntp), s_tp, r_tp)

    both = sums[0]
    for p in range(1, ntp):
        both = both + sums[p]
    totc[...] = jnp.concatenate([both, jnp.zeros((120, L), F32)], axis=0).T

    def token_scales(k):
        both = totc[...]
        square = jnp.sum(jnp.where(lane == 2 * k, both, 0.0), axis=1, keepdims=True)
        inner = jnp.sum(jnp.where(lane == 2 * k + 1, both, 0.0), axis=1, keepdims=True)
        return lax.rsqrt(square / total_width + 1e-05), inner

    def gradients(k, _):
        rows = at_chunk(k)
        scale, inner = token_scales(k)
        grad_mixed = scale * gvg[rows, :] - mixb[rows, :] * (
            (scale * scale * scale) * inner / total_width
        )
        grad_y = grad_mixed * act[rows, :]
        dyb[rows, :] = grad_y
        scaled = grad_y * startb[rows, :]
        hcb[k] = sum(dot(c_ref[rows, :], part, 0, 0) for part in pieces(scaled, 2))
        return 0

    lax.fori_loop(0, chunks, gradients, 0)
    run = hcb[chunks - 1]
    for k in range(chunks - 2, -1, -1):
        run = totb[k] * run + hcb[k]
    rloc[...] = run.astype(BF16)
    exchange_1(rloc, lb2, s_h1, r_h1)

    def gate_gradients(k, carry):
        gain_sum, skip_sum = carry
        rows = at_chunk(k)
        scale, inner = token_scales(k)
        mixed = mixb[rows, :]
        gate = gate_v[rows, :].astype(F32)
        sigma = jax.nn.sigmoid(gate)
        scaled_mixed = mixed * scale
        normed[rows, :] = (scaled_mixed * gain_row).astype(BF16)
        grad_mixed = scale * gvg[rows, :] - mixed * (
            (scale * scale * scale) * inner / total_width
        )
        ggate[rows, :] = (
            grad_mixed * yb[rows, :] * sigma * (1.0 + gate * (1.0 - sigma))
        ).astype(BF16)
        gain_sum = gain_sum + jnp.sum(gvb[rows, :] * scaled_mixed, axis=0, keepdims=True)
        skip_sum = skip_sum + jnp.sum(
            dyb[rows, :] * xb[rows, :].astype(F32), axis=0, keepdims=True
        )
        return gain_sum, skip_sum

    zero_row = jnp.zeros((1, width), F32)
    gain_sum, skip_sum = lax.fori_loop(0, chunks, gate_gradients, (zero_row, zero_row))
    gx[x, 0:1, :] = gain_sum
    gx[x, 1:2, :] = skip_sum
    send(X, lambda p: gx.at[x], gx.at[x], slots(gx, nx), s_gx, r_gx)

    columns = shard // nx
    front = pwa.shape[2]
    middle = nz // 2
    steps = sorted(range(1, nz), key=lambda i: -min(i, nz - i)) + [nz]

    def block_of(i):
        return lax.rem(z + i, nz)

    def mine_of(i, p):
        return pwa.at[block_of(i), pl.ds(pl.multiple_of(p * columns, columns), columns)]

    def sides(i):
        one, two = lax.rem(x + 1, nx), lax.rem(x + nx - 1, nx)
        return (one, two) if steps.index(i) % 2 == 0 else (two, one)

    def weight_copy(kind, i, to):
        source = (mine_of(i, lax.rem(x + 2, nx)), mine_of(i, to), xm.at[i - 1])[kind]
        target = (xa, xd, xc)[kind].at[i - 1]
        return rcopy(source, target, s_rx.at[kind], r_rx.at[kind, i - 1], dev_x(to))

    def weight_send(kind, i, to):
        weight_copy(kind, i, to).start()

    def weight_block(i):
        k = block_of(i)
        terms = dot(cot[pl.ds(pl.multiple_of(k * shard, shard), shard), :], normed[...]).astype(BF16)
        pwa[k] = terms[:, :front]
        pwb[k] = terms[:, front:]

    def block_send(i):
        near, far = sides(i)
        if nx == 4:
            weight_send(0, i, near)
        if nx > 1:
            weight_send(1, i, far)

    def weight_relay(i):
        near, _ = sides(i)
        if nx == 4:
            weight_copy(0, i, near).wait_recv()
            xm[i - 1] = (xa[i - 1].astype(F32) + mine_of(i, near)[...].astype(F32)).astype(BF16)
            weight_send(2, i, near)

    def ring_part(kind, i, up):
        rows = (columns, shard)[kind]
        cut = 16 * (3 * rows // 80)
        return (0, rows) if i != middle else (0, cut) if up else (cut, rows)

    def ring_copy(kind, i, up):
        first, end = ring_part(kind, i, up)
        slot = i - 1 if i != middle or up else nz - 1
        sends, lands, s_z, r_z = ((zsa, zra, s_za, r_za), (zsb, zrb, s_zb, r_zb))[kind]
        return rcopy(
            sends.at[i - 1, pl.ds(first, end - first)],
            lands.at[i - 1, pl.ds(first, end - first)],
            s_z.at[0],
            r_z.at[slot],
            dev_z(lax.rem(z + (1 if up else nz - 1), nz)),
        )

    def ring_add(kind, out, i, up):
        ring_copy(kind, i, up).wait_recv()
        first, end = ring_part(kind, i, up)
        part = (zra, zrb)[kind][i - 1, first:end, :].astype(F32)
        parts = [out[:first]] if first else []
        parts.append(out[first:end] + part)
        if end < out.shape[0]:
            parts.append(out[end:])
        return jnp.concatenate(parts, axis=0) if len(parts) > 1 else parts[0]

    def ring_step(kind, i, out):
        if i % nz < middle:
            out = ring_add(kind, out, i % nz + 1, True)
        if i > middle:
            out = ring_add(kind, out, i - 1, False)
        if i < nz:
            (zsa, zsb)[kind][i - 1] = out.astype(BF16)
            for up in (True, False):
                if i == middle or (i < middle) == up:
                    ring_copy(kind, i, up).start()
        return out

    def weight_rows(i):
        near, far = sides(i)
        out = mine_of(i, x)[...].astype(F32)
        if nx > 1:
            weight_copy(1, i, far).wait_recv()
            out = out + xd[i - 1].astype(F32)
        if nx == 4:
            weight_copy(2, i, near).wait_recv()
            out = out + xc[i - 1].astype(F32)
        out = ring_step(0, i, out)
        if i == nz:
            gow[:, :front] = out

    def back_rows(i):
        out = ring_step(1, i, pwb[block_of(i)].astype(F32))
        if i == nz:
            for p in range(nx):
                xsb[p] = out[p * columns : (p + 1) * columns, :].astype(BF16)
            send(X, lambda p: xsb.at[p], xrb.at[x], slots(xrb, nx), s_xb, r_xb)
            xrb[x] = xsb[x]

    def back_finish():
        arrive(X, slots(xrb, nx), s_xb, r_xb)
        out = xrb[0].astype(F32)
        for p in range(1, nx):
            out = out + xrb[p].astype(F32)
        gow[:, front:] = out

    def batch(first, end):
        return steps[(first * nz) // 8 : (end * nz) // 8]

    order = iter(steps)

    def back_steps(count):
        for _ in range(count):
            i = next(order, None)
            if i is not None:
                back_rows(i)

    for n, i in enumerate(steps):
        weight_block(i)
        if i in batch(0, 4):
            block_send(i)
        if n == 0:
            back_steps(1)
    exchange_2(lb2, tb2, ub2, s_h1, r_h1, s_h2, r_h2, True)
    arrive(X, slots(gx, nx), s_gx, r_gx)
    row = gx[0]
    for k in range(1, nx):
        row = row + gx[k]
    gz[z] = row
    send(Z, lambda p: gz.at[z], gz.at[z], slots(gz, nz), s_gz, r_gz)

    def inside_back(k, _):
        rows = at_chunk(k)
        both = cross[k]
        summed = jnp.zeros((L, L), F32)
        lane = iota((L, SLOT), 1)
        row_sums = jnp.zeros((L, SLOT), F32)
        for p in range(pairs):
            lanes = slice(128 * p, 128 * (p + 1))
            x_pair = xb[rows, lanes]
            high, low = pieces(dyb[rows, lanes], 2)
            grads = split_pair(high)
            dots = dot(grads, x_pair, 1, 1) + dot(split_pair(low), x_pair, 1, 1)
            mixing = []
            for i in range(2):
                h = 2 * p + i
                decay = dec[k, h]
                weighted = dots[i * L : (i + 1) * L, :] * decay
                summed = summed + weighted
                terms = weighted * both
                row_sums = row_sums + jnp.where(
                    lane == h, jnp.sum(terms, axis=1, keepdims=True), 0.0
                )
                segr[k, h : h + 1, :] = jnp.sum(terms, axis=0, keepdims=True)
                mixing.append((decay * both).astype(BF16))
            dxi[rows, lanes] = dot(jnp.concatenate(mixing, axis=0), grads, 0, 0)
        sum_parts = pieces(summed, 2)
        accp[rows, :] = sum(dot(part, c_ref[rows, :], 0, 0) for part in sum_parts)
        segc[k] = row_sums - segr[k].T
        scaled = dyb[rows, :] * startb[rows, :]
        accr[rows, :] = (
            sum(dot(part, b_ref[rows, :]) for part in sum_parts)
            + sum(dot(part, stb[k].astype(BF16), 1, 1) for part in pieces(scaled, 2))
        ).astype(BF16)
        return 0

    lax.fori_loop(0, chunks // 2, inside_back, 0)
    for i in batch(0, 1):
        weight_relay(i)
    back_steps(2 if nz == 8 else 0)
    exchange_3(ub2, qs2, qb2, s_h2, r_h2, s_h3, r_h3, True)
    for i in batch(4, 8):
        block_send(i)
    lax.fori_loop(chunks // 2, chunks, inside_back, 0)
    for i in batch(1, 3):
        weight_relay(i)
    for i in batch(0, 1):
        weight_rows(i)
    back_steps(2 if nz == 8 else 0)
    exchange_4(qb2, lb2, vs2, h_in, s_h3, r_h3, s_h4, r_h4, True)

    share = tokens // ntp

    def reduce_1(acc, which, ssem, rsem):
        send(
            TP,
            lambda p: acc.at[pl.ds(pl.multiple_of(p * share, share), share)],
            red.at[which, t],
            red.at[which, pl.ds(0, ntp - 1)],
            ssem,
            rsem,
        )
        red[which, t] = take_rows(acc, t, share)

    def reduce_2(which, s1, r1, ssem, rsem):
        arrive(TP, red.at[which, pl.ds(0, ntp - 1)], s1, r1)
        out = red[which, 0].astype(F32)
        for p in range(1, ntp):
            out = out + red[which, p].astype(F32)
        redo[which, t] = out.astype(BF16)
        send(TP, lambda p: redo.at[which, t], redo.at[which, t], redo.at[which, pl.ds(0, ntp - 1)], ssem, rsem)

    def reduce_3(out_ref, which, ssem, rsem):
        arrive(TP, redo.at[which, pl.ds(0, ntp - 1)], ssem, rsem)
        for p in range(ntp):
            out_ref[p * share : (p + 1) * share, :] = redo[which, p].astype(F32)

    reduce_1(accr, 0, s_c1, r_c1)
    for i in batch(3, 4):
        weight_relay(i)
    for i in batch(1, 3):
        weight_rows(i)
    for i in batch(4, 6):
        weight_relay(i)
    back_steps(2 if nz == 8 else 0)
    exchange_5(h_in, s_h4, r_h4)

    def states_back(i, run):
        k = chunks - 1 - i
        rows = at_chunk(k)
        state = run.astype(BF16)
        late = dot(xe[rows, :], state, 1, 1) + dot(xl[rows, :], state, 1, 1)
        accw[rows, :] = (accp[rows, :] + late).astype(BF16)
        return totb[k] * run + hcb[k]

    lax.fori_loop(0, chunks, states_back, h_in[...].astype(F32))
    reduce_1(accw, 1, s_w1, r_w1)
    reduce_2(0, s_c1, r_c1, s_c2, r_c2)
    def finish(i, run):
        k = chunks - 1 - i
        rows = at_chunk(k)
        grad_y = dyb[rows, :]
        write = endb[rows, :] * sum(dot(b_ref[rows, :], part) for part in pieces(run, 2))
        gin[rows, :] = (skip_row * grad_y + dxi[rows, :] + write).astype(BF16)
        leaving = xb[rows, :].astype(F32) * write
        arriving = grad_y * startb[rows, :] * rsb[rows, :]
        seg = segc[k] + head_sums(arriving - leaving)
        final = jnp.sum(leaving, axis=0, keepdims=True) + totb[k] * jnp.sum(
            run * stb[k], axis=0, keepdims=True
        )
        final = head_sums(jnp.broadcast_to(final, (8, width)))[0:1]
        whole = sum(dot(upper, part) for part in pieces(seg, 2)) + final
        sumd[k] = whole.T
        return totb[k] * run + hcb[k]

    exchange_5(h_low, s_hl, r_hl)
    run = lax.fori_loop(0, 3 * chunks // 4, finish, h_in[...].astype(F32) + h_low[...].astype(F32))
    for i in batch(3, 5):
        weight_rows(i)
    for i in batch(6, 8):
        weight_relay(i)

    reduce_2(1, s_w1, r_w1, s_w2, r_w2)
    lax.fori_loop(3 * chunks // 4, chunks, finish, run)
    for k in range(chunks):
        gdecay[:, k * L : (k + 1) * L] = sumd[k, 0:heads, :]
    back_steps(nz)
    for i in batch(5, 8)[:-1]:
        weight_rows(i)
    arrive(Z, slots(gz, nz), s_gz, r_gz)
    row = gz[0]
    for k in range(1, nz):
        row = row + gz[k]
    ggain[...] = row[0:1]
    gskip[...] = head_sums(jnp.concatenate([row, jnp.zeros((6, width), F32)], axis=0))[1:2, 0:heads]
    reduce_3(gread, 0, s_c2, r_c2)
    back_finish()
    weight_rows(nz)
    reduce_3(gwrite, 1, s_w2, r_w2)
    for copy in pending:
        copy.wait_send()

    def all_left(whole, sem):
        rcopy(whole, whole, sem, r_ag.at[0], dev_t(sibling)).wait_send()

    all_left(cot.at[pl.ds(0, (2 * ny - 1) * shard)], s_ag.at[0])
    for kind in range(3):
        if nx == 4 or (nx > 1 and kind == 1):
            all_left(xa, s_rx.at[kind])
    all_left(slots(zra, nz), s_za.at[0])
    all_left(slots(zrb, nz), s_zb.at[0])


def copy_out(*refs):
    count = 8
    sources, targets, sem = refs[:count], refs[count : 2 * count], refs[-1]
    stores = [
        pltpu.make_async_copy(sources[k], targets[k], sem.at[k])
        for k in range(count)
        if k not in (5, 6)
    ]
    for store in stores:
        store.start()
    for k in (5, 6):
        targets[k][...] = sources[k][...].reshape(targets[k].shape)
    for store in stores:
        store.wait()


def hand_out(outs):
    vmem = pl.BlockSpec(memory_space=pltpu.VMEM)
    hbm = pl.BlockSpec(memory_space=pl.ANY)
    shapes = [
        jax.ShapeDtypeStruct(o.shape[1:] if k in (5, 6) else o.shape, o.dtype)
        for k, o in enumerate(outs)
    ]
    done = pl.pallas_call(
        copy_out,
        out_shape=shapes,
        in_specs=[vmem] * 8,
        out_specs=[vmem if k in (5, 6) else hbm for k in range(8)],
        scratch_shapes=[pltpu.SemaphoreType.DMA((8,))],
        name="hand_out",
    )(*[pltpu.with_memory_space_constraint(o, pltpu.VMEM) for o in outs])
    return (*done[:7], done[7].T)


def on_device(nx, nz, ntp, packed, expo, gate, write, read, decay, skip, gain, weight, cotangent):
    cot = cotangent.T
    tokens, width = gate.shape
    heads = decay.shape[0]
    model = weight.shape[1]
    shard = cot.shape[0]
    chunks = tokens // L
    n = write.shape[1]
    columns = model // (nx * nz)
    qrows, erows = n // nx, n // (nx * nz)
    share = tokens // ntp
    front = FRONT

    def wide(kind=F32):
        return pltpu.VMEM((tokens, width), kind)

    def exchange(kind):
        return [
            pltpu.VMEM((n, width), kind),
            pltpu.VMEM((nx, qrows, width), kind),
            pltpu.VMEM((nz, erows, width), F32),
            pltpu.VMEM((nz, erows, width), F32),
            pltpu.VMEM((nz, erows, width), F32),
            pltpu.VMEM((nz, erows, width), F32),
            pltpu.VMEM((nx, qrows, width), kind),
            pltpu.VMEM((n, width), kind),
        ]

    def sems(sends, lands):
        return [pltpu.SemaphoreType.DMA((sends,)), pltpu.SemaphoreType.DMA((lands,))]

    scratch = [
        *[pltpu.VMEM(a.shape, a.dtype) for a in (packed, expo, write, read, decay)],
        pltpu.SMEM((1, heads), F32),
        pltpu.VMEM((width,), F32),
        pltpu.VMEM((tokens, width), BF16),
        pltpu.VMEM((width, model), BF16),
        pltpu.VMEM((model, tokens), BF16),
        wide(BF16),
        *[wide() for _ in range(7)],
        wide(BF16),
        wide(),
        wide(),
        wide(BF16),
        wide(BF16),
        pltpu.VMEM((tokens, n), F32),
        pltpu.VMEM((chunks, SLOT, L), F32),
        pltpu.VMEM((chunks, L, SLOT), F32),
        pltpu.VMEM((chunks, 1, width), F32),
        pltpu.VMEM((chunks, heads, L, L), F32),
        pltpu.VMEM((chunks, L, L), F32),
        pltpu.VMEM((chunks, n, width), F32),
        pltpu.VMEM((chunks, n, width), F32),
        pltpu.VMEM((chunks, n, width), F32),
        pltpu.VMEM((chunks, SLOT, L), F32),
        pltpu.VMEM((chunks, SLOT, L), F32),
        pltpu.VMEM((chunks, L, SLOT), F32),
        wide(),
        *exchange(F32),
        *exchange(BF16),
        *exchange(BF16)[-2:],
        pltpu.VMEM((qrows, width), F32),
        pltpu.VMEM((nx, 1, width), F32),
        pltpu.VMEM((nz, 1, width), F32),
        pltpu.VMEM((ntp, 8, L), F32),
        pltpu.VMEM((L, 128), F32),
        pltpu.VMEM((nx, 2, width), F32),
        pltpu.VMEM((nz, 2, width), F32),
        pltpu.VMEM((nz, shard, front), BF16),
        pltpu.VMEM((nz, shard, width - front), BF16),
        *[pltpu.VMEM((nz, columns, front), BF16) for _ in range(6)],
        *[pltpu.VMEM((nz, shard, width - front), BF16) for _ in range(2)],
        *[pltpu.VMEM((nx, columns, width - front), BF16) for _ in range(2)],
        pltpu.VMEM((tokens, n), BF16),
        pltpu.VMEM((tokens, n), BF16),
        pltpu.VMEM((2, ntp, share, n), BF16),
        pltpu.VMEM((2, ntp, share, n), BF16),
        pltpu.SemaphoreType.DMA((10,)),
        *sems(1, 10),
        *(sems(1, 1) * 2),
        *(sems(1, 1) * 9),
        *(sems(1, 1) * 3),
        pltpu.SemaphoreType.DMA((3,)),
        pltpu.SemaphoreType.DMA((3, nz)),
        *(sems(1, nz) * 2),
        *(sems(1, 1) * 5),
    ]
    vmem = pl.BlockSpec(memory_space=pltpu.VMEM)
    hbm = pl.BlockSpec(memory_space=pl.ANY)
    outs = pl.pallas_call(
        functools.partial(core, nx, nz, ntp),
        out_shape=(
            pltpu.VMEM((tokens, width), BF16),
            pltpu.VMEM((tokens, width), BF16),
            pltpu.VMEM((tokens, n), F32),
            pltpu.VMEM((tokens, n), F32),
            pltpu.VMEM((heads, tokens), F32),
            pltpu.VMEM((1, heads), F32),
            pltpu.VMEM((1, width), F32),
            pltpu.VMEM((columns, width), F32),
        ),
        in_specs=[hbm] * 10,
        out_specs=(vmem,) * 8,
        scratch_shapes=scratch,
        compiler_params=pltpu.CompilerParams(
            collective_id=0, has_side_effects=True, vmem_limit_bytes=54 * 1024 * 1024
        ),
        name="layer_backward",
    )(packed, expo, gate, write, read, decay, skip[None, :], gain, weight, cot)
    return hand_out(outs)


def solution(mesh):
    ntp = mesh.shape["tp"]
    nz = mesh.shape["seq"] // NX
    return jax.shard_map(
        functools.partial(on_device, NX, nz, ntp),
        mesh=mesh,
        in_specs=(
            P("seq", "tp"),
            P("tp", "seq"),
            P("seq", "tp"),
            P("seq", None),
            P("seq", None),
            P("tp", "seq"),
            P("tp"),
            P("tp"),
            P("tp", None),
            P("seq", "tp"),
        ),
        out_specs=(
            P("seq", "tp"),
            P("seq", "tp"),
            P("seq", None),
            P("seq", None),
            P("tp", "seq"),
            P("tp"),
            P("tp"),
            P("tp", "seq"),
        ),
        check_vma=False,
    )
```
